8 devices in a mesh: dp: 2 (over z, y), sp: 4 (over x, core).
Axes of the slice: x: 2, y: 2, z: 1, core: 2. Of those that a mesh axis runs over, the one named last changes fastest.
Arguments:
- hidden: bfloat16 [8192, 3072], P(('dp', 'sp')), parts along dimension 0
- positions: int32 [8192], P(('dp', 'sp')), parts along dimension 0
- d_attn: bfloat16 [8192, 3072], P(('dp', 'sp')), parts along dimension 0
- ln_weight: bfloat16 [3072], replicated
- w_q: bfloat16 [3072, 3072], replicated
- w_k: bfloat16 [3072, 1024], replicated
- w_v: bfloat16 [3072, 1024], replicated
- w_o: bfloat16 [3072, 3072], replicated
Outputs:
- output 1: bfloat16 [8192, 3072], P(('dp', 'sp')), parts along dimension 0
- output 2: bfloat16 [8192, 3072], P(('dp', 'sp')), parts along dimension 0
- output 3: bfloat16 [6144], P('dp'), parts along dimension 0
- output 4: bfloat16 [6144, 3072], P('dp'), parts along dimension 0
- output 5: bfloat16 [6144, 1024], P('dp'), parts along dimension 0
- output 6: bfloat16 [6144, 1024], P('dp'), parts along dimension 0
- output 7: bfloat16 [6144, 3072], P('dp'), parts along dimension 0
There are 2 independent parts. The reference program is written for one: setup_inputs(seed, part) draws one part's arguments, and reference() takes and returns one part's arrays. A program takes and returns all parts, laid end to end along the dimension named above; an argument that names none is the same for every part.
All inputs are finite; a program needn't handle non-finite values.
Results may differ from the reference program's by a relative error of at most 0.0121207.
Values are sent between devices in bfloat16 or wider.
A program may use at most 1 GiB of HBM per device.

```python
import math
import jax
import jax.numpy as jnp
from jax import lax

MODEL_DIM = 3072
NUM_HEADS = 24
NUM_KV_HEADS = 8
HEAD_DIM = 128
SEQ_LEN = 4096
LN_EPS = 1e-5
ROPE_BASE = 10000.0
GROUP_SIZE = NUM_HEADS // NUM_KV_HEADS
ROW_BLOCK = math.gcd(SEQ_LEN, 64)
NUM_BLOCKS = SEQ_LEN // ROW_BLOCK
SCORE_SCALE = HEAD_DIM ** -0.5


def setup_inputs(seed: int = 0, part: int = 0) -> dict:
    base_key = jax.random.key(seed)
    part_keys = jax.random.split(jax.random.fold_in(base_key, part), 3)
    weight_keys = jax.random.split(base_key, 5)
    hidden = jax.random.normal(part_keys[0], (SEQ_LEN, MODEL_DIM), jnp.float32).astype(jnp.bfloat16)
    pos_steps = jax.random.randint(part_keys[1], (SEQ_LEN,), 1, 4, dtype=jnp.int32)
    positions = (jnp.cumsum(pos_steps) - pos_steps[0]).astype(jnp.int32)
    d_attn = jax.random.normal(part_keys[2], (SEQ_LEN, MODEL_DIM), jnp.float32).astype(jnp.bfloat16)
    ln_weight = (1.0 + 0.25 * jax.random.normal(weight_keys[0], (MODEL_DIM,), jnp.float32)).astype(jnp.bfloat16)
    q_scale = math.sqrt(math.log(SEQ_LEN) / MODEL_DIM)
    kv_scale = MODEL_DIM ** -0.5
    o_scale = (NUM_HEADS * HEAD_DIM) ** -0.5
    w_q = (jax.random.normal(weight_keys[1], (MODEL_DIM, NUM_HEADS * HEAD_DIM), jnp.float32) * q_scale).astype(jnp.bfloat16)
    w_k = (jax.random.normal(weight_keys[2], (MODEL_DIM, NUM_KV_HEADS * HEAD_DIM), jnp.float32) * kv_scale).astype(jnp.bfloat16)
    w_v = (jax.random.normal(weight_keys[3], (MODEL_DIM, NUM_KV_HEADS * HEAD_DIM), jnp.float32) * kv_scale).astype(jnp.bfloat16)
    w_o = (jax.random.normal(weight_keys[4], (NUM_HEADS * HEAD_DIM, MODEL_DIM), jnp.float32) * o_scale).astype(jnp.bfloat16)
    return {'hidden': hidden, 'positions': positions, 'd_attn': d_attn, 'ln_weight': ln_weight,
            'w_q': w_q, 'w_k': w_k, 'w_v': w_v, 'w_o': w_o}


def norm_f32(hid_f32, weight_f32):
    mean_val = jnp.mean(hid_f32, axis=-1, keepdims=True)
    centered = hid_f32 - mean_val
    var_val = jnp.mean(centered * centered, axis=-1, keepdims=True)
    return centered * lax.rsqrt(var_val + LN_EPS) * weight_f32


def rope_tables(positions):
    inv_freq = ROPE_BASE ** (-jnp.arange(0, HEAD_DIM, 2, dtype=jnp.float32) / HEAD_DIM)
    angles = positions.astype(jnp.float32)[:, None] * inv_freq[None, :]
    return jnp.cos(angles)[:, None, :], jnp.sin(angles)[:, None, :]


def apply_rope(values, cos_t, sin_t):
    rot_pairs = values.reshape(values.shape[:-1] + (HEAD_DIM // 2, 2))
    even_part = rot_pairs[..., 0]
    odd_part = rot_pairs[..., 1]
    new_even = even_part * cos_t - odd_part * sin_t
    new_odd = odd_part * cos_t + even_part * sin_t
    return jnp.stack([new_even, new_odd], axis=-1).reshape(values.shape)


def block_probs(q_f32, row_start, k_f32):
    scores = jnp.einsum('qgrd,kgd->grqk', q_f32, k_f32) * SCORE_SCALE
    row_ids = row_start + jnp.arange(ROW_BLOCK)
    col_ids = jnp.arange(SEQ_LEN)
    scores = jnp.where(row_ids[:, None] >= col_ids[None, :], scores, -jnp.inf)
    return jax.nn.softmax(scores, axis=-1)


def reference(hidden, positions, d_attn, ln_weight, w_q, w_k, w_v, w_o):
    normed32, norm_vjp = jax.vjp(norm_f32, hidden.astype(jnp.float32), ln_weight.astype(jnp.float32))
    normed = normed32.astype(jnp.bfloat16)
    cos_t, sin_t = rope_tables(positions)
    q_rot = apply_rope(jnp.dot(normed, w_q, preferred_element_type=jnp.float32).reshape(SEQ_LEN, NUM_HEADS, HEAD_DIM), cos_t, sin_t).astype(jnp.bfloat16)
    k_rot = apply_rope(jnp.dot(normed, w_k, preferred_element_type=jnp.float32).reshape(SEQ_LEN, NUM_KV_HEADS, HEAD_DIM), cos_t, sin_t).astype(jnp.bfloat16)
    v_all = jnp.dot(normed, w_v, preferred_element_type=jnp.float32).astype(jnp.bfloat16).reshape(SEQ_LEN, NUM_KV_HEADS, HEAD_DIM)
    q_grp = q_rot.reshape(NUM_BLOCKS, ROW_BLOCK, NUM_KV_HEADS, GROUP_SIZE, HEAD_DIM)
    k_f32 = k_rot.astype(jnp.float32)
    v_f32 = v_all.astype(jnp.float32)
    block_ids = jnp.arange(NUM_BLOCKS)

    def fwd_block(block_in):
        q_block, block_idx = block_in
        attn_prob = block_probs(q_block.astype(jnp.float32), block_idx * ROW_BLOCK, k_f32)
        prob_bf = attn_prob.astype(jnp.bfloat16).astype(jnp.float32)
        return jnp.einsum('grqk,kgd->qgrd', prob_bf, v_f32).astype(jnp.bfloat16)

    o_grp = lax.map(fwd_block, (q_grp, block_ids))
    o_tok = o_grp.reshape(SEQ_LEN, NUM_HEADS * HEAD_DIM)
    attn_out = jnp.dot(o_tok, w_o, preferred_element_type=jnp.float32).astype(jnp.bfloat16)
    d_o = jnp.dot(d_attn, w_o.T, preferred_element_type=jnp.float32).astype(jnp.bfloat16)
    dw_o = jnp.dot(o_tok.T, d_attn, preferred_element_type=jnp.float32)
    do_grp = d_o.reshape(NUM_BLOCKS, ROW_BLOCK, NUM_KV_HEADS, GROUP_SIZE, HEAD_DIM)

    def bwd_block(carry, block_in):
        dk_acc, dv_acc = carry
        q_block, do_block, block_idx = block_in
        q_f32 = q_block.astype(jnp.float32)
        do_f32 = do_block.astype(jnp.float32)
        attn_prob = block_probs(q_f32, block_idx * ROW_BLOCK, k_f32)
        prob_bf = attn_prob.astype(jnp.bfloat16).astype(jnp.float32)
        d_prob = jnp.einsum('qgrd,kgd->grqk', do_f32, v_f32)
        row_dot = jnp.sum(attn_prob * d_prob, axis=-1, keepdims=True)
        d_score = (attn_prob * (d_prob - row_dot) * SCORE_SCALE).astype(jnp.bfloat16).astype(jnp.float32)
        dq_block = jnp.einsum('grqk,kgd->qgrd', d_score, k_f32).astype(jnp.bfloat16)
        dk_acc = dk_acc + jnp.einsum('grqk,qgrd->kgd', d_score, q_f32)
        dv_acc = dv_acc + jnp.einsum('grqk,qgrd->kgd', prob_bf, do_f32)
        return (dk_acc, dv_acc), dq_block

    zero_acc = jnp.zeros((SEQ_LEN, NUM_KV_HEADS, HEAD_DIM), jnp.float32)
    kv_sums, dq_grp = lax.scan(bwd_block, (zero_acc, zero_acc), (q_grp, do_grp, block_ids))
    dk_bf = kv_sums[0].astype(jnp.bfloat16)
    dv_bf = kv_sums[1].astype(jnp.bfloat16)
    g_q = apply_rope(dq_grp.reshape(SEQ_LEN, NUM_HEADS, HEAD_DIM).astype(jnp.float32), cos_t, -sin_t).astype(jnp.bfloat16).reshape(SEQ_LEN, NUM_HEADS * HEAD_DIM)
    g_k = apply_rope(dk_bf.astype(jnp.float32), cos_t, -sin_t).astype(jnp.bfloat16).reshape(SEQ_LEN, NUM_KV_HEADS * HEAD_DIM)
    g_v = dv_bf.reshape(SEQ_LEN, NUM_KV_HEADS * HEAD_DIM)
    d_normed = (jnp.dot(g_q, w_q.T, preferred_element_type=jnp.float32)
                + jnp.dot(g_k, w_k.T, preferred_element_type=jnp.float32)
                + jnp.dot(g_v, w_v.T, preferred_element_type=jnp.float32))
    dw_q = jnp.dot(normed.T, g_q, preferred_element_type=jnp.float32)
    dw_k = jnp.dot(normed.T, g_k, preferred_element_type=jnp.float32)
    dw_v = jnp.dot(normed.T, g_v, preferred_element_type=jnp.float32)
    d_hid, d_lnw = norm_vjp(d_normed)
    return (attn_out, d_hid.astype(jnp.bfloat16), d_lnw.astype(jnp.bfloat16), dw_q.astype(jnp.bfloat16),
            dw_k.astype(jnp.bfloat16), dw_v.astype(jnp.bfloat16), dw_o.astype(jnp.bfloat16))
```

```python
import math
import jax
import jax.numpy as jnp
from jax import lax
from jax.experimental import pallas as pl
from jax.experimental.pallas import tpu as pltpu
from jax.sharding import PartitionSpec as P

HEAD_DIM = 128
LN_EPS = 1e-5
ROPE_BASE = 10000.0
REP = 3
BQ = 256
BK = 512
LOG2E = math.log2(math.e)
SCALE = HEAD_DIM ** -0.5
VMEM_BYTES = 60 * 1024 * 1024
F32 = jnp.float32
BF16 = jnp.bfloat16


def cost(flops, nbytes):
    return pl.CostEstimate(flops=int(flops), bytes_accessed=int(nbytes), transcendentals=0)


def mm(lhs, rhs, dims):
    return lax.dot_general(lhs, rhs, (dims, ((), ())), preferred_element_type=F32)


def rotate(val, cos_t, sin_t):
    lane = lax.broadcasted_iota(jnp.int32, val.shape, 1)
    swapped = jnp.where(lane % 2 == 0, pltpu.roll(val, HEAD_DIM - 1, 1), pltpu.roll(val, 1, 1))
    return val * cos_t + swapped * sin_t


def qkv_kernel(idx, x_ref, lnw_ref, wq_ref, wk_ref, wv_ref, cos_ref, sin_ref, *rest):
    h_ref, qkv_ref = rest[-2:]
    xf = x_ref[...].astype(F32)
    mean = jnp.mean(xf, axis=-1, keepdims=True)
    cen = xf - mean
    var = jnp.mean(cen * cen, axis=-1, keepdims=True)
    h = (cen * lax.rsqrt(var + LN_EPS) * lnw_ref[...].astype(F32)).astype(BF16)
    h_ref[...] = h
    cos_t = cos_ref[...]
    sin_t = sin_ref[...]
    nq = wq_ref.shape[1]
    nk = wk_ref.shape[1]
    q = mm(h, wq_ref[...], ((1,), (0,)))
    for n in range(nq // HEAD_DIM):
        sl = slice(n * HEAD_DIM, (n + 1) * HEAD_DIM)
        qkv_ref[:, sl] = rotate(q[:, sl], cos_t, sin_t).astype(BF16)
    k = mm(h, wk_ref[...], ((1,), (0,)))
    for n in range(nk // HEAD_DIM):
        sl = slice(n * HEAD_DIM, (n + 1) * HEAD_DIM)
        qkv_ref[:, nq + n * HEAD_DIM:nq + (n + 1) * HEAD_DIM] = rotate(k[:, sl], cos_t, sin_t).astype(BF16)
    qkv_ref[:, nq + nk:] = mm(h, wv_ref[...], ((1,), (0,))).astype(BF16)


def qkv_block(idx, x, ln_w, w_q, w_k, w_v, cos_t, sin_t, seq, n_dev, prev):
    rows, dim = x.shape
    cq, ck = w_q.shape[1] // n_dev, w_k.shape[1] // n_dev
    per = rows // BQ
    const = lambda i, ix: (0, 0)
    head = lambda i, ix: (0, ix[0])
    here = lambda i, ix: (ix[1] * per + i, 0)
    in_specs = [
        pl.BlockSpec((BQ, dim), lambda i, ix: (i, 0)),
        pl.BlockSpec((1, dim), const),
        pl.BlockSpec((dim, cq), head),
        pl.BlockSpec((dim, ck), head),
        pl.BlockSpec((dim, ck), head),
        pl.BlockSpec((BQ, HEAD_DIM), here),
        pl.BlockSpec((BQ, HEAD_DIM), here),
    ]
    args = [idx, x, ln_w, w_q, w_k, w_v, cos_t, sin_t]
    aliases = {}
    if prev is not None:
        in_specs += [pl.BlockSpec(memory_space=pl.ANY)] * 2
        args += list(prev)
        aliases = {8: 0, 9: 1}
    cols = cq + 2 * ck
    return pl.pallas_call(
        qkv_kernel,
        out_shape=(jax.ShapeDtypeStruct((seq, dim), BF16), jax.ShapeDtypeStruct((seq, cols), BF16)),
        grid_spec=pltpu.PrefetchScalarGridSpec(
            num_scalar_prefetch=1, grid=(per,), in_specs=in_specs,
            out_specs=(pl.BlockSpec((BQ, dim), here), pl.BlockSpec((BQ, cols), here))),
        input_output_aliases=aliases,
        compiler_params=pltpu.CompilerParams(dimension_semantics=("arbitrary",), vmem_limit_bytes=VMEM_BYTES),
        cost_estimate=cost(2 * rows * dim * cols, 2 * (2 * rows * dim + dim * cols + rows * cols)),
        name="ln_qkv",
    )(*args)


def do_kernel(idx, g_ref, wo_ref, *rest):
    gall_ref, do_ref = rest[-2:]
    g = g_ref[...]
    gall_ref[...] = g
    do_ref[...] = mm(g, wo_ref[...], ((1,), (1,))).astype(BF16)


def do_block(idx, g, w_o, seq, n_dev, prev):
    rows, dim = g.shape
    ce = w_o.shape[0] // n_dev
    per = rows // BQ
    here = lambda i, ix: (ix[1] * per + i, 0)
    in_specs = [
        pl.BlockSpec((BQ, dim), lambda i, ix: (i, 0)),
        pl.BlockSpec((ce, dim), lambda i, ix: (ix[0], 0)),
    ]
    args = [idx, g, w_o]
    aliases = {}
    if prev is not None:
        in_specs += [pl.BlockSpec(memory_space=pl.ANY)] * 2
        args += list(prev)
        aliases = {3: 0, 4: 1}
    return pl.pallas_call(
        do_kernel,
        out_shape=(jax.ShapeDtypeStruct((seq, dim), BF16), jax.ShapeDtypeStruct((seq, ce), BF16)),
        grid_spec=pltpu.PrefetchScalarGridSpec(
            num_scalar_prefetch=1, grid=(per,), in_specs=in_specs,
            out_specs=(pl.BlockSpec((BQ, dim), here), pl.BlockSpec((BQ, ce), here))),
        input_output_aliases=aliases,
        compiler_params=pltpu.CompilerParams(dimension_semantics=("arbitrary",), vmem_limit_bytes=VMEM_BYTES),
        cost_estimate=cost(2 * rows * dim * ce, 2 * (2 * rows * dim + dim * ce + rows * ce)),
        name="d_o",
    )(*args)


def stack_heads(val):
    return jnp.concatenate([val[:, n * HEAD_DIM:(n + 1) * HEAD_DIM] for n in range(REP)], axis=0)


def flip(val):
    return val.astype(F32).T.astype(BF16)


def causal(row_start, key_start, shape):
    key = key_start + lax.broadcasted_iota(jnp.int32, shape, 0)
    query = row_start + lax.broadcasted_iota(jnp.int32, shape, 1) % BQ
    return key <= query


def fwd_kernel(q_ref, k_ref, v_ref, o_ref, ot_ref, lse_ref, qt_sc, vt_sc, acc_sc, ml_sc):
    blk = pl.program_id(1)
    width = REP * BQ
    n_chunks = k_ref.shape[0] // BK

    @pl.when(blk == 0)
    def _():
        def one(j, _):
            vt_sc[j] = flip(v_ref[pl.ds(j * BK, BK), :])
            return 0

        lax.fori_loop(0, n_chunks, one, 0)

    qt_sc[...] = flip(stack_heads(q_ref[...]))
    acc_sc[...] = jnp.zeros_like(acc_sc)
    ml_sc[0:1, :] = jnp.full((1, width), -jnp.inf, F32)
    ml_sc[1:2, :] = jnp.zeros((1, width), F32)

    def chunk(j, masked):
        s = mm(k_ref[pl.ds(j * BK, BK), :], qt_sc[...], ((1,), (0,))) * (SCALE * LOG2E)
        if masked:
            s = jnp.where(causal(blk * BQ, j * BK, s.shape), s, -jnp.inf)
        m_old = ml_sc[0:1, :]
        m_new = jnp.maximum(m_old, jnp.max(s, axis=0, keepdims=True))
        alpha = jnp.exp2(m_old - m_new)
        p = jnp.exp2(s - m_new)
        ml_sc[0:1, :] = m_new
        ml_sc[1:2, :] = ml_sc[1:2, :] * alpha + jnp.sum(p, axis=0, keepdims=True)
        acc_sc[...] = acc_sc[...] * alpha + mm(vt_sc[j], p.astype(BF16), ((1,), (0,)))

    n_full = (blk * BQ) // BK

    def body(j, _):
        chunk(j, False)
        return 0

    lax.fori_loop(0, n_full, body, 0)
    chunk(n_full, True)
    total = ml_sc[1:2, :]
    out_t = acc_sc[...] / total
    ot_ref[0, 0] = out_t
    lse_ref[0, 0] = ml_sc[0:1, :] + jnp.log2(total)
    for n in range(REP):
        o_ref[:, n * HEAD_DIM:(n + 1) * HEAD_DIM] = out_t[:, n * BQ:(n + 1) * BQ].T.astype(BF16)


def attn_forward(qkv, kv_local):
    seq = qkv.shape[0]
    nq = seq // BQ
    wide = REP * HEAD_DIM
    first_k = kv_local * REP
    flops = 2 * 2 * kv_local * REP * seq * seq // 2 * HEAD_DIM * 2
    return pl.pallas_call(
        fwd_kernel,
        grid=(kv_local, nq),
        in_specs=[
            pl.BlockSpec((BQ, wide), lambda t, i: (i, t)),
            pl.BlockSpec((seq, HEAD_DIM), lambda t, i: (0, first_k + t)),
            pl.BlockSpec((seq, HEAD_DIM), lambda t, i: (0, first_k + kv_local + t)),
        ],
        out_specs=(
            pl.BlockSpec((BQ, wide), lambda t, i: (i, t)),
            pl.BlockSpec((1, 1, HEAD_DIM, REP * BQ), lambda t, i: (t, i, 0, 0)),
            pl.BlockSpec((1, 1, 1, REP * BQ), lambda t, i: (t, i, 0, 0)),
        ),
        out_shape=(
            jax.ShapeDtypeStruct((seq, kv_local * wide), BF16),
            jax.ShapeDtypeStruct((kv_local, nq, HEAD_DIM, REP * BQ), F32),
            jax.ShapeDtypeStruct((kv_local, nq, 1, REP * BQ), F32),
        ),
        scratch_shapes=[
            pltpu.VMEM((HEAD_DIM, REP * BQ), BF16),
            pltpu.VMEM((seq // BK, HEAD_DIM, BK), BF16),
            pltpu.VMEM((HEAD_DIM, REP * BQ), F32),
            pltpu.VMEM((8, REP * BQ), F32),
        ],
        compiler_params=pltpu.CompilerParams(dimension_semantics=("arbitrary", "arbitrary"), vmem_limit_bytes=VMEM_BYTES),
        cost_estimate=cost(flops, 4 * seq * wide * kv_local * 2),
        name="attn_fwd",
    )(qkv, qkv, qkv)


def bwd_kernel(q_ref, k_ref, v_ref, do_ref, ot_ref, lse_ref, cos_ref, sin_ref, out_ref,
               qs_sc, qt_sc, ds_sc, dt_sc, kt_sc, dk_sc, dv_sc, dq_sc, row_sc):
    blk = pl.program_id(0)
    wide = REP * HEAD_DIM
    n_chunks = k_ref.shape[0] // BK

    @pl.when(blk == 0)
    def _():
        def one(j, _):
            rows = pl.ds(j * BK, BK)
            kt_sc[j] = flip(k_ref[rows, :])
            dk_sc[rows, :] = jnp.zeros((BK, HEAD_DIM), F32)
            dv_sc[rows, :] = jnp.zeros((BK, HEAD_DIM), F32)
            return 0

        lax.fori_loop(0, n_chunks, one, 0)

    q_all = stack_heads(q_ref[...])
    do_all = stack_heads(do_ref[...])
    qs_sc[...] = q_all
    qt_sc[...] = flip(q_all)
    ds_sc[...] = do_all
    do_t = do_all.astype(F32).T
    dt_sc[...] = do_t.astype(BF16)
    row_sc[0:1, :] = lse_ref[0, 0]
    row_sc[1:2, :] = jnp.sum(ot_ref[0, 0] * do_t, axis=0, keepdims=True)
    dq_sc[...] = jnp.zeros_like(dq_sc)

    def chunk(j, masked):
        rows = pl.ds(j * BK, BK)
        s = mm(k_ref[rows, :], qt_sc[...], ((1,), (0,))) * (SCALE * LOG2E)
        p = jnp.exp2(s - row_sc[0:1, :])
        if masked:
            p = jnp.where(causal(blk * BQ, j * BK, s.shape), p, 0.0)
        dp = mm(v_ref[rows, :], dt_sc[...], ((1,), (0,)))
        dv_sc[rows, :] += mm(p.astype(BF16), ds_sc[...], ((1,), (0,)))
        d_s = (p * (dp - row_sc[1:2, :]) * SCALE).astype(BF16)
        dk_sc[rows, :] += mm(d_s, qs_sc[...], ((1,), (0,)))
        dq_sc[...] += mm(kt_sc[j], d_s, ((1,), (0,)))

    n_full = (blk * BQ) // BK

    def body(j, _):
        chunk(j, False)
        return 0

    lax.fori_loop(0, n_full, body, 0)
    chunk(n_full, True)

    rows = pl.ds(blk * BQ, BQ)
    cos_t = cos_ref[rows, :]
    sin_t = -sin_ref[rows, :]
    for n in range(REP):
        dq = dq_sc[:, n * BQ:(n + 1) * BQ].T.astype(BF16).astype(F32)
        out_ref[rows, n * HEAD_DIM:(n + 1) * HEAD_DIM] = rotate(dq, cos_t, sin_t).astype(BF16)

    @pl.when(blk == pl.num_programs(0) - 1)
    def _():
        def one(j, _):
            kr = pl.ds(j * BK, BK)
            dk = dk_sc[kr, :].astype(BF16).astype(F32)
            out_ref[kr, wide:wide + HEAD_DIM] = rotate(dk, cos_ref[kr, :], -sin_ref[kr, :]).astype(BF16)
            out_ref[kr, wide + HEAD_DIM:wide + 2 * HEAD_DIM] = dv_sc[kr, :].astype(BF16)
            return 0

        lax.fori_loop(0, n_chunks, one, 0)


def attn_backward(qkv, d_o, o_t, lse, cos_t, sin_t, kv_local, t):
    seq = qkv.shape[0]
    nq = seq // BQ
    wide = REP * HEAD_DIM
    first_k = kv_local * REP
    flops = 5 * 2 * REP * seq * seq // 2 * HEAD_DIM * 2
    whole = lambda i: (0, 0)
    return pl.pallas_call(
        bwd_kernel,
        grid=(nq,),
        in_specs=[
            pl.BlockSpec((BQ, wide), lambda i: (i, t)),
            pl.BlockSpec((seq, HEAD_DIM), lambda i: (0, first_k + t)),
            pl.BlockSpec((seq, HEAD_DIM), lambda i: (0, first_k + kv_local + t)),
            pl.BlockSpec((BQ, wide), lambda i: (i, t)),
            pl.BlockSpec((1, 1, HEAD_DIM, REP * BQ), lambda i: (t, i, 0, 0)),
            pl.BlockSpec((1, 1, 1, REP * BQ), lambda i: (t, i, 0, 0)),
            pl.BlockSpec((seq, HEAD_DIM), whole),
            pl.BlockSpec((seq, HEAD_DIM), whole),
        ],
        out_specs=pl.BlockSpec((seq, wide + 2 * HEAD_DIM), whole),
        out_shape=jax.ShapeDtypeStruct((seq, wide + 2 * HEAD_DIM), BF16),
        scratch_shapes=[
            pltpu.VMEM((REP * BQ, HEAD_DIM), BF16),
            pltpu.VMEM((HEAD_DIM, REP * BQ), BF16),
            pltpu.VMEM((REP * BQ, HEAD_DIM), BF16),
            pltpu.VMEM((HEAD_DIM, REP * BQ), BF16),
            pltpu.VMEM((seq // BK, HEAD_DIM, BK), BF16),
            pltpu.VMEM((seq, HEAD_DIM), F32),
            pltpu.VMEM((seq, HEAD_DIM), F32),
            pltpu.VMEM((HEAD_DIM, REP * BQ), F32),
            pltpu.VMEM((8, REP * BQ), F32),
        ],
        compiler_params=pltpu.CompilerParams(dimension_semantics=("arbitrary",), vmem_limit_bytes=VMEM_BYTES),
        cost_estimate=cost(flops, 8 * seq * wide * 2),
        name="attn_bwd",
    )(qkv, qkv, qkv, d_o, o_t, lse, cos_t, sin_t)


def ln_bwd_kernel(dh0_ref, dh1_ref, x_ref, lnw_ref, dx_ref, dw_ref):
    @pl.when(pl.program_id(0) == 0)
    def _():
        dw_ref[...] = jnp.zeros_like(dw_ref)

    xf = x_ref[...].astype(F32)
    mean = jnp.mean(xf, axis=-1, keepdims=True)
    cen = xf - mean
    var = jnp.mean(cen * cen, axis=-1, keepdims=True)
    rstd = lax.rsqrt(var + LN_EPS)
    xhat = cen * rstd
    dh = dh0_ref[...] + dh1_ref[...]
    dw_ref[...] += jnp.sum(dh * xhat, axis=0, keepdims=True)
    dxh = dh * lnw_ref[...].astype(F32)
    mean_d = jnp.mean(dxh, axis=-1, keepdims=True)
    mean_dx = jnp.mean(dxh * xhat, axis=-1, keepdims=True)
    dx_ref[...] = (rstd * (dxh - mean_d - xhat * mean_dx)).astype(BF16)


def ln_backward(dh0, dh1, x, ln_w):
    rows, dim = x.shape
    blk = 128
    row = lambda i: (i, 0)
    const = lambda i: (0, 0)
    return pl.pallas_call(
        ln_bwd_kernel,
        grid=(rows // blk,),
        in_specs=[pl.BlockSpec((blk, dim), row), pl.BlockSpec((blk, dim), row),
                  pl.BlockSpec((blk, dim), row), pl.BlockSpec((1, dim), const)],
        out_specs=(pl.BlockSpec((blk, dim), row), pl.BlockSpec((1, dim), const)),
        out_shape=(jax.ShapeDtypeStruct((rows, dim), BF16), jax.ShapeDtypeStruct((1, dim), F32)),
        compiler_params=pltpu.CompilerParams(dimension_semantics=("arbitrary",), vmem_limit_bytes=VMEM_BYTES),
        cost_estimate=cost(20 * rows * dim, 12 * rows * dim),
        name="ln_bwd",
    )(dh0, dh1, x, ln_w)


def solution(mesh):
    n_dev = mesh.shape['sp']
    row_spec = P(('dp', 'sp'), None)
    pos_spec = P(('dp', 'sp'))
    full_spec = P(None, None)
    grad_spec = P('dp', None)

    def over_chip(val):
        return lax.ppermute(val, 'sp', [(i, i ^ 2) for i in range(n_dev)])

    def over_core(val):
        return lax.ppermute(val, 'sp', [(i, i ^ 1) for i in range(n_dev)])

    def layer(hidden, positions, d_attn, ln_weight, w_q, w_k, w_v, w_o):
        rows, dim = hidden.shape
        seq = rows * n_dev
        kv_local = w_k.shape[1] // HEAD_DIM // n_dev
        wide = REP * HEAD_DIM
        cq = w_q.shape[1] // n_dev
        ck = w_k.shape[1] // n_dev
        me = lax.axis_index('sp')
        chip, core = me // 2, me % 2
        hb = 2 * core + chip
        hbs = [hb, hb ^ 1, hb ^ 2, hb ^ 3]
        toks = [me, me ^ 2, me ^ 1, me ^ 3]

        x_par = over_chip(hidden)
        g_par = over_chip(d_attn)
        x_sib = over_core(hidden)
        g_sib = over_core(d_attn)
        pos = lax.all_gather(positions, 'sp', tiled=True)

        inv_freq = ROPE_BASE ** (-jnp.arange(0, HEAD_DIM, 2, dtype=F32) / HEAD_DIM)
        angles = pos.astype(F32)[:, None] * jnp.repeat(inv_freq, 2)[None, :]
        cos_t = jnp.cos(angles)
        sin_t = jnp.sin(angles) * jnp.where(jnp.arange(HEAD_DIM) % 2 == 0, -1.0, 1.0)[None, :]
        ln_row = ln_weight.reshape(1, dim)

        x_sp = over_core(x_par)
        g_sp = over_core(g_par)

        hq = None
        for tok, x in ((toks[0], hidden), (toks[2], x_sib), (toks[1], x_par), (toks[3], x_sp)):
            idx = jnp.stack([hb, tok]).astype(jnp.int32)
            hq = qkv_block(idx, x, ln_row, w_q, w_k, w_v, cos_t, sin_t, seq, n_dev, hq)
        h_all, qkv = hq
        o_own, o_t, lse = attn_forward(qkv, kv_local)

        gd = None
        for tok, g in ((toks[0], d_attn), (toks[2], g_sib), (toks[1], g_par), (toks[3], g_sp)):
            idx = jnp.stack([hb, tok]).astype(jnp.int32)
            gd = do_block(idx, g, w_o, seq, n_dev, gd)
        g_all, d_o = gd

        def own_rows(val, dev):
            return lax.dynamic_slice_in_dim(val, dev * rows, rows, 0)

        o_par = over_chip(o_own)
        o_tok = [own_rows(o_own, me), own_rows(o_par, me),
                 over_core(own_rows(o_own, me ^ 1)), over_core(own_rows(o_par, me ^ 1))]
        wo_perm = jnp.concatenate([lax.dynamic_slice_in_dim(w_o, b * cq, cq, 0) for b in hbs], axis=0)
        attn_out = jnp.dot(jnp.concatenate(o_tok, axis=1), wo_perm, preferred_element_type=F32).astype(BF16)

        def token_dot(lhs, rhs):
            return mm(lhs, rhs, ((0,), (0,))).astype(BF16)

        dwo_own = token_dot(o_own, g_all)
        dwo_par = token_dot(o_par, g_all)
        d_w_o = jnp.zeros(w_o.shape, BF16)
        for b, piece in zip(hbs, (dwo_own, dwo_par, over_core(dwo_own), over_core(dwo_par))):
            d_w_o = lax.dynamic_update_slice_in_dim(d_w_o, piece, b * cq, 0)

        d_w_q = jnp.zeros(w_q.shape, BF16)
        d_w_k = jnp.zeros(w_k.shape, BF16)
        d_w_v = jnp.zeros(w_v.shape, BF16)
        dhs = []
        for t in range(kv_local):
            gr_own = attn_backward(qkv, d_o, o_t, lse, cos_t, sin_t, kv_local, t)
            gr_par = over_chip(gr_own)
            gr_tok = [own_rows(gr_own, me), own_rows(gr_par, me),
                      over_core(own_rows(gr_own, me ^ 1)), over_core(own_rows(gr_par, me ^ 1))]
            parts = []
            for b in hbs:
                parts.append(lax.dynamic_slice_in_dim(w_q, b * cq + t * wide, wide, 1))
                parts.append(lax.dynamic_slice_in_dim(w_k, b * ck + t * HEAD_DIM, HEAD_DIM, 1))
                parts.append(lax.dynamic_slice_in_dim(w_v, b * ck + t * HEAD_DIM, HEAD_DIM, 1))
            w_perm = jnp.concatenate(parts, axis=1)
            dhs.append(mm(jnp.concatenate(gr_tok, axis=1), w_perm, ((1,), (1,))))
            dw_own = token_dot(h_all, gr_own)
            dw_par = token_dot(h_all, gr_par)
            for b, piece in zip(hbs, (dw_own, dw_par, over_core(dw_own), over_core(dw_par))):
                d_w_q = lax.dynamic_update_slice_in_dim(d_w_q, piece[:, :wide], b * cq + t * wide, 1)
                d_w_k = lax.dynamic_update_slice_in_dim(d_w_k, piece[:, wide:wide + HEAD_DIM], b * ck + t * HEAD_DIM, 1)
                d_w_v = lax.dynamic_update_slice_in_dim(d_w_v, piece[:, wide + HEAD_DIM:], b * ck + t * HEAD_DIM, 1)

        d_hid, d_lnw = ln_backward(dhs[0], dhs[1], hidden, ln_row)
        d_lnw = d_lnw + over_core(d_lnw)
        d_lnw = d_lnw + over_chip(d_lnw)
        return (attn_out, d_hid, d_lnw.reshape(dim).astype(BF16), d_w_q, d_w_k, d_w_v, d_w_o)

    return jax.shard_map(layer, mesh=mesh,
                         in_specs=(row_spec, pos_spec, row_spec, P(None), full_spec, full_spec, full_spec, full_spec),
                         out_specs=(row_spec, row_spec, P('dp'), grad_spec, grad_spec, grad_spec, grad_spec),
                         check_vma=False)
```

```python
import math
import jax
import jax.numpy as jnp
from jax import lax
from jax.experimental import pallas as pl
from jax.experimental.pallas import tpu as pltpu
from jax.sharding import PartitionSpec as P

HEAD_DIM = 128
LN_EPS = 1e-5
ROPE_BASE = 10000.0
REP = 3
BQ = 256
BK = 256
ROWS = 512
LOG2E = math.log2(math.e)
SCALE = HEAD_DIM ** -0.5
VMEM_BYTES = 60 * 1024 * 1024
F32 = jnp.float32
BF16 = jnp.bfloat16


def cost(flops, nbytes):
    return pl.CostEstimate(flops=int(flops), bytes_accessed=int(nbytes), transcendentals=0)


def mm(lhs, rhs, dims):
    return lax.dot_general(lhs, rhs, (dims, ((), ())), preferred_element_type=F32)


def rotate(val, cos_t, sin_t):
    lane = lax.broadcasted_iota(jnp.int32, val.shape, 1)
    swapped = jnp.where(lane % 2 == 0, pltpu.roll(val, HEAD_DIM - 1, 1), pltpu.roll(val, 1, 1))
    return val * cos_t + swapped * sin_t


def ln_kernel(x_ref, lnw_ref, h_ref):
    xf = x_ref[...].astype(F32)
    mean = jnp.mean(xf, axis=-1, keepdims=True)
    cen = xf - mean
    var = jnp.mean(cen * cen, axis=-1, keepdims=True)
    h_ref[...] = (cen * lax.rsqrt(var + LN_EPS) * lnw_ref[...].astype(F32)).astype(BF16)


def ln_forward(x, ln_w):
    rows, dim = x.shape
    blk = 128
    return pl.pallas_call(
        ln_kernel,
        grid=(rows // blk,),
        in_specs=[pl.BlockSpec((blk, dim), lambda i: (i, 0)), pl.BlockSpec((1, dim), lambda i: (0, 0))],
        out_specs=pl.BlockSpec((blk, dim), lambda i: (i, 0)),
        out_shape=jax.ShapeDtypeStruct((rows, dim), BF16),
        compiler_params=pltpu.CompilerParams(dimension_semantics=("arbitrary",)),
        cost_estimate=cost(10 * rows * dim, 4 * rows * dim),
        name="ln_fwd",
    )(x, ln_w)


def qkv_kernel(idx, h_ref, wq_ref, wk_ref, wv_ref, cos_ref, sin_ref, *rest):
    hall_ref, qkv_ref = rest[-2:]
    h = h_ref[...]
    hall_ref[...] = h
    cos_t = cos_ref[...]
    sin_t = sin_ref[...]
    nq = wq_ref.shape[1]
    nk = wk_ref.shape[1]
    step = 2 * HEAD_DIM
    for start in range(0, nq + nk, step):
        w = wq_ref[:, start:start + step] if start < nq else wk_ref[:, start - nq:start - nq + step]
        val = mm(h, w, ((1,), (0,)))
        for n in range(2):
            sl = slice(n * HEAD_DIM, (n + 1) * HEAD_DIM)
            qkv_ref[:, start + n * HEAD_DIM:start + (n + 1) * HEAD_DIM] = rotate(val[:, sl], cos_t, sin_t).astype(BF16)
    qkv_ref[:, nq + nk:] = mm(h, wv_ref[...], ((1,), (0,))).astype(BF16)


def qkv_block(idx, h, w_q, w_k, w_v, cos_t, sin_t, seq, n_dev, prev):
    rows, dim = h.shape
    cq, ck = w_q.shape[1] // n_dev, w_k.shape[1] // n_dev
    per = rows // ROWS
    head = lambda i, ix: (0, ix[0])
    here = lambda i, ix: (ix[1] * per + i, 0)
    in_specs = [
        pl.BlockSpec((ROWS, dim), lambda i, ix: (i, 0)),
        pl.BlockSpec((dim, cq), head),
        pl.BlockSpec((dim, ck), head),
        pl.BlockSpec((dim, ck), head),
        pl.BlockSpec((ROWS, HEAD_DIM), here),
        pl.BlockSpec((ROWS, HEAD_DIM), here),
    ]
    args = [idx, h, w_q, w_k, w_v, cos_t, sin_t]
    aliases = {}
    if prev is not None:
        in_specs += [pl.BlockSpec(memory_space=pl.ANY)] * 2
        args += list(prev)
        aliases = {7: 0, 8: 1}
    cols = cq + 2 * ck
    return pl.pallas_call(
        qkv_kernel,
        out_shape=(jax.ShapeDtypeStruct((seq, dim), BF16), jax.ShapeDtypeStruct((seq, cols), BF16)),
        grid_spec=pltpu.PrefetchScalarGridSpec(
            num_scalar_prefetch=1, grid=(per,), in_specs=in_specs,
            out_specs=(pl.BlockSpec((ROWS, dim), here), pl.BlockSpec((ROWS, cols), here))),
        input_output_aliases=aliases,
        compiler_params=pltpu.CompilerParams(dimension_semantics=("arbitrary",), vmem_limit_bytes=VMEM_BYTES),
        cost_estimate=cost(2 * rows * dim * cols, 2 * (2 * rows * dim + dim * cols + rows * cols)),
        name="qkv",
    )(*args)


def do_kernel(idx, g_ref, wo_ref, *rest):
    gall_ref, do_ref = rest[-2:]
    g = g_ref[...]
    gall_ref[...] = g
    do_ref[...] = mm(g, wo_ref[...], ((1,), (1,))).astype(BF16)


def do_block(idx, g, w_o, seq, n_dev, prev):
    rows, dim = g.shape
    ce = w_o.shape[0] // n_dev
    per = rows // ROWS
    here = lambda i, ix: (ix[1] * per + i, 0)
    in_specs = [
        pl.BlockSpec((ROWS, dim), lambda i, ix: (i, 0)),
        pl.BlockSpec((ce, dim), lambda i, ix: (ix[0], 0)),
    ]
    args = [idx, g, w_o]
    aliases = {}
    if prev is not None:
        in_specs += [pl.BlockSpec(memory_space=pl.ANY)] * 2
        args += list(prev)
        aliases = {3: 0, 4: 1}
    return pl.pallas_call(
        do_kernel,
        out_shape=(jax.ShapeDtypeStruct((seq, dim), BF16), jax.ShapeDtypeStruct((seq, ce), BF16)),
        grid_spec=pltpu.PrefetchScalarGridSpec(
            num_scalar_prefetch=1, grid=(per,), in_specs=in_specs,
            out_specs=(pl.BlockSpec((ROWS, dim), here), pl.BlockSpec((ROWS, ce), here))),
        input_output_aliases=aliases,
        compiler_params=pltpu.CompilerParams(dimension_semantics=("arbitrary",), vmem_limit_bytes=VMEM_BYTES),
        cost_estimate=cost(2 * rows * dim * ce, 2 * (2 * rows * dim + dim * ce + rows * ce)),
        name="d_o",
    )(*args)


def stack_heads(val):
    return jnp.concatenate([val[:, n * HEAD_DIM:(n + 1) * HEAD_DIM] for n in range(REP)], axis=0)


def flip(val):
    return val.astype(F32).T.astype(BF16)


def causal(shape):
    return lax.broadcasted_iota(jnp.int32, shape, 0) <= lax.broadcasted_iota(jnp.int32, shape, 1) % BQ


def fwd_kernel(q_ref, k_ref, v_ref, o_ref, ot_ref, lse_ref, qt_sc, vt_sc, acc_sc, ml_sc):
    blk = pl.program_id(1)
    width = REP * BQ
    n_chunks = k_ref.shape[0] // BK

    @pl.when(blk == 0)
    def _():
        def one(j, _):
            vt_sc[j] = flip(v_ref[pl.ds(j * BK, BK), :])
            return 0

        lax.fori_loop(0, n_chunks, one, 0)

    qt_sc[...] = flip(stack_heads(q_ref[...]))
    acc_sc[...] = jnp.zeros_like(acc_sc)
    ml_sc[0:1, :] = jnp.full((1, width), -jnp.inf, F32)
    ml_sc[1:2, :] = jnp.zeros((1, width), F32)

    def chunks(js, masked):
        scores = [mm(k_ref[pl.ds(j * BK, BK), :], qt_sc[...], ((1,), (0,))) * (SCALE * LOG2E) for j in js]
        if masked:
            scores[-1] = jnp.where(causal(scores[-1].shape), scores[-1], -jnp.inf)
        m = ml_sc[0:1, :]
        total = ml_sc[1:2, :]
        acc = acc_sc[...]
        for j, s in zip(js, scores):
            m_new = jnp.maximum(m, jnp.max(s, axis=0, keepdims=True))
            alpha = jnp.exp2(m - m_new)
            p = jnp.exp2(s - m_new)
            total = total * alpha + jnp.sum(p, axis=0, keepdims=True)
            acc = acc * alpha + mm(vt_sc[j], p.astype(BF16), ((1,), (0,)))
            m = m_new
        ml_sc[0:1, :] = m
        ml_sc[1:2, :] = total
        acc_sc[...] = acc

    def body(j, _):
        chunks((2 * j, 2 * j + 1), False)
        return 0

    lax.fori_loop(0, blk // 2, body, 0)

    @pl.when(blk % 2 == 1)
    def _():
        chunks((blk - 1, blk), True)

    @pl.when(blk % 2 == 0)
    def _():
        chunks((blk,), True)

    total = ml_sc[1:2, :]
    out_t = acc_sc[...] / total
    ot_ref[0, 0] = out_t
    lse_ref[0, 0] = ml_sc[0:1, :] + jnp.log2(total)
    for n in range(REP):
        o_ref[:, n * HEAD_DIM:(n + 1) * HEAD_DIM] = out_t[:, n * BQ:(n + 1) * BQ].T.astype(BF16)


def attn_forward(qkv, kv_local):
    seq = qkv.shape[0]
    nq = seq // BQ
    wide = REP * HEAD_DIM
    first_k = kv_local * REP
    flops = 2 * 2 * kv_local * REP * seq * seq // 2 * HEAD_DIM * 2
    return pl.pallas_call(
        fwd_kernel,
        grid=(kv_local, nq),
        in_specs=[
            pl.BlockSpec((BQ, wide), lambda t, i: (i, t)),
            pl.BlockSpec((seq, HEAD_DIM), lambda t, i: (0, first_k + t)),
            pl.BlockSpec((seq, HEAD_DIM), lambda t, i: (0, first_k + kv_local + t)),
        ],
        out_specs=(
            pl.BlockSpec((BQ, wide), lambda t, i: (i, t)),
            pl.BlockSpec((1, 1, HEAD_DIM, REP * BQ), lambda t, i: (t, i, 0, 0)),
            pl.BlockSpec((1, 1, 1, REP * BQ), lambda t, i: (t, i, 0, 0)),
        ),
        out_shape=(
            jax.ShapeDtypeStruct((seq, kv_local * wide), BF16),
            jax.ShapeDtypeStruct((kv_local, nq, HEAD_DIM, REP * BQ), F32),
            jax.ShapeDtypeStruct((kv_local, nq, 1, REP * BQ), F32),
        ),
        scratch_shapes=[
            pltpu.VMEM((HEAD_DIM, REP * BQ), BF16),
            pltpu.VMEM((seq // BK, HEAD_DIM, BK), BF16),
            pltpu.VMEM((HEAD_DIM, REP * BQ), F32),
            pltpu.VMEM((8, REP * BQ), F32),
        ],
        compiler_params=pltpu.CompilerParams(dimension_semantics=("arbitrary", "arbitrary"), vmem_limit_bytes=VMEM_BYTES),
        cost_estimate=cost(flops, 4 * seq * wide * kv_local * 2),
        name="attn_fwd",
    )(qkv, qkv, qkv)


def bwd_kernel(q_ref, k_ref, v_ref, do_ref, ot_ref, lse_ref, cos_ref, sin_ref, out_ref,
               qs_sc, qt_sc, ds_sc, dt_sc, kt_sc, dk_sc, dv_sc, dq_sc, row_sc):
    blk = pl.program_id(0)
    wide = REP * HEAD_DIM
    n_chunks = k_ref.shape[0] // BK

    @pl.when(blk == 0)
    def _():
        def one(j, _):
            rows = pl.ds(j * BK, BK)
            kt_sc[j] = flip(k_ref[rows, :])
            dk_sc[rows, :] = jnp.zeros((BK, HEAD_DIM), F32)
            dv_sc[rows, :] = jnp.zeros((BK, HEAD_DIM), F32)
            return 0

        lax.fori_loop(0, n_chunks, one, 0)

    q_all = stack_heads(q_ref[...])
    do_all = stack_heads(do_ref[...])
    qs_sc[...] = q_all
    qt_sc[...] = flip(q_all)
    ds_sc[...] = do_all
    do_t = do_all.astype(F32).T
    dt_sc[...] = do_t.astype(BF16)
    row_sc[0:1, :] = lse_ref[0, 0]
    row_sc[1:2, :] = jnp.sum(ot_ref[0, 0] * do_t, axis=0, keepdims=True)
    dq_sc[...] = jnp.zeros_like(dq_sc)

    def chunks(js, masked):
        rows = [pl.ds(j * BK, BK) for j in js]
        scores = [mm(k_ref[r, :], qt_sc[...], ((1,), (0,))) * (SCALE * LOG2E) for r in rows]
        dps = [mm(v_ref[r, :], dt_sc[...], ((1,), (0,))) for r in rows]
        dq = dq_sc[...]
        for n, (j, r) in enumerate(zip(js, rows)):
            p = jnp.exp2(scores[n] - row_sc[0:1, :])
            if masked and n == len(js) - 1:
                p = jnp.where(causal(p.shape), p, 0.0)
            dv_sc[r, :] += mm(p.astype(BF16), ds_sc[...], ((1,), (0,)))
            d_s = (p * (dps[n] - row_sc[1:2, :]) * SCALE).astype(BF16)
            dk_sc[r, :] += mm(d_s, qs_sc[...], ((1,), (0,)))
            dq = dq + mm(kt_sc[j], d_s, ((1,), (0,)))
        dq_sc[...] = dq

    def body(j, _):
        chunks((2 * j, 2 * j + 1), False)
        return 0

    lax.fori_loop(0, blk // 2, body, 0)

    @pl.when(blk % 2 == 1)
    def _():
        chunks((blk - 1, blk), True)

    @pl.when(blk % 2 == 0)
    def _():
        chunks((blk,), True)

    rows = pl.ds(blk * BQ, BQ)
    cos_t = cos_ref[rows, :]
    sin_t = -sin_ref[rows, :]
    for n in range(REP):
        dq = dq_sc[:, n * BQ:(n + 1) * BQ].T.astype(BF16).astype(F32)
        out_ref[rows, n * HEAD_DIM:(n + 1) * HEAD_DIM] = rotate(dq, cos_t, sin_t).astype(BF16)

    @pl.when(blk == pl.num_programs(0) - 1)
    def _():
        def one(j, _):
            kr = pl.ds(j * BK, BK)
            dk = dk_sc[kr, :].astype(BF16).astype(F32)
            out_ref[kr, wide:wide + HEAD_DIM] = rotate(dk, cos_ref[kr, :], -sin_ref[kr, :]).astype(BF16)
            out_ref[kr, wide + HEAD_DIM:wide + 2 * HEAD_DIM] = dv_sc[kr, :].astype(BF16)
            return 0

        lax.fori_loop(0, n_chunks, one, 0)


def attn_backward(qkv, d_o, o_t, lse, cos_t, sin_t, kv_local, t):
    seq = qkv.shape[0]
    nq = seq // BQ
    wide = REP * HEAD_DIM
    first_k = kv_local * REP
    flops = 5 * 2 * REP * seq * seq // 2 * HEAD_DIM * 2
    whole = lambda i: (0, 0)
    return pl.pallas_call(
        bwd_kernel,
        grid=(nq,),
        in_specs=[
            pl.BlockSpec((BQ, wide), lambda i: (i, t)),
            pl.BlockSpec((seq, HEAD_DIM), lambda i: (0, first_k + t)),
            pl.BlockSpec((seq, HEAD_DIM), lambda i: (0, first_k + kv_local + t)),
            pl.BlockSpec((BQ, wide), lambda i: (i, t)),
            pl.BlockSpec((1, 1, HEAD_DIM, REP * BQ), lambda i: (t, i, 0, 0)),
            pl.BlockSpec((1, 1, 1, REP * BQ), lambda i: (t, i, 0, 0)),
            pl.BlockSpec((seq, HEAD_DIM), whole),
            pl.BlockSpec((seq, HEAD_DIM), whole),
        ],
        out_specs=pl.BlockSpec((seq, wide + 2 * HEAD_DIM), whole),
        out_shape=jax.ShapeDtypeStruct((seq, wide + 2 * HEAD_DIM), BF16),
        scratch_shapes=[
            pltpu.VMEM((REP * BQ, HEAD_DIM), BF16),
            pltpu.VMEM((HEAD_DIM, REP * BQ), BF16),
            pltpu.VMEM((REP * BQ, HEAD_DIM), BF16),
            pltpu.VMEM((HEAD_DIM, REP * BQ), BF16),
            pltpu.VMEM((seq // BK, HEAD_DIM, BK), BF16),
            pltpu.VMEM((seq, HEAD_DIM), F32),
            pltpu.VMEM((seq, HEAD_DIM), F32),
            pltpu.VMEM((HEAD_DIM, REP * BQ), F32),
            pltpu.VMEM((8, REP * BQ), F32),
        ],
        compiler_params=pltpu.CompilerParams(dimension_semantics=("arbitrary",), vmem_limit_bytes=VMEM_BYTES),
        cost_estimate=cost(flops, 8 * seq * wide * 2),
        name="attn_bwd",
    )(qkv, qkv, qkv, d_o, o_t, lse, cos_t, sin_t)


def ln_bwd_kernel(dh0_ref, dh1_ref, x_ref, lnw_ref, dx_ref, dw_ref):
    @pl.when(pl.program_id(0) == 0)
    def _():
        dw_ref[...] = jnp.zeros_like(dw_ref)

    xf = x_ref[...].astype(F32)
    mean = jnp.mean(xf, axis=-1, keepdims=True)
    cen = xf - mean
    var = jnp.mean(cen * cen, axis=-1, keepdims=True)
    rstd = lax.rsqrt(var + LN_EPS)
    xhat = cen * rstd
    dh = dh0_ref[...] + dh1_ref[...]
    dw_ref[...] += jnp.sum(dh * xhat, axis=0, keepdims=True)
    dxh = dh * lnw_ref[...].astype(F32)
    mean_d = jnp.mean(dxh, axis=-1, keepdims=True)
    mean_dx = jnp.mean(dxh * xhat, axis=-1, keepdims=True)
    dx_ref[...] = (rstd * (dxh - mean_d - xhat * mean_dx)).astype(BF16)


def ln_backward(dh0, dh1, x, ln_w):
    rows, dim = x.shape
    blk = 128
    row = lambda i: (i, 0)
    const = lambda i: (0, 0)
    return pl.pallas_call(
        ln_bwd_kernel,
        grid=(rows // blk,),
        in_specs=[pl.BlockSpec((blk, dim), row), pl.BlockSpec((blk, dim), row),
                  pl.BlockSpec((blk, dim), row), pl.BlockSpec((1, dim), const)],
        out_specs=(pl.BlockSpec((blk, dim), row), pl.BlockSpec((1, dim), const)),
        out_shape=(jax.ShapeDtypeStruct((rows, dim), BF16), jax.ShapeDtypeStruct((1, dim), F32)),
        compiler_params=pltpu.CompilerParams(dimension_semantics=("arbitrary",), vmem_limit_bytes=VMEM_BYTES),
        cost_estimate=cost(20 * rows * dim, 12 * rows * dim),
        name="ln_bwd",
    )(dh0, dh1, x, ln_w)


def reserve(*shapes):
    return pl.pallas_call(
        lambda *refs: None,
        out_shape=tuple(jax.ShapeDtypeStruct(s, BF16) for s in shapes),
        out_specs=tuple(pl.BlockSpec(memory_space=pl.ANY) for _ in shapes),
        cost_estimate=cost(1, 1),
        name="reserve",
    )()


def place_kernel(idx, *refs):
    pieces, outs = refs[:4], refs[-3:]
    wide = outs[0].shape[1]
    for n, piece in enumerate(pieces):
        @pl.when(pl.program_id(0) == n)
        def _():
            outs[0][...] = piece[:, :wide]
            outs[1][...] = piece[:, wide:wide + HEAD_DIM]
            outs[2][...] = piece[:, wide + HEAD_DIM:]


def place(idx, pieces, bufs):
    dim, cols = pieces[0].shape
    wide = cols - 2 * HEAD_DIM
    blk = dim // 4

    def piece_spec(n):
        return pl.BlockSpec((blk, cols), lambda s, i, ix: (jnp.where(s == n, i, jnp.where(s < n, 0, 3)), 0))

    there = lambda s, i, ix: (i, ix[s])
    return pl.pallas_call(
        place_kernel,
        out_shape=tuple(jax.ShapeDtypeStruct(b.shape, BF16) for b in bufs),
        grid_spec=pltpu.PrefetchScalarGridSpec(
            num_scalar_prefetch=1, grid=(4, 4),
            in_specs=[piece_spec(n) for n in range(4)] + [pl.BlockSpec(memory_space=pl.ANY)] * 3,
            out_specs=(pl.BlockSpec((blk, wide), there), pl.BlockSpec((blk, HEAD_DIM), there),
                       pl.BlockSpec((blk, HEAD_DIM), there))),
        input_output_aliases={5: 0, 6: 1, 7: 2},
        compiler_params=pltpu.CompilerParams(dimension_semantics=("arbitrary", "arbitrary"), vmem_limit_bytes=VMEM_BYTES),
        cost_estimate=cost(8 * dim * cols, 16 * dim * cols),
        name="place",
    )(idx, *pieces, *bufs)


def solution(mesh):
    n_dev = mesh.shape['sp']
    row_spec = P(('dp', 'sp'), None)
    pos_spec = P(('dp', 'sp'))
    full_spec = P(None, None)
    grad_spec = P('dp', None)

    def over_chip(val):
        return lax.ppermute(val, 'sp', [(i, i ^ 2) for i in range(n_dev)])

    def over_core(val):
        return lax.ppermute(val, 'sp', [(i, i ^ 1) for i in range(n_dev)])

    def layer(hidden, positions, d_attn, ln_weight, w_q, w_k, w_v, w_o):
        rows, dim = hidden.shape
        seq = rows * n_dev
        kv_local = w_k.shape[1] // HEAD_DIM // n_dev
        wide = REP * HEAD_DIM
        cq = w_q.shape[1] // n_dev
        ck = w_k.shape[1] // n_dev
        me = lax.axis_index('sp')
        chip, core = me // 2, me % 2
        hb = 2 * core + chip
        hbs = [hb, hb ^ 1, hb ^ 2, hb ^ 3]
        toks = [me, me ^ 2, me ^ 1, me ^ 3]

        pos_par = over_chip(positions)
        pos_src = (positions, over_core(positions), pos_par, over_core(pos_par))
        pos = jnp.concatenate([lax.select_n(me ^ b, *pos_src) for b in range(n_dev)])
        ln_row = ln_weight.reshape(1, dim)
        h_own = ln_forward(hidden, ln_row)
        h_par = over_chip(h_own)
        g_par = over_chip(d_attn)
        h_sib = over_core(h_own)
        g_sib = over_core(d_attn)

        inv_freq = ROPE_BASE ** (-jnp.arange(0, HEAD_DIM, 2, dtype=F32) / HEAD_DIM)
        angles = pos.astype(F32)[:, None] * jnp.repeat(inv_freq, 2)[None, :]
        cos_t = jnp.cos(angles)
        sin_t = jnp.sin(angles) * jnp.where(jnp.arange(HEAD_DIM) % 2 == 0, -1.0, 1.0)[None, :]

        h_sp = over_core(h_par)
        g_sp = over_core(g_par)

        hq = None
        for tok, h in ((toks[0], h_own), (toks[2], h_sib), (toks[1], h_par), (toks[3], h_sp)):
            idx = jnp.stack([hb, tok]).astype(jnp.int32)
            hq = qkv_block(idx, h, w_q, w_k, w_v, cos_t, sin_t, seq, n_dev, hq)
        h_all, qkv = hq
        o_own, o_t, lse = attn_forward(qkv, kv_local)

        gd = None
        for tok, g in ((toks[0], d_attn), (toks[2], g_sib), (toks[1], g_par), (toks[3], g_sp)):
            idx = jnp.stack([hb, tok]).astype(jnp.int32)
            gd = do_block(idx, g, w_o, seq, n_dev, gd)
        g_all, d_o = gd

        def own_rows(val, dev):
            return lax.dynamic_slice_in_dim(val, dev * rows, rows, 0)

        o_par = over_chip(o_own)
        o_tok = [own_rows(o_own, me), own_rows(o_par, me),
                 over_core(own_rows(o_own, me ^ 1)), over_core(own_rows(o_par, me ^ 1))]
        wo_perm = jnp.concatenate([lax.dynamic_slice_in_dim(w_o, b * cq, cq, 0) for b in hbs], axis=0)
        attn_out = jnp.dot(jnp.concatenate(o_tok, axis=1), wo_perm, preferred_element_type=F32).astype(BF16)

        def token_dot(lhs, rhs):
            return mm(lhs, rhs, ((0,), (0,))).astype(BF16)

        dwo_own = token_dot(o_own, g_all)
        dwo_par = token_dot(o_par, g_all)
        d_w_o, *d_w = reserve(w_o.shape, w_q.shape, w_k.shape, w_v.shape)
        for b, piece in zip(hbs, (dwo_own, dwo_par, over_core(dwo_own), over_core(dwo_par))):
            d_w_o = lax.dynamic_update_slice_in_dim(d_w_o, piece, b * cq, 0)

        dhs = []
        for t in range(kv_local):
            gr_own = attn_backward(qkv, d_o, o_t, lse, cos_t, sin_t, kv_local, t)
            gr_par = over_chip(gr_own)
            gr_tok = [own_rows(gr_own, me), own_rows(gr_par, me),
                      over_core(own_rows(gr_own, me ^ 1)), over_core(own_rows(gr_par, me ^ 1))]
            parts = []
            for b in hbs:
                parts.append(lax.dynamic_slice_in_dim(w_q, b * cq + t * wide, wide, 1))
                parts.append(lax.dynamic_slice_in_dim(w_k, b * ck + t * HEAD_DIM, HEAD_DIM, 1))
                parts.append(lax.dynamic_slice_in_dim(w_v, b * ck + t * HEAD_DIM, HEAD_DIM, 1))
            w_perm = jnp.concatenate(parts, axis=1)
            dhs.append(mm(jnp.concatenate(gr_tok, axis=1), w_perm, ((1,), (1,))))
            dw_own = token_dot(h_all, gr_own)
            dw_par = token_dot(h_all, gr_par)
            pieces = (dw_own, dw_par, over_core(dw_own), over_core(dw_par))
            d_w = place(jnp.stack([b * kv_local + t for b in hbs]).astype(jnp.int32), pieces, d_w)

        d_hid, d_lnw = ln_backward(dhs[0], dhs[1], hidden, ln_row)
        d_lnw = d_lnw + over_core(d_lnw)
        d_lnw = d_lnw + over_chip(d_lnw)
        return (attn_out, d_hid, d_lnw.reshape(dim).astype(BF16), *d_w, d_w_o)

    return jax.shard_map(layer, mesh=mesh,
                         in_specs=(row_spec, pos_spec, row_spec, P(None), full_spec, full_spec, full_spec, full_spec),
                         out_specs=(row_spec, row_spec, P('dp'), grad_spec, grad_spec, grad_spec, grad_spec),
                         check_vma=False)
```

```python
import functools
import math
import jax
import jax.numpy as jnp
from jax import lax
from jax.experimental import pallas as pl
from jax.experimental.pallas import tpu as pltpu
from jax.sharding import PartitionSpec as P

HEAD_DIM = 128
LN_EPS = 1e-5
ROPE_BASE = 10000.0
REP = 3
BQ = 256
BK = 256
ROWS = 512
LOG2E = math.log2(math.e)
SCALE = HEAD_DIM ** -0.5
VMEM_BYTES = 60 * 1024 * 1024
F32 = jnp.float32
BF16 = jnp.bfloat16


def cost(flops, nbytes):
    return pl.CostEstimate(flops=int(flops), bytes_accessed=int(nbytes), transcendentals=0)


def mm(lhs, rhs, dims):
    return lax.dot_general(lhs, rhs, (dims, ((), ())), preferred_element_type=F32)


def rotate(val, cos_t, sin_t):
    lane = lax.broadcasted_iota(jnp.int32, val.shape, 1)
    swapped = jnp.where(lane % 2 == 0, pltpu.roll(val, HEAD_DIM - 1, 1), pltpu.roll(val, 1, 1))
    return val * cos_t + swapped * sin_t


def ln_kernel(x_ref, lnw_ref, h_ref):
    xf = x_ref[...].astype(F32)
    mean = jnp.mean(xf, axis=-1, keepdims=True)
    cen = xf - mean
    var = jnp.mean(cen * cen, axis=-1, keepdims=True)
    h_ref[...] = (cen * lax.rsqrt(var + LN_EPS) * lnw_ref[...].astype(F32)).astype(BF16)


def ln_forward(x, ln_w):
    rows, dim = x.shape
    blk = 128
    return pl.pallas_call(
        ln_kernel,
        grid=(rows // blk,),
        in_specs=[pl.BlockSpec((blk, dim), lambda i: (i, 0)), pl.BlockSpec((1, dim), lambda i: (0, 0))],
        out_specs=pl.BlockSpec((blk, dim), lambda i: (i, 0)),
        out_shape=jax.ShapeDtypeStruct((rows, dim), BF16),
        compiler_params=pltpu.CompilerParams(dimension_semantics=("arbitrary",)),
        cost_estimate=cost(10 * rows * dim, 4 * rows * dim),
        name="ln_fwd",
    )(x, ln_w)


def qkv_kernel(idx, h_ref, wq_ref, wk_ref, wv_ref, cos_ref, sin_ref, *rest):
    hall_ref, qkv_ref = rest[-2:]
    h = h_ref[...]
    hall_ref[...] = h
    cos_t = cos_ref[...]
    sin_t = sin_ref[...]
    nq = wq_ref.shape[1]
    nk = wk_ref.shape[1]
    step = 2 * HEAD_DIM
    for start in range(0, nq + nk, step):
        w = wq_ref[:, start:start + step] if start < nq else wk_ref[:, start - nq:start - nq + step]
        val = mm(h, w, ((1,), (0,)))
        for n in range(2):
            sl = slice(n * HEAD_DIM, (n + 1) * HEAD_DIM)
            qkv_ref[:, start + n * HEAD_DIM:start + (n + 1) * HEAD_DIM] = rotate(val[:, sl], cos_t, sin_t).astype(BF16)
    qkv_ref[:, nq + nk:] = mm(h, wv_ref[...], ((1,), (0,))).astype(BF16)


def qkv_block(idx, h, w_q, w_k, w_v, cos_t, sin_t, seq, n_dev, prev):
    rows, dim = h.shape
    cq, ck = w_q.shape[1] // n_dev, w_k.shape[1] // n_dev
    per = rows // ROWS
    head = lambda i, ix: (0, ix[0])
    here = lambda i, ix: (ix[1] * per + i, 0)
    in_specs = [
        pl.BlockSpec((ROWS, dim), lambda i, ix: (i, 0)),
        pl.BlockSpec((dim, cq), head),
        pl.BlockSpec((dim, ck), head),
        pl.BlockSpec((dim, ck), head),
        pl.BlockSpec((ROWS, HEAD_DIM), here),
        pl.BlockSpec((ROWS, HEAD_DIM), here),
    ]
    args = [idx, h, w_q, w_k, w_v, cos_t, sin_t]
    aliases = {}
    if prev is not None:
        in_specs += [pl.BlockSpec(memory_space=pl.ANY)] * 2
        args += list(prev)
        aliases = {7: 0, 8: 1}
    cols = cq + 2 * ck
    return pl.pallas_call(
        qkv_kernel,
        out_shape=(jax.ShapeDtypeStruct((seq, dim), BF16), jax.ShapeDtypeStruct((seq, cols), BF16)),
        grid_spec=pltpu.PrefetchScalarGridSpec(
            num_scalar_prefetch=1, grid=(per,), in_specs=in_specs,
            out_specs=(pl.BlockSpec((ROWS, dim), here), pl.BlockSpec((ROWS, cols), here))),
        input_output_aliases=aliases,
        compiler_params=pltpu.CompilerParams(dimension_semantics=("arbitrary",), vmem_limit_bytes=VMEM_BYTES),
        cost_estimate=cost(2 * rows * dim * cols, 2 * (2 * rows * dim + dim * cols + rows * cols)),
        name="qkv",
    )(*args)


def wo_t_kernel(idx, wo_ref, out_ref):
    out_ref[...] = wo_ref[...].astype(F32).T.astype(BF16)


def transpose_rows(idx, w_o, n_dev):
    ce, dim = w_o.shape[0] // n_dev, w_o.shape[1]
    blk = 512
    return pl.pallas_call(
        wo_t_kernel,
        out_shape=jax.ShapeDtypeStruct((dim, ce), BF16),
        grid_spec=pltpu.PrefetchScalarGridSpec(
            num_scalar_prefetch=1, grid=(dim // blk,),
            in_specs=[pl.BlockSpec((ce, blk), lambda i, ix: (ix[0], i))],
            out_specs=pl.BlockSpec((blk, ce), lambda i, ix: (i, 0))),
        compiler_params=pltpu.CompilerParams(dimension_semantics=("arbitrary",)),
        cost_estimate=cost(4 * ce * dim, 4 * ce * dim),
        name="wo_t",
    )(idx, w_o)


def do_kernel(idx, g_ref, wo_ref, *rest):
    gall_ref, do_ref = rest[-2:]
    g = g_ref[...]
    gall_ref[...] = g
    do_ref[...] = mm(g, wo_ref[...], ((1,), (0,))).astype(BF16)


def do_block(idx, g, wo_t, seq, prev):
    rows, dim = g.shape
    ce = wo_t.shape[1]
    per = rows // ROWS
    here = lambda i, ix: (ix[1] * per + i, 0)
    in_specs = [
        pl.BlockSpec((ROWS, dim), lambda i, ix: (i, 0)),
        pl.BlockSpec((dim, ce), lambda i, ix: (0, 0)),
    ]
    args = [idx, g, wo_t]
    aliases = {}
    if prev is not None:
        in_specs += [pl.BlockSpec(memory_space=pl.ANY)] * 2
        args += list(prev)
        aliases = {3: 0, 4: 1}
    return pl.pallas_call(
        do_kernel,
        out_shape=(jax.ShapeDtypeStruct((seq, dim), BF16), jax.ShapeDtypeStruct((seq, ce), BF16)),
        grid_spec=pltpu.PrefetchScalarGridSpec(
            num_scalar_prefetch=1, grid=(per,), in_specs=in_specs,
            out_specs=(pl.BlockSpec((ROWS, dim), here), pl.BlockSpec((ROWS, ce), here))),
        input_output_aliases=aliases,
        compiler_params=pltpu.CompilerParams(dimension_semantics=("arbitrary",), vmem_limit_bytes=VMEM_BYTES),
        cost_estimate=cost(2 * rows * dim * ce, 2 * (2 * rows * dim + dim * ce + rows * ce)),
        name="d_o",
    )(*args)


def stack_heads(val):
    return jnp.concatenate([val[:, n * HEAD_DIM:(n + 1) * HEAD_DIM] for n in range(REP)], axis=0)


def flip(val):
    return val.astype(F32).T.astype(BF16)


def causal(shape):
    return lax.broadcasted_iota(jnp.int32, shape, 0) <= lax.broadcasted_iota(jnp.int32, shape, 1) % BQ


def fwd_kernel(q_ref, k_ref, v_ref, o_ref, ot_ref, lse_ref, qt_sc, vt_sc, acc_sc, ml_sc, s_sc):
    blk = pl.program_id(1)
    n_chunks = k_ref.shape[0] // BK
    pairs = blk // 2

    @pl.when(blk == 0)
    def _():
        def one(j, _):
            vt_sc[j] = flip(v_ref[pl.ds(j * BK, BK), :])
            return 0

        lax.fori_loop(0, n_chunks, one, 0)

    qt_sc[...] = flip(stack_heads(q_ref[...]))

    def score(j):
        return mm(k_ref[pl.ds(j * BK, BK), :], qt_sc[...], ((1,), (0,))) * (SCALE * LOG2E)

    def ahead(pair):
        for n in range(2):
            nxt = score(2 * pair + n)
            s_sc[n] = nxt
            ml_sc[2 + n:3 + n, :] = jnp.max(nxt, axis=0, keepdims=True)

    def update(m_new, js, scores, first):
        if first:
            total, acc = 0.0, 0.0
        else:
            alpha = jnp.exp2(ml_sc[0:1, :] - m_new)
            total, acc = ml_sc[1:2, :] * alpha, acc_sc[...] * alpha
        for j, s in zip(js, scores):
            p = jnp.exp2(s - m_new)
            total = total + jnp.sum(p, axis=0, keepdims=True)
            acc = acc + mm(vt_sc[j], p.astype(BF16), ((1,), (0,)))
        ml_sc[0:1, :] = m_new
        ml_sc[1:2, :] = total
        acc_sc[...] = acc

    def last_chunks(js):
        scores = [score(j) for j in js]
        scores[-1] = jnp.where(causal(scores[-1].shape), scores[-1], -jnp.inf)
        m_new = functools.reduce(jnp.maximum, [jnp.max(s, axis=0, keepdims=True) for s in scores])
        ahead(0)
        update(m_new, js, scores, True)

    def held(pair, more):
        m_new = jnp.maximum(ml_sc[0:1, :], jnp.maximum(ml_sc[2:3, :], ml_sc[3:4, :]))
        scores = [s_sc[n] for n in range(2)]
        if more:
            ahead(pair + 1)
        update(m_new, (2 * pair, 2 * pair + 1), scores, False)

    @pl.when(blk % 2 == 1)
    def _():
        last_chunks((blk - 1, blk))

    @pl.when(blk % 2 == 0)
    def _():
        last_chunks((blk,))

    def body(pair, _):
        held(pair, True)
        return 0

    lax.fori_loop(0, pairs - 1, body, 0)

    @pl.when(pairs > 0)
    def _():
        held(pairs - 1, False)

    total = ml_sc[1:2, :]
    out_t = acc_sc[...] / total
    ot_ref[0, 0] = out_t
    lse_ref[0, 0] = ml_sc[0:1, :] + jnp.log2(total)
    for n in range(REP):
        o_ref[:, n * HEAD_DIM:(n + 1) * HEAD_DIM] = out_t[:, n * BQ:(n + 1) * BQ].T.astype(BF16)


def attn_forward(qkv, kv_local):
    seq = qkv.shape[0]
    nq = seq // BQ
    wide = REP * HEAD_DIM
    first_k = kv_local * REP
    flops = 2 * 2 * kv_local * REP * seq * seq // 2 * HEAD_DIM * 2
    return pl.pallas_call(
        fwd_kernel,
        grid=(kv_local, nq),
        in_specs=[
            pl.BlockSpec((BQ, wide), lambda t, i: (i, t)),
            pl.BlockSpec((seq, HEAD_DIM), lambda t, i: (0, first_k + t)),
            pl.BlockSpec((seq, HEAD_DIM), lambda t, i: (0, first_k + kv_local + t)),
        ],
        out_specs=(
            pl.BlockSpec((BQ, wide), lambda t, i: (i, t)),
            pl.BlockSpec((1, 1, HEAD_DIM, REP * BQ), lambda t, i: (t, i, 0, 0)),
            pl.BlockSpec((1, 1, 1, REP * BQ), lambda t, i: (t, i, 0, 0)),
        ),
        out_shape=(
            jax.ShapeDtypeStruct((seq, kv_local * wide), BF16),
            jax.ShapeDtypeStruct((kv_local, nq, HEAD_DIM, REP * BQ), F32),
            jax.ShapeDtypeStruct((kv_local, nq, 1, REP * BQ), F32),
        ),
        scratch_shapes=[
            pltpu.VMEM((HEAD_DIM, REP * BQ), BF16),
            pltpu.VMEM((seq // BK, HEAD_DIM, BK), BF16),
            pltpu.VMEM((HEAD_DIM, REP * BQ), F32),
            pltpu.VMEM((8, REP * BQ), F32),
            pltpu.VMEM((2, BK, REP * BQ), F32),
        ],
        compiler_params=pltpu.CompilerParams(dimension_semantics=("arbitrary", "arbitrary"), vmem_limit_bytes=VMEM_BYTES),
        cost_estimate=cost(flops, 4 * seq * wide * kv_local * 2),
        name="attn_fwd",
    )(qkv, qkv, qkv)


def bwd_kernel(q_ref, k_ref, v_ref, do_ref, ot_ref, lse_ref, cos_ref, sin_ref, out_ref,
               qs_sc, qt_sc, ds_sc, dt_sc, kt_sc, dk_sc, dv_sc, dq_sc, row_sc):
    blk = pl.program_id(0)
    wide = REP * HEAD_DIM
    n_chunks = k_ref.shape[0] // BK

    @pl.when(blk == 0)
    def _():
        def one(j, _):
            rows = pl.ds(j * BK, BK)
            kt_sc[j] = flip(k_ref[rows, :])
            dk_sc[rows, :] = jnp.zeros((BK, HEAD_DIM), F32)
            dv_sc[rows, :] = jnp.zeros((BK, HEAD_DIM), F32)
            return 0

        lax.fori_loop(0, n_chunks, one, 0)

    q_all = stack_heads(q_ref[...])
    do_all = stack_heads(do_ref[...])
    qs_sc[...] = q_all
    qt_sc[...] = flip(q_all)
    ds_sc[...] = do_all
    do_t = do_all.astype(F32).T
    dt_sc[...] = do_t.astype(BF16)
    row_sc[0:1, :] = lse_ref[0, 0]
    row_sc[1:2, :] = jnp.sum(ot_ref[0, 0] * do_t, axis=0, keepdims=True)
    dq_sc[...] = jnp.zeros_like(dq_sc)

    def chunks(js, masked):
        rows = [pl.ds(j * BK, BK) for j in js]
        scores = [mm(k_ref[r, :], qt_sc[...], ((1,), (0,))) * (SCALE * LOG2E) for r in rows]
        dps = [mm(v_ref[r, :], dt_sc[...], ((1,), (0,))) for r in rows]
        dq = dq_sc[...]
        for n, (j, r) in enumerate(zip(js, rows)):
            p = jnp.exp2(scores[n] - row_sc[0:1, :])
            if masked and n == len(js) - 1:
                p = jnp.where(causal(p.shape), p, 0.0)
            dv_sc[r, :] += mm(p.astype(BF16), ds_sc[...], ((1,), (0,)))
            d_s = (p * (dps[n] - row_sc[1:2, :]) * SCALE).astype(BF16)
            dk_sc[r, :] += mm(d_s, qs_sc[...], ((1,), (0,)))
            dq = dq + mm(kt_sc[j], d_s, ((1,), (0,)))
        dq_sc[...] = dq

    def body(j, _):
        chunks((2 * j, 2 * j + 1), False)
        return 0

    lax.fori_loop(0, blk // 2, body, 0)

    @pl.when(blk % 2 == 1)
    def _():
        chunks((blk - 1, blk), True)

    @pl.when(blk % 2 == 0)
    def _():
        chunks((blk,), True)

    rows = pl.ds(blk * BQ, BQ)
    cos_t = cos_ref[rows, :]
    sin_t = -sin_ref[rows, :]
    for n in range(REP):
        dq = dq_sc[:, n * BQ:(n + 1) * BQ].T.astype(BF16).astype(F32)
        out_ref[rows, n * HEAD_DIM:(n + 1) * HEAD_DIM] = rotate(dq, cos_t, sin_t).astype(BF16)

    @pl.when(blk == pl.num_programs(0) - 1)
    def _():
        def one(j, _):
            kr = pl.ds(j * BK, BK)
            dk = dk_sc[kr, :].astype(BF16).astype(F32)
            out_ref[kr, wide:wide + HEAD_DIM] = rotate(dk, cos_ref[kr, :], -sin_ref[kr, :]).astype(BF16)
            out_ref[kr, wide + HEAD_DIM:wide + 2 * HEAD_DIM] = dv_sc[kr, :].astype(BF16)
            return 0

        lax.fori_loop(0, n_chunks, one, 0)


def attn_backward(qkv, d_o, o_t, lse, cos_t, sin_t, kv_local, t):
    seq = qkv.shape[0]
    nq = seq // BQ
    wide = REP * HEAD_DIM
    first_k = kv_local * REP
    flops = 5 * 2 * REP * seq * seq // 2 * HEAD_DIM * 2
    whole = lambda i: (0, 0)
    return pl.pallas_call(
        bwd_kernel,
        grid=(nq,),
        in_specs=[
            pl.BlockSpec((BQ, wide), lambda i: (i, t)),
            pl.BlockSpec((seq, HEAD_DIM), lambda i: (0, first_k + t)),
            pl.BlockSpec((seq, HEAD_DIM), lambda i: (0, first_k + kv_local + t)),
            pl.BlockSpec((BQ, wide), lambda i: (i, t)),
            pl.BlockSpec((1, 1, HEAD_DIM, REP * BQ), lambda i: (t, i, 0, 0)),
            pl.BlockSpec((1, 1, 1, REP * BQ), lambda i: (t, i, 0, 0)),
            pl.BlockSpec((seq, HEAD_DIM), whole),
            pl.BlockSpec((seq, HEAD_DIM), whole),
        ],
        out_specs=pl.BlockSpec((seq, wide + 2 * HEAD_DIM), whole),
        out_shape=jax.ShapeDtypeStruct((seq, wide + 2 * HEAD_DIM), BF16),
        scratch_shapes=[
            pltpu.VMEM((REP * BQ, HEAD_DIM), BF16),
            pltpu.VMEM((HEAD_DIM, REP * BQ), BF16),
            pltpu.VMEM((REP * BQ, HEAD_DIM), BF16),
            pltpu.VMEM((HEAD_DIM, REP * BQ), BF16),
            pltpu.VMEM((seq // BK, HEAD_DIM, BK), BF16),
            pltpu.VMEM((seq, HEAD_DIM), F32),
            pltpu.VMEM((seq, HEAD_DIM), F32),
            pltpu.VMEM((HEAD_DIM, REP * BQ), F32),
            pltpu.VMEM((8, REP * BQ), F32),
        ],
        compiler_params=pltpu.CompilerParams(dimension_semantics=("arbitrary",), vmem_limit_bytes=VMEM_BYTES),
        cost_estimate=cost(flops, 8 * seq * wide * 2),
        name="attn_bwd",
    )(qkv, qkv, qkv, d_o, o_t, lse, cos_t, sin_t)


def ln_bwd_kernel(dh0_ref, dh1_ref, x_ref, lnw_ref, dx_ref, dw_ref):
    @pl.when(pl.program_id(0) == 0)
    def _():
        dw_ref[...] = jnp.zeros_like(dw_ref)

    xf = x_ref[...].astype(F32)
    mean = jnp.mean(xf, axis=-1, keepdims=True)
    cen = xf - mean
    var = jnp.mean(cen * cen, axis=-1, keepdims=True)
    rstd = lax.rsqrt(var + LN_EPS)
    xhat = cen * rstd
    dh = dh0_ref[...] + dh1_ref[...]
    dw_ref[...] += jnp.sum(dh * xhat, axis=0, keepdims=True)
    dxh = dh * lnw_ref[...].astype(F32)
    mean_d = jnp.mean(dxh, axis=-1, keepdims=True)
    mean_dx = jnp.mean(dxh * xhat, axis=-1, keepdims=True)
    dx_ref[...] = (rstd * (dxh - mean_d - xhat * mean_dx)).astype(BF16)


def ln_backward(dh0, dh1, x, ln_w):
    rows, dim = x.shape
    blk = 128
    row = lambda i: (i, 0)
    const = lambda i: (0, 0)
    return pl.pallas_call(
        ln_bwd_kernel,
        grid=(rows // blk,),
        in_specs=[pl.BlockSpec((blk, dim), row), pl.BlockSpec((blk, dim), row),
                  pl.BlockSpec((blk, dim), row), pl.BlockSpec((1, dim), const)],
        out_specs=(pl.BlockSpec((blk, dim), row), pl.BlockSpec((1, dim), const)),
        out_shape=(jax.ShapeDtypeStruct((rows, dim), BF16), jax.ShapeDtypeStruct((1, dim), F32)),
        compiler_params=pltpu.CompilerParams(dimension_semantics=("arbitrary",), vmem_limit_bytes=VMEM_BYTES),
        cost_estimate=cost(20 * rows * dim, 12 * rows * dim),
        name="ln_bwd",
    )(dh0, dh1, x, ln_w)


def reserve(*shapes):
    return pl.pallas_call(
        lambda *refs: None,
        out_shape=tuple(jax.ShapeDtypeStruct(s, BF16) for s in shapes),
        out_specs=tuple(pl.BlockSpec(memory_space=pl.ANY) for _ in shapes),
        cost_estimate=cost(1, 1),
        name="reserve",
    )()


def dw_kernel(idx, h_ref, *refs):
    n = len(refs) - 8
    grs, (q_ref, k_ref, v_ref, piece_ref, gr_sc) = refs[:n], refs[-5:]
    wide = q_ref.shape[1] // n
    cols = piece_ref.shape[1]

    @pl.when(pl.program_id(0) == 0)
    def _():
        for t, gr in enumerate(grs):
            gr_sc[:, t * wide:(t + 1) * wide] = gr[:, :wide]
            for part in range(2):
                start = n * wide + part * n * HEAD_DIM + t * HEAD_DIM
                gr_sc[:, start:start + HEAD_DIM] = gr[:, wide + part * HEAD_DIM:wide + (part + 1) * HEAD_DIM]

    for start in range(0, cols, 256):
        stop = min(start + 256, cols)
        piece_ref[:, start:stop] = mm(h_ref[...], gr_sc[:, start:stop], ((0,), (0,))).astype(BF16)
    q_ref[...] = piece_ref[:, :n * wide]
    k_ref[...] = piece_ref[:, n * wide:n * (wide + HEAD_DIM)]
    v_ref[...] = piece_ref[:, n * (wide + HEAD_DIM):]


def weight_grad(idx, h_all, grs, bufs):
    seq, dim = h_all.shape
    n = len(grs)
    cols = n * grs[0].shape[1]
    wide = REP * HEAD_DIM * n
    blk = 512
    there = lambda i, ix: (i, ix[0])
    flops = 2 * seq * dim * cols
    return pl.pallas_call(
        dw_kernel,
        out_shape=tuple(jax.ShapeDtypeStruct(b.shape, BF16) for b in bufs) + (jax.ShapeDtypeStruct((dim, cols), BF16),),
        grid_spec=pltpu.PrefetchScalarGridSpec(
            num_scalar_prefetch=1, grid=(dim // blk,),
            in_specs=[pl.BlockSpec((seq, blk), lambda i, ix: (0, i))]
            + [pl.BlockSpec((seq, cols // n), lambda i, ix: (0, 0), pipeline_mode=pl.Buffered(1)) for _ in grs]
            + [pl.BlockSpec(memory_space=pl.ANY)] * 3,
            out_specs=(pl.BlockSpec((blk, wide), there), pl.BlockSpec((blk, n * HEAD_DIM), there),
                       pl.BlockSpec((blk, n * HEAD_DIM), there), pl.BlockSpec((blk, cols), lambda i, ix: (i, 0))),
            scratch_shapes=[pltpu.VMEM((seq, cols), BF16)]),
        input_output_aliases={2 + n: 0, 3 + n: 1, 4 + n: 2},
        compiler_params=pltpu.CompilerParams(dimension_semantics=("arbitrary",), vmem_limit_bytes=VMEM_BYTES),
        cost_estimate=cost(flops, 2 * (seq * dim + seq * cols + 2 * dim * cols)),
        name="weight_grad",
    )(idx, h_all, *grs, *bufs)


def place_kernel(idx, piece_ref, *refs):
    q_ref, k_ref, v_ref = refs[-3:]
    wide, one = q_ref.shape[1], k_ref.shape[1]
    q_ref[...] = piece_ref[:, :wide]
    k_ref[...] = piece_ref[:, wide:wide + one]
    v_ref[...] = piece_ref[:, wide + one:]


def place(idx, piece, bufs):
    dim, cols = piece.shape
    one = cols // (REP + 2)
    blk = 512
    there = lambda i, ix: (i, ix[0])
    return pl.pallas_call(
        place_kernel,
        out_shape=tuple(jax.ShapeDtypeStruct(b.shape, BF16) for b in bufs),
        grid_spec=pltpu.PrefetchScalarGridSpec(
            num_scalar_prefetch=1, grid=(dim // blk,),
            in_specs=[pl.BlockSpec((blk, cols), lambda i, ix: (i, 0))] + [pl.BlockSpec(memory_space=pl.ANY)] * 3,
            out_specs=(pl.BlockSpec((blk, REP * one), there), pl.BlockSpec((blk, one), there),
                       pl.BlockSpec((blk, one), there))),
        input_output_aliases={2: 0, 3: 1, 4: 2},
        compiler_params=pltpu.CompilerParams(dimension_semantics=("arbitrary",)),
        cost_estimate=cost(4 * dim * cols, 4 * dim * cols),
        name="place",
    )(idx, piece, *bufs)


def solution(mesh):
    n_dev = mesh.shape['sp']
    row_spec = P(('dp', 'sp'), None)
    pos_spec = P(('dp', 'sp'))
    full_spec = P(None, None)
    grad_spec = P('dp', None)

    def over_chip(val):
        return lax.ppermute(val, 'sp', [(i, i ^ 2) for i in range(n_dev)])

    def over_core(val):
        return lax.ppermute(val, 'sp', [(i, i ^ 1) for i in range(n_dev)])

    def layer(hidden, positions, d_attn, ln_weight, w_q, w_k, w_v, w_o):
        rows, dim = hidden.shape
        seq = rows * n_dev
        kv_local = w_k.shape[1] // HEAD_DIM // n_dev
        wide = REP * HEAD_DIM
        cq = w_q.shape[1] // n_dev
        ck = w_k.shape[1] // n_dev
        me = lax.axis_index('sp')
        chip, core = me // 2, me % 2
        hb = 2 * core + chip
        hbs = [hb, hb ^ 1, hb ^ 2, hb ^ 3]
        toks = [me, me ^ 2, me ^ 1, me ^ 3]

        pos_par = over_chip(positions)
        pos_src = (positions, over_core(positions), pos_par, over_core(pos_par))
        pos = jnp.concatenate([lax.select_n(me ^ b, *pos_src) for b in range(n_dev)])
        ln_row = ln_weight.reshape(1, dim)
        half = rows // 2
        h_own = [ln_forward(hidden[n * half:(n + 1) * half], ln_row) for n in range(2)]
        h_par = [over_chip(h) for h in h_own]
        g_par = over_chip(d_attn)
        h_sib = [over_core(h) for h in h_own]
        g_sib = over_core(d_attn)

        inv_freq = ROPE_BASE ** (-jnp.arange(0, HEAD_DIM, 2, dtype=F32) / HEAD_DIM)
        angles = pos.astype(F32)[:, None] * jnp.repeat(inv_freq, 2)[None, :]
        cos_t = jnp.cos(angles)
        sin_t = jnp.sin(angles) * jnp.where(jnp.arange(HEAD_DIM) % 2 == 0, -1.0, 1.0)[None, :]

        h_sp = [over_core(h) for h in h_par]
        g_sp = over_core(g_par)

        hq = None
        for tok, h in ((toks[0], h_own), (toks[2], h_sib)):
            for n in range(2):
                hq = qkv_block(jnp.stack([hb, 2 * tok + n]).astype(jnp.int32), h[n], w_q, w_k, w_v, cos_t, sin_t, seq, n_dev, hq)
        for n in range(2):
            for tok, h in ((toks[1], h_par), (toks[3], h_sp)):
                hq = qkv_block(jnp.stack([hb, 2 * tok + n]).astype(jnp.int32), h[n], w_q, w_k, w_v, cos_t, sin_t, seq, n_dev, hq)
        h_all, qkv = hq
        o_own, o_t, lse = attn_forward(qkv, kv_local)

        wo_t = transpose_rows(hb.reshape(1).astype(jnp.int32), w_o, n_dev)
        gd = None
        for tok, g in ((toks[0], d_attn), (toks[2], g_sib), (toks[1], g_par), (toks[3], g_sp)):
            idx = jnp.stack([hb, tok]).astype(jnp.int32)
            gd = do_block(idx, g, wo_t, seq, gd)
        g_all, d_o = gd

        def own_rows(val, dev):
            return lax.dynamic_slice_in_dim(val, dev * rows, rows, 0)

        o_par = over_chip(o_own)
        o_tok = [own_rows(o_own, me), own_rows(o_par, me),
                 over_core(own_rows(o_own, me ^ 1)), over_core(own_rows(o_par, me ^ 1))]
        wo_perm = jnp.concatenate([lax.dynamic_slice_in_dim(w_o, b * cq, cq, 0) for b in hbs], axis=0)
        attn_out = jnp.dot(jnp.concatenate(o_tok, axis=1), wo_perm, preferred_element_type=F32).astype(BF16)

        def token_dot(lhs, rhs):
            return mm(lhs, rhs, ((0,), (0,))).astype(BF16)

        dwo_own = token_dot(o_own, g_all)
        dwo_par = token_dot(o_par, g_all)
        d_w_o, *d_w = reserve(w_o.shape, w_q.shape, w_k.shape, w_v.shape)
        for b, piece in zip(hbs, (dwo_own, dwo_par, over_core(dwo_own), over_core(dwo_par))):
            d_w_o = lax.dynamic_update_slice_in_dim(d_w_o, piece, b * cq, 0)

        dhs = []
        gr = []
        for t in range(kv_local):
            gr.append(attn_backward(qkv, d_o, o_t, lse, cos_t, sin_t, kv_local, t))
        gr_par = [over_chip(val) for val in gr]

        def col(val):
            return val.reshape(1).astype(jnp.int32)

        *d_w, piece = weight_grad(col(hbs[0]), h_all, gr, d_w)
        piece = over_core(piece)
        d_w = place(col(hbs[2]), piece, d_w)
        for t in range(kv_local):
            gr_tok = [own_rows(gr[t], me), own_rows(gr_par[t], me),
                      over_core(own_rows(gr[t], me ^ 1)), over_core(own_rows(gr_par[t], me ^ 1))]
            parts = []
            for b in hbs:
                parts.append(lax.dynamic_slice_in_dim(w_q, b * cq + t * wide, wide, 1))
                parts.append(lax.dynamic_slice_in_dim(w_k, b * ck + t * HEAD_DIM, HEAD_DIM, 1))
                parts.append(lax.dynamic_slice_in_dim(w_v, b * ck + t * HEAD_DIM, HEAD_DIM, 1))
            w_perm = jnp.concatenate(parts, axis=1)
            dhs.append(mm(jnp.concatenate(gr_tok, axis=1), w_perm, ((1,), (1,))))
            *d_w, piece = weight_grad(col(hbs[1] * kv_local + t), h_all, (gr_par[t],), d_w)
            piece = over_core(piece)
            d_w = place(col(hbs[3] * kv_local + t), piece, d_w)

        d_hid, d_lnw = ln_backward(dhs[0], dhs[1], hidden, ln_row)
        d_lnw = d_lnw + over_core(d_lnw)
        d_lnw = d_lnw + over_chip(d_lnw)
        return (attn_out, d_hid, d_lnw.reshape(dim).astype(BF16), *d_w, d_w_o)

    return jax.shard_map(layer, mesh=mesh,
                         in_specs=(row_spec, pos_spec, row_spec, P(None), full_spec, full_spec, full_spec, full_spec),
                         out_specs=(row_spec, row_spec, P('dp'), grad_spec, grad_spec, grad_spec, grad_spec),
                         check_vma=False)
```

```python
import functools
import math
import jax
import jax.numpy as jnp
from jax import lax
from jax.experimental import pallas as pl
from jax.experimental.pallas import tpu as pltpu
from jax.sharding import PartitionSpec as P

HEAD_DIM = 128
LN_EPS = 1e-5
ROPE_BASE = 10000.0
REP = 3
BQ = 256
BK = 256
ROWS = 512
LOG2E = math.log2(math.e)
SCALE = HEAD_DIM ** -0.5
VMEM_BYTES = 60 * 1024 * 1024
F32 = jnp.float32
BF16 = jnp.bfloat16


def cost(flops, nbytes):
    return pl.CostEstimate(flops=int(flops), bytes_accessed=int(nbytes), transcendentals=0)


def mm(lhs, rhs, dims):
    return lax.dot_general(lhs, rhs, (dims, ((), ())), preferred_element_type=F32)


def rotate(val, cos_t, sin_t):
    lane = lax.broadcasted_iota(jnp.int32, val.shape, 1)
    swapped = jnp.where(lane % 2 == 0, pltpu.roll(val, HEAD_DIM - 1, 1), pltpu.roll(val, 1, 1))
    return val * cos_t + swapped * sin_t


def ln_kernel(x_ref, lnw_ref, h_ref):
    xf = x_ref[...].astype(F32)
    mean = jnp.mean(xf, axis=-1, keepdims=True)
    cen = xf - mean
    var = jnp.mean(cen * cen, axis=-1, keepdims=True)
    h_ref[...] = (cen * lax.rsqrt(var + LN_EPS) * lnw_ref[...].astype(F32)).astype(BF16)


def ln_forward(x, ln_w):
    rows, dim = x.shape
    blk = 128
    return pl.pallas_call(
        ln_kernel,
        grid=(rows // blk,),
        in_specs=[pl.BlockSpec((blk, dim), lambda i: (i, 0)), pl.BlockSpec((1, dim), lambda i: (0, 0))],
        out_specs=pl.BlockSpec((blk, dim), lambda i: (i, 0)),
        out_shape=jax.ShapeDtypeStruct((rows, dim), BF16),
        compiler_params=pltpu.CompilerParams(dimension_semantics=("arbitrary",)),
        cost_estimate=cost(10 * rows * dim, 4 * rows * dim),
        name="ln_fwd",
    )(x, ln_w)


def qkv_kernel(idx, h_ref, wq_ref, wk_ref, wv_ref, cos_ref, sin_ref, *rest):
    qkv_ref = rest[-1]
    h = h_ref[...]
    cos_t = cos_ref[...]
    sin_t = sin_ref[...]
    nq = wq_ref.shape[1]
    nk = wk_ref.shape[1]
    step = 2 * HEAD_DIM
    for start in range(0, nq + nk, step):
        w = wq_ref[:, start:start + step] if start < nq else wk_ref[:, start - nq:start - nq + step]
        val = mm(h, w, ((1,), (0,)))
        for n in range(2):
            sl = slice(n * HEAD_DIM, (n + 1) * HEAD_DIM)
            qkv_ref[:, start + n * HEAD_DIM:start + (n + 1) * HEAD_DIM] = rotate(val[:, sl], cos_t, sin_t).astype(BF16)
    qkv_ref[:, nq + nk:] = mm(h, wv_ref[...], ((1,), (0,))).astype(BF16)


def qkv_block(idx, h, w_q, w_k, w_v, cos_t, sin_t, seq, n_dev, prev):
    rows, dim = h.shape
    cq, ck = w_q.shape[1] // n_dev, w_k.shape[1] // n_dev
    per = rows // ROWS
    head = lambda i, ix: (0, ix[0])
    here = lambda i, ix: (ix[1] * per + i, 0)
    in_specs = [
        pl.BlockSpec((ROWS, dim), lambda i, ix: (i, 0)),
        pl.BlockSpec((dim, cq), head),
        pl.BlockSpec((dim, ck), head),
        pl.BlockSpec((dim, ck), head),
        pl.BlockSpec((ROWS, HEAD_DIM), here),
        pl.BlockSpec((ROWS, HEAD_DIM), here),
    ]
    args = [idx, h, w_q, w_k, w_v, cos_t, sin_t]
    aliases = {}
    if prev is not None:
        in_specs.append(pl.BlockSpec(memory_space=pl.ANY))
        args.append(prev)
        aliases = {7: 0}
    cols = cq + 2 * ck
    return pl.pallas_call(
        qkv_kernel,
        out_shape=jax.ShapeDtypeStruct((seq, cols), BF16),
        grid_spec=pltpu.PrefetchScalarGridSpec(
            num_scalar_prefetch=1, grid=(per,), in_specs=in_specs,
            out_specs=pl.BlockSpec((ROWS, cols), here)),
        input_output_aliases=aliases,
        compiler_params=pltpu.CompilerParams(dimension_semantics=("arbitrary",), vmem_limit_bytes=VMEM_BYTES),
        cost_estimate=cost(2 * rows * dim * cols, 2 * (rows * dim + dim * cols + rows * cols)),
        name="qkv",
    )(*args)


def wo_t_kernel(idx, wo_ref, out_ref):
    out_ref[...] = wo_ref[...].astype(F32).T.astype(BF16)


def transpose_rows(idx, w_o, n_dev):
    ce, dim = w_o.shape[0] // n_dev, w_o.shape[1]
    blk = 512
    return pl.pallas_call(
        wo_t_kernel,
        out_shape=jax.ShapeDtypeStruct((dim, ce), BF16),
        grid_spec=pltpu.PrefetchScalarGridSpec(
            num_scalar_prefetch=1, grid=(dim // blk,),
            in_specs=[pl.BlockSpec((ce, blk), lambda i, ix: (ix[0], i))],
            out_specs=pl.BlockSpec((blk, ce), lambda i, ix: (i, 0))),
        compiler_params=pltpu.CompilerParams(dimension_semantics=("arbitrary",)),
        cost_estimate=cost(4 * ce * dim, 4 * ce * dim),
        name="wo_t",
    )(idx, w_o)


def do_kernel(idx, g_ref, wo_ref, *rest):
    do_ref = rest[-1]
    do_ref[...] = mm(g_ref[...], wo_ref[...], ((1,), (0,))).astype(BF16)


def do_block(idx, g, wo_t, seq, prev):
    rows, dim = g.shape
    ce = wo_t.shape[1]
    per = rows // ROWS
    here = lambda i, ix: (ix[1] * per + i, 0)
    in_specs = [
        pl.BlockSpec((ROWS, dim), lambda i, ix: (i, 0)),
        pl.BlockSpec((dim, ce), lambda i, ix: (0, 0)),
    ]
    args = [idx, g, wo_t]
    aliases = {}
    if prev is not None:
        in_specs.append(pl.BlockSpec(memory_space=pl.ANY))
        args.append(prev)
        aliases = {3: 0}
    return pl.pallas_call(
        do_kernel,
        out_shape=jax.ShapeDtypeStruct((seq, ce), BF16),
        grid_spec=pltpu.PrefetchScalarGridSpec(
            num_scalar_prefetch=1, grid=(per,), in_specs=in_specs,
            out_specs=pl.BlockSpec((ROWS, ce), here)),
        input_output_aliases=aliases,
        compiler_params=pltpu.CompilerParams(dimension_semantics=("arbitrary",), vmem_limit_bytes=VMEM_BYTES),
        cost_estimate=cost(2 * rows * dim * ce, 2 * (rows * dim + dim * ce + rows * ce)),
        name="d_o",
    )(*args)


def stack_heads(val):
    return jnp.concatenate([val[:, n * HEAD_DIM:(n + 1) * HEAD_DIM] for n in range(REP)], axis=0)


def flip(val):
    return val.astype(F32).T.astype(BF16)


def causal(shape):
    return lax.broadcasted_iota(jnp.int32, shape, 0) <= lax.broadcasted_iota(jnp.int32, shape, 1) % BQ


def fwd_kernel(q_ref, k_ref, v_ref, o_ref, ot_ref, lse_ref, qt_sc, vt_sc, acc_sc, ml_sc, s_sc):
    blk = pl.program_id(1)
    n_chunks = k_ref.shape[0] // BK
    pairs = blk // 2

    @pl.when(blk == 0)
    def _():
        def one(j, _):
            vt_sc[j] = flip(v_ref[pl.ds(j * BK, BK), :])
            return 0

        lax.fori_loop(0, n_chunks, one, 0)

    qt_sc[...] = flip(stack_heads(q_ref[...]))

    def score(j):
        return mm(k_ref[pl.ds(j * BK, BK), :], qt_sc[...], ((1,), (0,))) * (SCALE * LOG2E)

    def ahead(pair):
        for n in range(2):
            nxt = score(2 * pair + n)
            s_sc[n] = nxt
            ml_sc[2 + n:3 + n, :] = jnp.max(nxt, axis=0, keepdims=True)

    def update(m_new, js, scores, first):
        if first:
            total, acc = 0.0, 0.0
        else:
            alpha = jnp.exp2(ml_sc[0:1, :] - m_new)
            total, acc = ml_sc[1:2, :] * alpha, acc_sc[...] * alpha
        for j, s in zip(js, scores):
            p = jnp.exp2(s - m_new)
            total = total + jnp.sum(p, axis=0, keepdims=True)
            acc = acc + mm(vt_sc[j], p.astype(BF16), ((1,), (0,)))
        ml_sc[0:1, :] = m_new
        ml_sc[1:2, :] = total
        acc_sc[...] = acc

    def last_chunks(js):
        scores = [score(j) for j in js]
        scores[-1] = jnp.where(causal(scores[-1].shape), scores[-1], -jnp.inf)
        m_new = functools.reduce(jnp.maximum, [jnp.max(s, axis=0, keepdims=True) for s in scores])
        ahead(0)
        update(m_new, js, scores, True)

    def held(pair, more):
        m_new = jnp.maximum(ml_sc[0:1, :], jnp.maximum(ml_sc[2:3, :], ml_sc[3:4, :]))
        scores = [s_sc[n] for n in range(2)]
        if more:
            ahead(pair + 1)
        update(m_new, (2 * pair, 2 * pair + 1), scores, False)

    @pl.when(blk % 2 == 1)
    def _():
        last_chunks((blk - 1, blk))

    @pl.when(blk % 2 == 0)
    def _():
        last_chunks((blk,))

    def body(pair, _):
        held(pair, True)
        return 0

    lax.fori_loop(0, pairs - 1, body, 0)

    @pl.when(pairs > 0)
    def _():
        held(pairs - 1, False)

    total = ml_sc[1:2, :]
    out_t = acc_sc[...] / total
    ot_ref[0, 0] = out_t
    lse_ref[0, 0] = ml_sc[0:1, :] + jnp.log2(total)
    for n in range(REP):
        o_ref[:, n * HEAD_DIM:(n + 1) * HEAD_DIM] = out_t[:, n * BQ:(n + 1) * BQ].T.astype(BF16)


def attn_forward(qkv, kv_local):
    seq = qkv.shape[0]
    nq = seq // BQ
    wide = REP * HEAD_DIM
    first_k = kv_local * REP
    flops = 2 * 2 * kv_local * REP * seq * seq // 2 * HEAD_DIM * 2
    return pl.pallas_call(
        fwd_kernel,
        grid=(kv_local, nq),
        in_specs=[
            pl.BlockSpec((BQ, wide), lambda t, i: (i, t)),
            pl.BlockSpec((seq, HEAD_DIM), lambda t, i: (0, first_k + t)),
            pl.BlockSpec((seq, HEAD_DIM), lambda t, i: (0, first_k + kv_local + t)),
        ],
        out_specs=(
            pl.BlockSpec((BQ, wide), lambda t, i: (i, t)),
            pl.BlockSpec((1, 1, HEAD_DIM, REP * BQ), lambda t, i: (t, i, 0, 0)),
            pl.BlockSpec((1, 1, 1, REP * BQ), lambda t, i: (t, i, 0, 0)),
        ),
        out_shape=(
            jax.ShapeDtypeStruct((seq, kv_local * wide), BF16),
            jax.ShapeDtypeStruct((kv_local, nq, HEAD_DIM, REP * BQ), F32),
            jax.ShapeDtypeStruct((kv_local, nq, 1, REP * BQ), F32),
        ),
        scratch_shapes=[
            pltpu.VMEM((HEAD_DIM, REP * BQ), BF16),
            pltpu.VMEM((seq // BK, HEAD_DIM, BK), BF16),
            pltpu.VMEM((HEAD_DIM, REP * BQ), F32),
            pltpu.VMEM((8, REP * BQ), F32),
            pltpu.VMEM((2, BK, REP * BQ), F32),
        ],
        compiler_params=pltpu.CompilerParams(dimension_semantics=("arbitrary", "arbitrary"), vmem_limit_bytes=VMEM_BYTES),
        cost_estimate=cost(flops, 4 * seq * wide * kv_local * 2),
        name="attn_fwd",
    )(qkv, qkv, qkv)


def bwd_kernel(q_ref, k_ref, v_ref, do_ref, ot_ref, lse_ref, cos_ref, sin_ref, out_ref,
               qs_sc, qt_sc, ds_sc, dt_sc, kt_sc, dk_sc, dv_sc, dq_sc, row_sc):
    blk = pl.program_id(0)
    wide = REP * HEAD_DIM
    n_chunks = k_ref.shape[0] // BK

    @pl.when(blk == 0)
    def _():
        def one(j, _):
            rows = pl.ds(j * BK, BK)
            kt_sc[j] = flip(k_ref[rows, :])
            dk_sc[rows, :] = jnp.zeros((BK, HEAD_DIM), F32)
            dv_sc[rows, :] = jnp.zeros((BK, HEAD_DIM), F32)
            return 0

        lax.fori_loop(0, n_chunks, one, 0)

    q_all = stack_heads(q_ref[...])
    do_all = stack_heads(do_ref[...])
    qs_sc[...] = q_all
    qt_sc[...] = flip(q_all)
    ds_sc[...] = do_all
    do_t = do_all.astype(F32).T
    dt_sc[...] = do_t.astype(BF16)
    row_sc[0:1, :] = lse_ref[0, 0]
    row_sc[1:2, :] = jnp.sum(ot_ref[0, 0] * do_t, axis=0, keepdims=True)
    dq_sc[...] = jnp.zeros_like(dq_sc)

    def chunks(js, masked):
        rows = [pl.ds(j * BK, BK) for j in js]
        scores = [mm(k_ref[r, :], qt_sc[...], ((1,), (0,))) * (SCALE * LOG2E) for r in rows]
        dps = [mm(v_ref[r, :], dt_sc[...], ((1,), (0,))) for r in rows]
        dq = dq_sc[...]
        for n, (j, r) in enumerate(zip(js, rows)):
            p = jnp.exp2(scores[n] - row_sc[0:1, :])
            if masked and n == len(js) - 1:
                p = jnp.where(causal(p.shape), p, 0.0)
            dv_sc[r, :] += mm(p.astype(BF16), ds_sc[...], ((1,), (0,)))
            d_s = (p * (dps[n] - row_sc[1:2, :]) * SCALE).astype(BF16)
            dk_sc[r, :] += mm(d_s, qs_sc[...], ((1,), (0,)))
            dq = dq + mm(kt_sc[j], d_s, ((1,), (0,)))
        dq_sc[...] = dq

    def body(j, _):
        chunks((2 * j, 2 * j + 1), False)
        return 0

    lax.fori_loop(0, blk // 2, body, 0)

    @pl.when(blk % 2 == 1)
    def _():
        chunks((blk - 1, blk), True)

    @pl.when(blk % 2 == 0)
    def _():
        chunks((blk,), True)

    rows = pl.ds(blk * BQ, BQ)
    cos_t = cos_ref[rows, :]
    sin_t = -sin_ref[rows, :]
    for n in range(REP):
        dq = dq_sc[:, n * BQ:(n + 1) * BQ].T.astype(BF16).astype(F32)
        out_ref[rows, n * HEAD_DIM:(n + 1) * HEAD_DIM] = rotate(dq, cos_t, sin_t).astype(BF16)

    @pl.when(blk == pl.num_programs(0) - 1)
    def _():
        def one(j, _):
            kr = pl.ds(j * BK, BK)
            dk = dk_sc[kr, :].astype(BF16).astype(F32)
            out_ref[kr, wide:wide + HEAD_DIM] = rotate(dk, cos_ref[kr, :], -sin_ref[kr, :]).astype(BF16)
            out_ref[kr, wide + HEAD_DIM:wide + 2 * HEAD_DIM] = dv_sc[kr, :].astype(BF16)
            return 0

        lax.fori_loop(0, n_chunks, one, 0)


def attn_backward(qkv, d_o, o_t, lse, cos_t, sin_t, kv_local, t):
    seq = qkv.shape[0]
    nq = seq // BQ
    wide = REP * HEAD_DIM
    first_k = kv_local * REP
    flops = 5 * 2 * REP * seq * seq // 2 * HEAD_DIM * 2
    whole = lambda i: (0, 0)
    return pl.pallas_call(
        bwd_kernel,
        grid=(nq,),
        in_specs=[
            pl.BlockSpec((BQ, wide), lambda i: (i, t)),
            pl.BlockSpec((seq, HEAD_DIM), lambda i: (0, first_k + t)),
            pl.BlockSpec((seq, HEAD_DIM), lambda i: (0, first_k + kv_local + t)),
            pl.BlockSpec((BQ, wide), lambda i: (i, t)),
            pl.BlockSpec((1, 1, HEAD_DIM, REP * BQ), lambda i: (t, i, 0, 0)),
            pl.BlockSpec((1, 1, 1, REP * BQ), lambda i: (t, i, 0, 0)),
            pl.BlockSpec((seq, HEAD_DIM), whole),
            pl.BlockSpec((seq, HEAD_DIM), whole),
        ],
        out_specs=pl.BlockSpec((seq, wide + 2 * HEAD_DIM), whole),
        out_shape=jax.ShapeDtypeStruct((seq, wide + 2 * HEAD_DIM), BF16),
        scratch_shapes=[
            pltpu.VMEM((REP * BQ, HEAD_DIM), BF16),
            pltpu.VMEM((HEAD_DIM, REP * BQ), BF16),
            pltpu.VMEM((REP * BQ, HEAD_DIM), BF16),
            pltpu.VMEM((HEAD_DIM, REP * BQ), BF16),
            pltpu.VMEM((seq // BK, HEAD_DIM, BK), BF16),
            pltpu.VMEM((seq, HEAD_DIM), F32),
            pltpu.VMEM((seq, HEAD_DIM), F32),
            pltpu.VMEM((HEAD_DIM, REP * BQ), F32),
            pltpu.VMEM((8, REP * BQ), F32),
        ],
        compiler_params=pltpu.CompilerParams(dimension_semantics=("arbitrary",), vmem_limit_bytes=VMEM_BYTES),
        cost_estimate=cost(flops, 8 * seq * wide * 2),
        name="attn_bwd",
    )(qkv, qkv, qkv, d_o, o_t, lse, cos_t, sin_t)


N_TILE = 1024


def accumulate(acc_sc, weight):
    def tile(n, _):
        cols = pl.ds(pl.multiple_of(n * N_TILE, N_TILE), N_TILE)
        acc_sc[:, cols] += weight(cols)
        return 0

    lax.fori_loop(0, acc_sc.shape[1] // N_TILE, tile, 0)


def out_kernel(idx, *refs):
    pieces, (w_ref, out_ref, cur_sc, acc_sc) = refs[:4], refs[4:]
    src = pl.program_id(0)
    for n, piece in enumerate(pieces):
        @pl.when(src == n)
        def _():
            cur_sc[...] = piece[...]

    @pl.when(src == 0)
    def _():
        acc_sc[...] = jnp.zeros_like(acc_sc)

    accumulate(acc_sc, lambda cols: mm(cur_sc[...], w_ref[:, cols], ((1,), (0,))))

    @pl.when(src == 3)
    def _():
        out_ref[...] = acc_sc[...].astype(BF16)


def single(shape, index):
    return pl.BlockSpec(shape, index, pipeline_mode=pl.Buffered(1))


def out_proj(idx, pieces, w_o, rows):
    wide = pieces[0].shape[1]
    dim = w_o.shape[1]
    mine = single((rows, wide), lambda s, ix: (ix[0], 0))
    sent = single((rows, wide), lambda s, ix: (0, 0))
    return pl.pallas_call(
        out_kernel,
        out_shape=jax.ShapeDtypeStruct((rows, dim), BF16),
        grid_spec=pltpu.PrefetchScalarGridSpec(
            num_scalar_prefetch=1, grid=(4,),
            in_specs=[mine, mine, sent, sent, pl.BlockSpec((wide, dim), lambda s, ix: (ix[1 + s], 0))],
            out_specs=pl.BlockSpec((rows, dim), lambda s, ix: (0, 0)),
            scratch_shapes=[pltpu.VMEM((rows, wide), BF16), pltpu.VMEM((rows, dim), F32)]),
        compiler_params=pltpu.CompilerParams(dimension_semantics=("arbitrary",), vmem_limit_bytes=VMEM_BYTES),
        cost_estimate=cost(8 * rows * dim * wide, 2 * (5 * rows * dim)),
        name="out_proj",
    )(idx, *pieces, w_o)


def dh_kernel(idx, *refs):
    pieces = refs[:8]
    wq_ref, wk_ref, wv_ref, x_ref, lnw_ref, dx_ref, dw_ref, cur_sc, acc_sc, dx_sc, sem = refs[8:]
    src = pl.program_id(0)
    wide = wq_ref.shape[1]
    each = wide // 2
    for n in range(4):
        @pl.when(src == n)
        def _():
            for t in range(2):
                piece = pieces[2 * n + t]
                cur_sc[:, t * each:(t + 1) * each] = piece[:, :each]
                for part in range(2):
                    start = wide + (2 * part + t) * HEAD_DIM
                    cur_sc[:, start:start + HEAD_DIM] = piece[:, each + part * HEAD_DIM:each + (part + 1) * HEAD_DIM]

    @pl.when(src == 0)
    def _():
        acc_sc[...] = jnp.zeros_like(acc_sc)

    both = wide + 2 * HEAD_DIM
    accumulate(acc_sc, lambda cols: mm(cur_sc[:, :wide], wq_ref[cols, :], ((1,), (1,)))
               + mm(cur_sc[:, wide:both], wk_ref[cols, :], ((1,), (1,)))
               + mm(cur_sc[:, both:], wv_ref[cols, :], ((1,), (1,))))

    @pl.when(src == 3)
    def _():
        blk = dx_sc.shape[1]
        n_blk = x_ref.shape[0] // blk
        weight = lnw_ref[...].astype(F32)
        dw_ref[...] = jnp.zeros_like(dw_ref)

        def put(n, slot):
            return pltpu.make_async_copy(dx_sc.at[slot], dx_ref.at[pl.ds(n * blk, blk), :], sem.at[slot])

        def one(n, _):
            slot = n % 2
            rows = pl.ds(n * blk, blk)

            @pl.when(n >= 2)
            def _():
                put(n - 2, slot).wait()

            xf = x_ref[rows, :].astype(F32)
            mean = jnp.mean(xf, axis=-1, keepdims=True)
            cen = xf - mean
            var = jnp.mean(cen * cen, axis=-1, keepdims=True)
            rstd = lax.rsqrt(var + LN_EPS)
            xhat = cen * rstd
            dh = acc_sc[rows, :]
            dw_ref[...] += jnp.sum(dh * xhat, axis=0, keepdims=True)
            dxh = dh * weight
            mean_d = jnp.mean(dxh, axis=-1, keepdims=True)
            mean_dx = jnp.mean(dxh * xhat, axis=-1, keepdims=True)
            dx_sc[slot] = (rstd * (dxh - mean_d - xhat * mean_dx)).astype(BF16)
            put(n, slot).start()
            return 0

        lax.fori_loop(0, n_blk, one, 0)
        for n in range(n_blk - 2, n_blk):
            put(n, n % 2).wait()


def hidden_grad(idx, pieces, w_q, w_k, w_v, x, ln_w, n_dev):
    rows, dim = x.shape
    cols = pieces[0].shape[1]
    cq, ck = w_q.shape[1] // n_dev, w_k.shape[1] // n_dev
    mine = single((rows, cols), lambda s, ix: (ix[0], 0))
    sent = single((rows, cols), lambda s, ix: (0, 0))
    const = lambda s, ix: (0, 0)
    head = lambda s, ix: (0, ix[1 + s])
    blk = 128
    return pl.pallas_call(
        dh_kernel,
        out_shape=(jax.ShapeDtypeStruct((rows, dim), BF16), jax.ShapeDtypeStruct((1, dim), F32)),
        grid_spec=pltpu.PrefetchScalarGridSpec(
            num_scalar_prefetch=1, grid=(4,),
            in_specs=[mine] * 4 + [sent] * 4
            + [pl.BlockSpec((dim, cq), head), pl.BlockSpec((dim, ck), head), pl.BlockSpec((dim, ck), head),
               single((rows, dim), const), pl.BlockSpec((1, dim), const)],
            out_specs=(pl.BlockSpec(memory_space=pl.ANY), pl.BlockSpec((1, dim), const)),
            scratch_shapes=[pltpu.VMEM((rows, 2 * cols), BF16), pltpu.VMEM((rows, dim), F32),
                            pltpu.VMEM((2, blk, dim), BF16), pltpu.SemaphoreType.DMA((2,))]),
        compiler_params=pltpu.CompilerParams(dimension_semantics=("arbitrary",), vmem_limit_bytes=VMEM_BYTES),
        cost_estimate=cost(16 * rows * dim * cols, 2 * (2 * rows * dim + 8 * cols * (rows + dim))),
        name="hidden_grad",
    )(idx, *pieces, w_q, w_k, w_v, x, ln_w)


def reserve(*shapes):
    return pl.pallas_call(
        lambda *refs: None,
        out_shape=tuple(jax.ShapeDtypeStruct(s, BF16) for s in shapes),
        out_specs=tuple(pl.BlockSpec(memory_space=pl.ANY) for _ in shapes),
        cost_estimate=cost(1, 1),
        name="reserve",
    )()


def dw_kernel(idx, *refs):
    hs, refs = refs[:4], refs[4:]
    n = len(refs) - 8
    rows = hs[0].shape[0]
    grs, (q_ref, k_ref, v_ref, piece_ref, gr_sc) = refs[:n], refs[-5:]
    wide = q_ref.shape[1] // n
    cols = piece_ref.shape[1]

    @pl.when(pl.program_id(0) == 0)
    def _():
        for b in range(4):
            to = slice(b * rows, (b + 1) * rows)
            at = pl.ds(idx[1 + b] * rows, rows)
            for t, gr in enumerate(grs):
                gr_sc[to, t * wide:(t + 1) * wide] = gr[at, :wide]
                for part in range(2):
                    start = n * wide + part * n * HEAD_DIM + t * HEAD_DIM
                    gr_sc[to, start:start + HEAD_DIM] = gr[at, wide + part * HEAD_DIM:wide + (part + 1) * HEAD_DIM]

    for start in range(0, cols, 256):
        stop = min(start + 256, cols)
        val = sum(mm(h[...], gr_sc[b * rows:(b + 1) * rows, start:stop], ((0,), (0,))) for b, h in enumerate(hs))
        piece_ref[:, start:stop] = val.astype(BF16)
    q_ref[...] = piece_ref[:, :n * wide]
    k_ref[...] = piece_ref[:, n * wide:n * (wide + HEAD_DIM)]
    v_ref[...] = piece_ref[:, n * (wide + HEAD_DIM):]


def weight_grad(idx, hs, grs, bufs):
    rows, dim = hs[0].shape
    seq = 4 * rows
    n = len(grs)
    cols = n * grs[0].shape[1]
    wide = REP * HEAD_DIM * n
    blk = 512
    there = lambda i, ix: (i, ix[0])
    flops = 2 * seq * dim * cols
    return pl.pallas_call(
        dw_kernel,
        out_shape=tuple(jax.ShapeDtypeStruct(b.shape, BF16) for b in bufs) + (jax.ShapeDtypeStruct((dim, cols), BF16),),
        grid_spec=pltpu.PrefetchScalarGridSpec(
            num_scalar_prefetch=1, grid=(dim // blk,),
            in_specs=[pl.BlockSpec((rows, blk), lambda i, ix: (0, i))] * 4
            + [pl.BlockSpec((seq, cols // n), lambda i, ix: (0, 0), pipeline_mode=pl.Buffered(1)) for _ in grs]
            + [pl.BlockSpec(memory_space=pl.ANY)] * 3,
            out_specs=(pl.BlockSpec((blk, wide), there), pl.BlockSpec((blk, n * HEAD_DIM), there),
                       pl.BlockSpec((blk, n * HEAD_DIM), there), pl.BlockSpec((blk, cols), lambda i, ix: (i, 0))),
            scratch_shapes=[pltpu.VMEM((seq, cols), BF16)]),
        input_output_aliases={5 + n: 0, 6 + n: 1, 7 + n: 2},
        compiler_params=pltpu.CompilerParams(dimension_semantics=("arbitrary",), vmem_limit_bytes=VMEM_BYTES),
        cost_estimate=cost(flops, 2 * (seq * dim + seq * cols + 2 * dim * cols)),
        name="weight_grad",
    )(idx, *hs, *grs, *bufs)


def dwo_kernel(idx, o_ref, *refs):
    gs, (buf_ref, out_ref, piece_ref) = refs[:4], refs[4:]
    rows = gs[0].shape[0]
    for start in range(0, piece_ref.shape[1], 256):
        cols = slice(start, start + 256)
        val = sum(mm(o_ref[pl.ds(idx[1 + b] * rows, rows), :], g[:, cols], ((0,), (0,))) for b, g in enumerate(gs))
        piece_ref[:, cols] = val.astype(BF16)
    out_ref[...] = piece_ref[...]


def out_weight_grad(idx, o, gs, buf):
    seq, wide = o.shape
    rows, dim = gs[0].shape
    blk = 512
    return pl.pallas_call(
        dwo_kernel,
        out_shape=(jax.ShapeDtypeStruct(buf.shape, BF16), jax.ShapeDtypeStruct((wide, dim), BF16)),
        grid_spec=pltpu.PrefetchScalarGridSpec(
            num_scalar_prefetch=1, grid=(dim // blk,),
            in_specs=[single((seq, wide), lambda i, ix: (0, 0))]
            + [pl.BlockSpec((rows, blk), lambda i, ix: (0, i))] * 4 + [pl.BlockSpec(memory_space=pl.ANY)],
            out_specs=(pl.BlockSpec((wide, blk), lambda i, ix: (ix[0], i)), pl.BlockSpec((wide, blk), lambda i, ix: (0, i)))),
        input_output_aliases={6: 0},
        compiler_params=pltpu.CompilerParams(dimension_semantics=("arbitrary",), vmem_limit_bytes=VMEM_BYTES),
        cost_estimate=cost(2 * seq * wide * dim, 2 * (seq * dim + seq * wide + 2 * wide * dim)),
        name="out_weight_grad",
    )(idx, o, *gs, buf)


def place_kernel(idx, piece_ref, *refs):
    q_ref, k_ref, v_ref = refs[-3:]
    wide, one = q_ref.shape[1], k_ref.shape[1]
    q_ref[...] = piece_ref[:, :wide]
    k_ref[...] = piece_ref[:, wide:wide + one]
    v_ref[...] = piece_ref[:, wide + one:]


def place(idx, piece, bufs):
    dim, cols = piece.shape
    one = cols // (REP + 2)
    blk = 512
    there = lambda i, ix: (i, ix[0])
    return pl.pallas_call(
        place_kernel,
        out_shape=tuple(jax.ShapeDtypeStruct(b.shape, BF16) for b in bufs),
        grid_spec=pltpu.PrefetchScalarGridSpec(
            num_scalar_prefetch=1, grid=(dim // blk,),
            in_specs=[pl.BlockSpec((blk, cols), lambda i, ix: (i, 0))] + [pl.BlockSpec(memory_space=pl.ANY)] * 3,
            out_specs=(pl.BlockSpec((blk, REP * one), there), pl.BlockSpec((blk, one), there),
                       pl.BlockSpec((blk, one), there))),
        input_output_aliases={2: 0, 3: 1, 4: 2},
        compiler_params=pltpu.CompilerParams(dimension_semantics=("arbitrary",)),
        cost_estimate=cost(4 * dim * cols, 4 * dim * cols),
        name="place",
    )(idx, piece, *bufs)


def solution(mesh):
    n_dev = mesh.shape['sp']
    row_spec = P(('dp', 'sp'), None)
    pos_spec = P(('dp', 'sp'))
    full_spec = P(None, None)
    grad_spec = P('dp', None)

    def over_chip(val):
        return lax.ppermute(val, 'sp', [(i, i ^ 2) for i in range(n_dev)])

    def over_core(val):
        return lax.ppermute(val, 'sp', [(i, i ^ 1) for i in range(n_dev)])

    def layer(hidden, positions, d_attn, ln_weight, w_q, w_k, w_v, w_o):
        rows, dim = hidden.shape
        seq = rows * n_dev
        kv_local = w_k.shape[1] // HEAD_DIM // n_dev
        cq = w_q.shape[1] // n_dev
        me = lax.axis_index('sp')
        chip, core = me // 2, me % 2
        hb = 2 * core + chip
        hbs = [hb, hb ^ 1, hb ^ 2, hb ^ 3]
        toks = [me, me ^ 2, me ^ 1, me ^ 3]

        pos_par = over_chip(positions)
        pos_src = (positions, over_core(positions), pos_par, over_core(pos_par))
        pos = jnp.concatenate([lax.select_n(me ^ b, *pos_src) for b in range(n_dev)])
        ln_row = ln_weight.reshape(1, dim)
        x_par = over_chip(hidden)
        g_par = over_chip(d_attn)
        x_sib = over_core(hidden)
        g_sib = over_core(d_attn)

        inv_freq = ROPE_BASE ** (-jnp.arange(0, HEAD_DIM, 2, dtype=F32) / HEAD_DIM)
        angles = pos.astype(F32)[:, None] * jnp.repeat(inv_freq, 2)[None, :]
        cos_t = jnp.cos(angles)
        sin_t = jnp.sin(angles) * jnp.where(jnp.arange(HEAD_DIM) % 2 == 0, -1.0, 1.0)[None, :]

        x_sp = over_core(x_par)
        g_sp = over_core(g_par)

        hs = [None] * 4
        qkv = None
        for b, x in ((0, hidden), (2, x_sib), (1, x_par), (3, x_sp)):
            hs[b] = ln_forward(x, ln_row)
            qkv = qkv_block(jnp.stack([hb, toks[b]]).astype(jnp.int32), hs[b], w_q, w_k, w_v, cos_t, sin_t, seq, n_dev, qkv)
        o_own, o_t, lse = attn_forward(qkv, kv_local)

        wo_t = transpose_rows(hb.reshape(1).astype(jnp.int32), w_o, n_dev)
        gs = [d_attn, g_par, g_sib, g_sp]
        d_o = None
        for b in (0, 2, 1, 3):
            d_o = do_block(jnp.stack([hb, toks[b]]).astype(jnp.int32), gs[b], wo_t, seq, d_o)

        def own_rows(val, dev):
            return lax.dynamic_slice_in_dim(val, dev * rows, rows, 0)

        o_par = over_chip(o_own)
        sources = jnp.stack([me, *hbs]).astype(jnp.int32)
        o_tok = [o_own, o_par, over_core(own_rows(o_own, me ^ 1)), over_core(own_rows(o_par, me ^ 1))]
        attn_out = out_proj(sources, o_tok, w_o, rows)

        def blocks(where):
            return jnp.stack([where, *toks]).astype(jnp.int32)

        d_w_o, *d_w = reserve(w_o.shape, w_q.shape, w_k.shape, w_v.shape)
        sent = []
        for b, o in ((hbs[0], o_own), (hbs[1], o_par)):
            d_w_o, piece = out_weight_grad(blocks(b), o, gs, d_w_o)
            sent.append(over_core(piece))
        for b, piece in zip(hbs[2:], sent):
            d_w_o = lax.dynamic_update_slice_in_dim(d_w_o, piece, b * cq, 0)

        gr = []
        for t in range(kv_local):
            gr.append(attn_backward(qkv, d_o, o_t, lse, cos_t, sin_t, kv_local, t))
        gr_par = [over_chip(val) for val in gr]

        def col(val):
            return val.reshape(1).astype(jnp.int32)

        *d_w, piece = weight_grad(blocks(hbs[0]), hs, gr, d_w)
        piece = over_core(piece)
        d_w = place(col(hbs[2]), piece, d_w)
        gr_tok = [gr, gr_par, [], []]
        for t in range(kv_local):
            gr_tok[2].append(over_core(own_rows(gr[t], me ^ 1)))
            gr_tok[3].append(over_core(own_rows(gr_par[t], me ^ 1)))
            *d_w, piece = weight_grad(blocks(hbs[1] * kv_local + t), hs, (gr_par[t],), d_w)
            piece = over_core(piece)
            d_w = place(col(hbs[3] * kv_local + t), piece, d_w)
        d_hid, d_lnw = hidden_grad(sources, [val for pair in gr_tok for val in pair], w_q, w_k, w_v, hidden, ln_row, n_dev)
        d_lnw = d_lnw + over_core(d_lnw)
        d_lnw = d_lnw + over_chip(d_lnw)
        return (attn_out, d_hid, d_lnw.reshape(dim).astype(BF16), *d_w, d_w_o)

    return jax.shard_map(layer, mesh=mesh,
                         in_specs=(row_spec, pos_spec, row_spec, P(None), full_spec, full_spec, full_spec, full_spec),
                         out_specs=(row_spec, row_spec, P('dp'), grad_spec, grad_spec, grad_spec, grad_spec),
                         check_vma=False)
```

```python
import functools
import math
import jax
import jax.numpy as jnp
from jax import lax
from jax.experimental import pallas as pl
from jax.experimental.pallas import tpu as pltpu
from jax.sharding import PartitionSpec as P

HEAD_DIM = 128
LN_EPS = 1e-5
ROPE_BASE = 10000.0
REP = 3
BQ = 256
BK = 256
ROWS = 512
LOG2E = math.log2(math.e)
SCALE = HEAD_DIM ** -0.5
VMEM_BYTES = 60 * 1024 * 1024
F32 = jnp.float32
BF16 = jnp.bfloat16


def cost(flops, nbytes):
    return pl.CostEstimate(flops=int(flops), bytes_accessed=int(nbytes), transcendentals=0)


def mm(lhs, rhs, dims):
    return lax.dot_general(lhs, rhs, (dims, ((), ())), preferred_element_type=F32)


def rotate(val, cos_t, sin_t):
    lane = lax.broadcasted_iota(jnp.int32, val.shape, 1)
    swapped = jnp.where(lane % 2 == 0, pltpu.roll(val, HEAD_DIM - 1, 1), pltpu.roll(val, 1, 1))
    return val * cos_t + swapped * sin_t


def pick(pair, sc):
    for n, ref in enumerate(pair):
        @pl.when(pl.program_id(0) == n)
        def _():
            sc[...] = ref[...]


def pair_specs(shape, per):
    return [pl.BlockSpec(shape, lambda p, i, ix: (jnp.where(p == 0, i, per - 1), 0)),
            pl.BlockSpec(shape, lambda p, i, ix: (jnp.where(p == 1, i, 0), 0))]


def qkv_kernel(idx, xa_ref, xb_ref, lnw_ref, wq_ref, wk_ref, wv_ref, cos_ref, sin_ref, *rest):
    h_ref, qkv_ref, x_sc = rest[-3:]
    pick((xa_ref, xb_ref), x_sc)
    weight = lnw_ref[...].astype(F32)
    nq = wq_ref.shape[1]
    nk = wk_ref.shape[1]
    step = 2 * HEAD_DIM
    for sub in range(ROWS // BQ):
        rows = slice(sub * BQ, (sub + 1) * BQ)
        xf = x_sc[rows, :].astype(F32)
        mean = jnp.mean(xf, axis=-1, keepdims=True)
        cen = xf - mean
        var = jnp.mean(cen * cen, axis=-1, keepdims=True)
        h = (cen * lax.rsqrt(var + LN_EPS) * weight).astype(BF16)
        h_ref[rows, :] = h
        cos_t = cos_ref[rows, :]
        sin_t = sin_ref[rows, :]
        for start in range(0, nq + nk, step):
            w = wq_ref[:, start:start + step] if start < nq else wk_ref[:, start - nq:start - nq + step]
            val = mm(h, w, ((1,), (0,)))
            for n in range(2):
                at = start + n * HEAD_DIM
                part = val[:, n * HEAD_DIM:(n + 1) * HEAD_DIM]
                qkv_ref[rows, at:at + HEAD_DIM] = rotate(part, cos_t, sin_t).astype(BF16)
        qkv_ref[rows, nq + nk:] = mm(h, wv_ref[...], ((1,), (0,))).astype(BF16)


def qkv_blocks(idx, xs, ln_w, w_q, w_k, w_v, cos_t, sin_t, seq, n_dev, prev):
    rows, dim = xs[0].shape
    cq, ck = w_q.shape[1] // n_dev, w_k.shape[1] // n_dev
    per = rows // ROWS
    head = lambda p, i, ix: (0, ix[0])
    here = lambda p, i, ix: (ix[1 + p] * per + i, 0)
    in_specs = pair_specs((ROWS, dim), per) + [
        pl.BlockSpec((1, dim), lambda p, i, ix: (0, 0)),
        pl.BlockSpec((dim, cq), head),
        pl.BlockSpec((dim, ck), head),
        pl.BlockSpec((dim, ck), head),
        pl.BlockSpec((ROWS, HEAD_DIM), here),
        pl.BlockSpec((ROWS, HEAD_DIM), here),
    ]
    args = [idx, *xs, ln_w, w_q, w_k, w_v, cos_t, sin_t]
    aliases = {}
    if prev is not None:
        in_specs.append(pl.BlockSpec(memory_space=pl.ANY))
        args.append(prev)
        aliases = {9: 1}
    cols = cq + 2 * ck
    return pl.pallas_call(
        qkv_kernel,
        out_shape=(jax.ShapeDtypeStruct((2 * rows, dim), BF16), jax.ShapeDtypeStruct((seq, cols), BF16)),
        grid_spec=pltpu.PrefetchScalarGridSpec(
            num_scalar_prefetch=1, grid=(2, per), in_specs=in_specs,
            out_specs=(pl.BlockSpec((ROWS, dim), lambda p, i, ix: (p * per + i, 0)), pl.BlockSpec((ROWS, cols), here)),
            scratch_shapes=[pltpu.VMEM((ROWS, dim), BF16)]),
        input_output_aliases=aliases,
        compiler_params=pltpu.CompilerParams(dimension_semantics=("arbitrary", "arbitrary"), vmem_limit_bytes=VMEM_BYTES),
        cost_estimate=cost(4 * rows * dim * cols, 2 * (4 * rows * dim + dim * cols + 2 * rows * cols)),
        name="ln_qkv",
    )(*args)


def wo_t_kernel(idx, wo_ref, out_ref):
    out_ref[...] = wo_ref[...].astype(F32).T.astype(BF16)


def transpose_rows(idx, w_o, n_dev):
    ce, dim = w_o.shape[0] // n_dev, w_o.shape[1]
    blk = 512
    return pl.pallas_call(
        wo_t_kernel,
        out_shape=jax.ShapeDtypeStruct((dim, ce), BF16),
        grid_spec=pltpu.PrefetchScalarGridSpec(
            num_scalar_prefetch=1, grid=(dim // blk,),
            in_specs=[pl.BlockSpec((ce, blk), lambda i, ix: (ix[0], i))],
            out_specs=pl.BlockSpec((blk, ce), lambda i, ix: (i, 0))),
        compiler_params=pltpu.CompilerParams(dimension_semantics=("arbitrary",)),
        cost_estimate=cost(4 * ce * dim, 4 * ce * dim),
        name="wo_t",
    )(idx, w_o)


def do_kernel(idx, ga_ref, gb_ref, wo_ref, *rest):
    do_ref, g_sc = rest[-2:]
    pick((ga_ref, gb_ref), g_sc)
    do_ref[...] = mm(g_sc[...], wo_ref[...], ((1,), (0,))).astype(BF16)


def do_blocks(idx, gs, wo_t, seq, prev):
    rows, dim = gs[0].shape
    ce = wo_t.shape[1]
    per = rows // BQ
    in_specs = pair_specs((BQ, dim), per) + [pl.BlockSpec((dim, ce), lambda p, i, ix: (0, 0))]
    args = [idx, *gs, wo_t]
    aliases = {}
    if prev is not None:
        in_specs.append(pl.BlockSpec(memory_space=pl.ANY))
        args.append(prev)
        aliases = {4: 0}
    return pl.pallas_call(
        do_kernel,
        out_shape=jax.ShapeDtypeStruct((seq, ce), BF16),
        grid_spec=pltpu.PrefetchScalarGridSpec(
            num_scalar_prefetch=1, grid=(2, per), in_specs=in_specs,
            out_specs=pl.BlockSpec((BQ, ce), lambda p, i, ix: (ix[1 + p] * per + i, 0)),
            scratch_shapes=[pltpu.VMEM((BQ, dim), BF16)]),
        input_output_aliases=aliases,
        compiler_params=pltpu.CompilerParams(dimension_semantics=("arbitrary", "arbitrary"), vmem_limit_bytes=VMEM_BYTES),
        cost_estimate=cost(4 * rows * dim * ce, 2 * (2 * rows * dim + dim * ce + 2 * rows * ce)),
        name="d_o",
    )(*args)


def stack_heads(val):
    return jnp.concatenate([val[:, n * HEAD_DIM:(n + 1) * HEAD_DIM] for n in range(REP)], axis=0)


def flip(val):
    return val.astype(F32).T.astype(BF16)


def causal(shape):
    return lax.broadcasted_iota(jnp.int32, shape, 0) <= lax.broadcasted_iota(jnp.int32, shape, 1) % BQ


def fwd_kernel(q_ref, k_ref, v_ref, o_ref, ot_ref, lse_ref, qt_sc, vt_sc, acc_sc, ml_sc, s_sc):
    blk = pl.program_id(1)
    n_chunks = k_ref.shape[0] // BK
    pairs = blk // 2

    @pl.when(blk == 0)
    def _():
        def one(j, _):
            vt_sc[j] = flip(v_ref[pl.ds(j * BK, BK), :])
            return 0

        lax.fori_loop(0, n_chunks, one, 0)

    qt_sc[...] = flip(stack_heads(q_ref[...]))

    def score(j):
        return mm(k_ref[pl.ds(j * BK, BK), :], qt_sc[...], ((1,), (0,))) * (SCALE * LOG2E)

    def ahead(pair):
        for n in range(2):
            nxt = score(2 * pair + n)
            s_sc[n] = nxt
            ml_sc[2 + n:3 + n, :] = jnp.max(nxt, axis=0, keepdims=True)

    def update(m_new, js, scores, first):
        if first:
            total, acc = 0.0, 0.0
        else:
            alpha = jnp.exp2(ml_sc[0:1, :] - m_new)
            total, acc = ml_sc[1:2, :] * alpha, acc_sc[...] * alpha
        for j, s in zip(js, scores):
            p = jnp.exp2(s - m_new)
            total = total + jnp.sum(p, axis=0, keepdims=True)
            acc = acc + mm(vt_sc[j], p.astype(BF16), ((1,), (0,)))
        ml_sc[0:1, :] = m_new
        ml_sc[1:2, :] = total
        acc_sc[...] = acc

    def last_chunks(js):
        scores = [score(j) for j in js]
        scores[-1] = jnp.where(causal(scores[-1].shape), scores[-1], -jnp.inf)
        m_new = functools.reduce(jnp.maximum, [jnp.max(s, axis=0, keepdims=True) for s in scores])
        ahead(0)
        update(m_new, js, scores, True)

    def held(pair, more):
        m_new = jnp.maximum(ml_sc[0:1, :], jnp.maximum(ml_sc[2:3, :], ml_sc[3:4, :]))
        scores = [s_sc[n] for n in range(2)]
        if more:
            ahead(pair + 1)
        update(m_new, (2 * pair, 2 * pair + 1), scores, False)

    @pl.when(blk % 2 == 1)
    def _():
        last_chunks((blk - 1, blk))

    @pl.when(blk % 2 == 0)
    def _():
        last_chunks((blk,))

    def body(pair, _):
        held(pair, True)
        return 0

    lax.fori_loop(0, pairs - 1, body, 0)

    @pl.when(pairs > 0)
    def _():
        held(pairs - 1, False)

    total = ml_sc[1:2, :]
    out_t = acc_sc[...] / total
    ot_ref[0, 0] = out_t
    lse_ref[0, 0] = ml_sc[0:1, :] + jnp.log2(total)
    for n in range(REP):
        o_ref[:, n * HEAD_DIM:(n + 1) * HEAD_DIM] = out_t[:, n * BQ:(n + 1) * BQ].T.astype(BF16)


def attn_forward(qkv, kv_local):
    seq = qkv.shape[0]
    nq = seq // BQ
    wide = REP * HEAD_DIM
    first_k = kv_local * REP
    flops = 2 * 2 * kv_local * REP * seq * seq // 2 * HEAD_DIM * 2
    return pl.pallas_call(
        fwd_kernel,
        grid=(kv_local, nq),
        in_specs=[
            pl.BlockSpec((BQ, wide), lambda t, i: (i, t)),
            pl.BlockSpec((seq, HEAD_DIM), lambda t, i: (0, first_k + t)),
            pl.BlockSpec((seq, HEAD_DIM), lambda t, i: (0, first_k + kv_local + t)),
        ],
        out_specs=(
            pl.BlockSpec((BQ, wide), lambda t, i: (i, t)),
            pl.BlockSpec((1, 1, HEAD_DIM, REP * BQ), lambda t, i: (t, i, 0, 0)),
            pl.BlockSpec((1, 1, 1, REP * BQ), lambda t, i: (t, i, 0, 0)),
        ),
        out_shape=(
            jax.ShapeDtypeStruct((seq, kv_local * wide), BF16),
            jax.ShapeDtypeStruct((kv_local, nq, HEAD_DIM, REP * BQ), F32),
            jax.ShapeDtypeStruct((kv_local, nq, 1, REP * BQ), F32),
        ),
        scratch_shapes=[
            pltpu.VMEM((HEAD_DIM, REP * BQ), BF16),
            pltpu.VMEM((seq // BK, HEAD_DIM, BK), BF16),
            pltpu.VMEM((HEAD_DIM, REP * BQ), F32),
            pltpu.VMEM((8, REP * BQ), F32),
            pltpu.VMEM((2, BK, REP * BQ), F32),
        ],
        compiler_params=pltpu.CompilerParams(dimension_semantics=("arbitrary", "arbitrary"), vmem_limit_bytes=VMEM_BYTES),
        cost_estimate=cost(flops, 4 * seq * wide * kv_local * 2),
        name="attn_fwd",
    )(qkv, qkv, qkv)


def bwd_kernel(q_ref, k_ref, v_ref, do_ref, ot_ref, lse_ref, cos_ref, sin_ref, out_ref,
               qs_sc, qt_sc, ds_sc, dt_sc, kt_sc, dk_sc, dv_sc, dq_sc, row_sc):
    blk = pl.program_id(0)
    wide = REP * HEAD_DIM
    n_chunks = k_ref.shape[0] // BK

    @pl.when(blk == 0)
    def _():
        def one(j, _):
            rows = pl.ds(j * BK, BK)
            kt_sc[j] = flip(k_ref[rows, :])
            dk_sc[rows, :] = jnp.zeros((BK, HEAD_DIM), F32)
            dv_sc[rows, :] = jnp.zeros((BK, HEAD_DIM), F32)
            return 0

        lax.fori_loop(0, n_chunks, one, 0)

    q_all = stack_heads(q_ref[...])
    do_all = stack_heads(do_ref[...])
    qs_sc[...] = q_all
    qt_sc[...] = flip(q_all)
    ds_sc[...] = do_all
    do_t = do_all.astype(F32).T
    dt_sc[...] = do_t.astype(BF16)
    row_sc[0:1, :] = lse_ref[0, 0]
    row_sc[1:2, :] = jnp.sum(ot_ref[0, 0] * do_t, axis=0, keepdims=True)
    dq_sc[...] = jnp.zeros_like(dq_sc)

    def chunks(js, masked):
        rows = [pl.ds(j * BK, BK) for j in js]
        scores = [mm(k_ref[r, :], qt_sc[...], ((1,), (0,))) * (SCALE * LOG2E) for r in rows]
        dps = [mm(v_ref[r, :], dt_sc[...], ((1,), (0,))) for r in rows]
        dq = dq_sc[...]
        for n, (j, r) in enumerate(zip(js, rows)):
            p = jnp.exp2(scores[n] - row_sc[0:1, :])
            if masked and n == len(js) - 1:
                p = jnp.where(causal(p.shape), p, 0.0)
            dv_sc[r, :] += mm(p.astype(BF16), ds_sc[...], ((1,), (0,)))
            d_s = (p * (dps[n] - row_sc[1:2, :]) * SCALE).astype(BF16)
            dk_sc[r, :] += mm(d_s, qs_sc[...], ((1,), (0,)))
            dq = dq + mm(kt_sc[j], d_s, ((1,), (0,)))
        dq_sc[...] = dq

    def body(j, _):
        chunks((2 * j, 2 * j + 1), False)
        return 0

    lax.fori_loop(0, blk // 2, body, 0)

    @pl.when(blk % 2 == 1)
    def _():
        chunks((blk - 1, blk), True)

    @pl.when(blk % 2 == 0)
    def _():
        chunks((blk,), True)

    rows = pl.ds(blk * BQ, BQ)
    cos_t = cos_ref[rows, :]
    sin_t = -sin_ref[rows, :]
    for n in range(REP):
        dq = dq_sc[:, n * BQ:(n + 1) * BQ].T.astype(BF16).astype(F32)
        out_ref[rows, n * HEAD_DIM:(n + 1) * HEAD_DIM] = rotate(dq, cos_t, sin_t).astype(BF16)

    @pl.when(blk == pl.num_programs(0) - 1)
    def _():
        def one(j, _):
            kr = pl.ds(j * BK, BK)
            dk = dk_sc[kr, :].astype(BF16).astype(F32)
            out_ref[kr, wide:wide + HEAD_DIM] = rotate(dk, cos_ref[kr, :], -sin_ref[kr, :]).astype(BF16)
            out_ref[kr, wide + HEAD_DIM:wide + 2 * HEAD_DIM] = dv_sc[kr, :].astype(BF16)
            return 0

        lax.fori_loop(0, n_chunks, one, 0)


def attn_backward(qkv, d_o, o_t, lse, cos_t, sin_t, kv_local, t):
    seq = qkv.shape[0]
    nq = seq // BQ
    wide = REP * HEAD_DIM
    first_k = kv_local * REP
    flops = 5 * 2 * REP * seq * seq // 2 * HEAD_DIM * 2
    whole = lambda i: (0, 0)
    return pl.pallas_call(
        bwd_kernel,
        grid=(nq,),
        in_specs=[
            pl.BlockSpec((BQ, wide), lambda i: (i, t)),
            pl.BlockSpec((seq, HEAD_DIM), lambda i: (0, first_k + t)),
            pl.BlockSpec((seq, HEAD_DIM), lambda i: (0, first_k + kv_local + t)),
            pl.BlockSpec((BQ, wide), lambda i: (i, t)),
            pl.BlockSpec((1, 1, HEAD_DIM, REP * BQ), lambda i: (t, i, 0, 0)),
            pl.BlockSpec((1, 1, 1, REP * BQ), lambda i: (t, i, 0, 0)),
            pl.BlockSpec((seq, HEAD_DIM), whole),
            pl.BlockSpec((seq, HEAD_DIM), whole),
        ],
        out_specs=pl.BlockSpec((seq, wide + 2 * HEAD_DIM), whole),
        out_shape=jax.ShapeDtypeStruct((seq, wide + 2 * HEAD_DIM), BF16),
        scratch_shapes=[
            pltpu.VMEM((REP * BQ, HEAD_DIM), BF16),
            pltpu.VMEM((HEAD_DIM, REP * BQ), BF16),
            pltpu.VMEM((REP * BQ, HEAD_DIM), BF16),
            pltpu.VMEM((HEAD_DIM, REP * BQ), BF16),
            pltpu.VMEM((seq // BK, HEAD_DIM, BK), BF16),
            pltpu.VMEM((seq, HEAD_DIM), F32),
            pltpu.VMEM((seq, HEAD_DIM), F32),
            pltpu.VMEM((HEAD_DIM, REP * BQ), F32),
            pltpu.VMEM((8, REP * BQ), F32),
        ],
        compiler_params=pltpu.CompilerParams(dimension_semantics=("arbitrary",), vmem_limit_bytes=VMEM_BYTES),
        cost_estimate=cost(flops, 8 * seq * wide * 2),
        name="attn_bwd",
    )(qkv, qkv, qkv, d_o, o_t, lse, cos_t, sin_t)


N_TILE = 1024


def accumulate(acc_sc, weight):
    def tile(n, _):
        cols = pl.ds(pl.multiple_of(n * N_TILE, N_TILE), N_TILE)
        acc_sc[:, cols] += weight(cols)
        return 0

    lax.fori_loop(0, acc_sc.shape[1] // N_TILE, tile, 0)


def fetch_ahead(src, copies):
    @pl.when(src == 0)
    def _():
        for c in copies(0):
            c.start()

    for n in range(4):
        @pl.when(src == n)
        def _():
            if n < 3:
                for c in copies(n + 1):
                    c.start()
            for c in copies(n):
                c.wait()


def out_kernel(idx, *refs):
    pieces, (w_ref, out_ref, cur_sc, acc_sc, sem) = refs[:4], refs[4:]
    src = pl.program_id(0)
    rows = cur_sc.shape[1]

    def copies(n):
        at = pl.ds(pl.multiple_of(idx[0] * rows, rows) if n == 0 else pl.multiple_of(idx[0] % 2 * rows, rows) if n == 1 else 0, rows)
        return [pltpu.make_async_copy(pieces[n].at[at, :], cur_sc.at[n % 2], sem.at[n % 2])]

    fetch_ahead(src, copies)

    @pl.when(src == 0)
    def _():
        acc_sc[...] = jnp.zeros_like(acc_sc)

    accumulate(acc_sc, lambda cols: mm(cur_sc[src % 2], w_ref[:, cols], ((1,), (0,))))

    @pl.when(src == 3)
    def _():
        out_ref[...] = acc_sc[...].astype(BF16)


def single(shape, index):
    return pl.BlockSpec(shape, index, pipeline_mode=pl.Buffered(1))


def out_proj(idx, pieces, w_o, rows):
    wide = pieces[0].shape[1]
    dim = w_o.shape[1]
    return pl.pallas_call(
        out_kernel,
        out_shape=jax.ShapeDtypeStruct((rows, dim), BF16),
        grid_spec=pltpu.PrefetchScalarGridSpec(
            num_scalar_prefetch=1, grid=(4,),
            in_specs=[pl.BlockSpec(memory_space=pl.ANY)] * 4 + [pl.BlockSpec((wide, dim), lambda s, ix: (ix[1 + s], 0))],
            out_specs=pl.BlockSpec((rows, dim), lambda s, ix: (0, 0)),
            scratch_shapes=[pltpu.VMEM((2, rows, wide), BF16), pltpu.VMEM((rows, dim), F32), pltpu.SemaphoreType.DMA((2,))]),
        compiler_params=pltpu.CompilerParams(dimension_semantics=("arbitrary",), vmem_limit_bytes=VMEM_BYTES),
        cost_estimate=cost(8 * rows * dim * wide, 2 * (5 * rows * dim)),
        name="out_proj",
    )(idx, *pieces, w_o)


def dh_kernel(idx, *refs):
    pieces = refs[:8]
    wq_ref, wk_ref, wv_ref, x_hbm, lnw_ref, dx_ref, dw_ref, cur_sc, acc_sc, x_ref, dx_sc, sem, piece_sem, x_sem = refs[8:]
    src = pl.program_id(0)
    wide = wq_ref.shape[1]
    each = wide // 2
    rows = cur_sc.shape[1]
    x_copy = pltpu.make_async_copy(x_hbm, x_ref, x_sem)

    def copies(n):
        at = pl.ds(pl.multiple_of(idx[0] * rows, rows) if n < 2 else 0, rows)
        out = []
        for t in range(2):
            piece = pieces[2 * n + t]
            spans = [(0, each, t * each)] + [(each + part * HEAD_DIM, HEAD_DIM, wide + (2 * part + t) * HEAD_DIM) for part in range(2)]
            for start, size, to in spans:
                out.append(pltpu.make_async_copy(piece.at[at, start:start + size], cur_sc.at[n % 2, :, to:to + size],
                                                 piece_sem.at[n % 2]))
        return out

    fetch_ahead(src, copies)

    @pl.when(src == 0)
    def _():
        x_copy.start()
        acc_sc[...] = jnp.zeros_like(acc_sc)

    both = wide + 2 * HEAD_DIM
    cur = src % 2
    accumulate(acc_sc, lambda cols: mm(cur_sc[cur, :, :wide], wq_ref[cols, :], ((1,), (1,)))
               + mm(cur_sc[cur, :, wide:both], wk_ref[cols, :], ((1,), (1,)))
               + mm(cur_sc[cur, :, both:], wv_ref[cols, :], ((1,), (1,))))

    @pl.when(src == 3)
    def _():
        x_copy.wait()
        blk = dx_sc.shape[1]
        n_blk = x_ref.shape[0] // blk
        weight = lnw_ref[...].astype(F32)
        dw_ref[...] = jnp.zeros_like(dw_ref)

        def put(n, slot):
            return pltpu.make_async_copy(dx_sc.at[slot], dx_ref.at[pl.ds(n * blk, blk), :], sem.at[slot])

        def one(n, _):
            slot = n % 2
            rows = pl.ds(n * blk, blk)

            @pl.when(n >= 2)
            def _():
                put(n - 2, slot).wait()

            xf = x_ref[rows, :].astype(F32)
            mean = jnp.mean(xf, axis=-1, keepdims=True)
            cen = xf - mean
            var = jnp.mean(cen * cen, axis=-1, keepdims=True)
            rstd = lax.rsqrt(var + LN_EPS)
            xhat = cen * rstd
            dh = acc_sc[rows, :]
            dw_ref[...] += jnp.sum(dh * xhat, axis=0, keepdims=True)
            dxh = dh * weight
            mean_d = jnp.mean(dxh, axis=-1, keepdims=True)
            mean_dx = jnp.mean(dxh * xhat, axis=-1, keepdims=True)
            dx_sc[slot] = (rstd * (dxh - mean_d - xhat * mean_dx)).astype(BF16)
            put(n, slot).start()
            return 0

        lax.fori_loop(0, n_blk, one, 0)
        for n in range(n_blk - 2, n_blk):
            put(n, n % 2).wait()


def hidden_grad(idx, pieces, w_q, w_k, w_v, x, ln_w, n_dev):
    rows, dim = x.shape
    cols = pieces[0].shape[1]
    cq, ck = w_q.shape[1] // n_dev, w_k.shape[1] // n_dev
    const = lambda s, ix: (0, 0)
    head = lambda s, ix: (0, ix[1 + s])
    blk = 128
    return pl.pallas_call(
        dh_kernel,
        out_shape=(jax.ShapeDtypeStruct((rows, dim), BF16), jax.ShapeDtypeStruct((1, dim), F32)),
        grid_spec=pltpu.PrefetchScalarGridSpec(
            num_scalar_prefetch=1, grid=(4,),
            in_specs=[pl.BlockSpec(memory_space=pl.ANY)] * 8
            + [pl.BlockSpec((dim, cq), head), pl.BlockSpec((dim, ck), head), pl.BlockSpec((dim, ck), head),
               pl.BlockSpec(memory_space=pl.ANY), pl.BlockSpec((1, dim), const)],
            out_specs=(pl.BlockSpec(memory_space=pl.ANY), pl.BlockSpec((1, dim), const)),
            scratch_shapes=[pltpu.VMEM((2, rows, 2 * cols), BF16), pltpu.VMEM((rows, dim), F32),
                            pltpu.VMEM((rows, dim), BF16), pltpu.VMEM((2, blk, dim), BF16),
                            pltpu.SemaphoreType.DMA((2,)), pltpu.SemaphoreType.DMA((2,)), pltpu.SemaphoreType.DMA]),
        compiler_params=pltpu.CompilerParams(dimension_semantics=("arbitrary",), vmem_limit_bytes=VMEM_BYTES),
        cost_estimate=cost(16 * rows * dim * cols, 2 * (2 * rows * dim + 8 * cols * (rows + dim))),
        name="hidden_grad",
    )(idx, *pieces, w_q, w_k, w_v, x, ln_w)


def reserve(*shapes):
    return pl.pallas_call(
        lambda *refs: None,
        out_shape=tuple(jax.ShapeDtypeStruct(s, BF16) for s in shapes),
        out_specs=tuple(pl.BlockSpec(memory_space=pl.ANY) for _ in shapes),
        cost_estimate=cost(1, 1),
        name="reserve",
    )()


def dw_kernel(idx, *refs):
    hs, refs = refs[:4], refs[4:]
    n = len(refs) - 8
    rows = hs[0].shape[0]
    grs, (q_ref, k_ref, v_ref, piece_ref, gr_sc) = refs[:n], refs[-5:]
    wide = q_ref.shape[1] // n
    cols = piece_ref.shape[1]

    @pl.when(pl.program_id(0) == 0)
    def _():
        for b in range(4):
            to = slice(b * rows, (b + 1) * rows)
            at = pl.ds(idx[1 + b] * rows, rows)
            for t, gr in enumerate(grs):
                gr_sc[to, t * wide:(t + 1) * wide] = gr[at, :wide]
                for part in range(2):
                    start = n * wide + part * n * HEAD_DIM + t * HEAD_DIM
                    gr_sc[to, start:start + HEAD_DIM] = gr[at, wide + part * HEAD_DIM:wide + (part + 1) * HEAD_DIM]

    for start in range(0, cols, 256):
        stop = min(start + 256, cols)
        val = sum(mm(h[...], gr_sc[b * rows:(b + 1) * rows, start:stop], ((0,), (0,))) for b, h in enumerate(hs))
        piece_ref[:, start:stop] = val.astype(BF16)
    q_ref[...] = piece_ref[:, :n * wide]
    k_ref[...] = piece_ref[:, n * wide:n * (wide + HEAD_DIM)]
    v_ref[...] = piece_ref[:, n * (wide + HEAD_DIM):]


def weight_grad(idx, hs, grs, bufs):
    (both, dim), n = hs[0].shape, len(grs)
    rows = both // 2
    seq = 2 * both
    cols = n * grs[0].shape[1]
    wide = REP * HEAD_DIM * n
    blk = 512
    there = lambda i, ix: (i, ix[0])
    flops = 2 * seq * dim * cols
    return pl.pallas_call(
        dw_kernel,
        out_shape=tuple(jax.ShapeDtypeStruct(b.shape, BF16) for b in bufs) + (jax.ShapeDtypeStruct((dim, cols), BF16),),
        grid_spec=pltpu.PrefetchScalarGridSpec(
            num_scalar_prefetch=1, grid=(dim // blk,),
            in_specs=[pl.BlockSpec((rows, blk), lambda i, ix: (0, i))] * 2 + [pl.BlockSpec((rows, blk), lambda i, ix: (1, i))] * 2
            + [pl.BlockSpec((seq, cols // n), lambda i, ix: (0, 0), pipeline_mode=pl.Buffered(1)) for _ in grs]
            + [pl.BlockSpec(memory_space=pl.ANY)] * 3,
            out_specs=(pl.BlockSpec((blk, wide), there), pl.BlockSpec((blk, n * HEAD_DIM), there),
                       pl.BlockSpec((blk, n * HEAD_DIM), there), pl.BlockSpec((blk, cols), lambda i, ix: (i, 0))),
            scratch_shapes=[pltpu.VMEM((seq, cols), BF16)]),
        input_output_aliases={5 + n: 0, 6 + n: 1, 7 + n: 2},
        compiler_params=pltpu.CompilerParams(dimension_semantics=("arbitrary",), vmem_limit_bytes=VMEM_BYTES),
        cost_estimate=cost(flops, 2 * (seq * dim + seq * cols + 2 * dim * cols)),
        name="weight_grad",
    )(idx, *hs, *grs, *bufs)


def dwo_kernel(idx, o_ref, *refs):
    gs, (buf_ref, out_ref, piece_ref) = refs[:4], refs[4:]
    rows = gs[0].shape[0]
    for start in range(0, piece_ref.shape[1], 256):
        cols = slice(start, start + 256)
        val = sum(mm(o_ref[pl.ds(idx[1 + b] * rows, rows), :], g[:, cols], ((0,), (0,))) for b, g in enumerate(gs))
        piece_ref[:, cols] = val.astype(BF16)
    out_ref[...] = piece_ref[...]


def out_weight_grad(idx, o, gs, buf):
    seq, wide = o.shape
    rows, dim = gs[0].shape
    blk = 512
    return pl.pallas_call(
        dwo_kernel,
        out_shape=(jax.ShapeDtypeStruct(buf.shape, BF16), jax.ShapeDtypeStruct((wide, dim), BF16)),
        grid_spec=pltpu.PrefetchScalarGridSpec(
            num_scalar_prefetch=1, grid=(dim // blk,),
            in_specs=[single((seq, wide), lambda i, ix: (0, 0))]
            + [pl.BlockSpec((rows, blk), lambda i, ix: (0, i))] * 4 + [pl.BlockSpec(memory_space=pl.ANY)],
            out_specs=(pl.BlockSpec((wide, blk), lambda i, ix: (ix[0], i)), pl.BlockSpec((wide, blk), lambda i, ix: (0, i)))),
        input_output_aliases={6: 0},
        compiler_params=pltpu.CompilerParams(dimension_semantics=("arbitrary",), vmem_limit_bytes=VMEM_BYTES),
        cost_estimate=cost(2 * seq * wide * dim, 2 * (seq * dim + seq * wide + 2 * wide * dim)),
        name="out_weight_grad",
    )(idx, o, *gs, buf)


def place_kernel(idx, piece_ref, *refs):
    q_ref, k_ref, v_ref = refs[-3:]
    wide, one = q_ref.shape[1], k_ref.shape[1]
    q_ref[...] = piece_ref[:, :wide]
    k_ref[...] = piece_ref[:, wide:wide + one]
    v_ref[...] = piece_ref[:, wide + one:]


def place(idx, piece, bufs):
    dim, cols = piece.shape
    one = cols // (REP + 2)
    blk = 512
    there = lambda i, ix: (i, ix[0])
    return pl.pallas_call(
        place_kernel,
        out_shape=tuple(jax.ShapeDtypeStruct(b.shape, BF16) for b in bufs),
        grid_spec=pltpu.PrefetchScalarGridSpec(
            num_scalar_prefetch=1, grid=(dim // blk,),
            in_specs=[pl.BlockSpec((blk, cols), lambda i, ix: (i, 0))] + [pl.BlockSpec(memory_space=pl.ANY)] * 3,
            out_specs=(pl.BlockSpec((blk, REP * one), there), pl.BlockSpec((blk, one), there),
                       pl.BlockSpec((blk, one), there))),
        input_output_aliases={2: 0, 3: 1, 4: 2},
        compiler_params=pltpu.CompilerParams(dimension_semantics=("arbitrary",)),
        cost_estimate=cost(4 * dim * cols, 4 * dim * cols),
        name="place",
    )(idx, piece, *bufs)


def solution(mesh):
    n_dev = mesh.shape['sp']
    row_spec = P(('dp', 'sp'), None)
    pos_spec = P(('dp', 'sp'))
    full_spec = P(None, None)
    grad_spec = P('dp', None)

    def over_chip(val):
        return lax.ppermute(val, 'sp', [(i, i ^ 2) for i in range(n_dev)])

    def over_core(val):
        return lax.ppermute(val, 'sp', [(i, i ^ 1) for i in range(n_dev)])

    def layer(hidden, positions, d_attn, ln_weight, w_q, w_k, w_v, w_o):
        rows, dim = hidden.shape
        seq = rows * n_dev
        kv_local = w_k.shape[1] // HEAD_DIM // n_dev
        cq = w_q.shape[1] // n_dev
        me = lax.axis_index('sp')
        chip, core = me // 2, me % 2
        hb = 2 * core + chip
        hbs = [hb, hb ^ 1, hb ^ 2, hb ^ 3]
        toks = [me, me ^ 2, me ^ 1, me ^ 3]

        pos_par = over_chip(positions)
        pos_src = (positions, over_core(positions), pos_par, over_core(pos_par))
        pos = jnp.concatenate([lax.select_n(me ^ b, *pos_src) for b in range(n_dev)])
        ln_row = ln_weight.reshape(1, dim)
        x_par = over_chip(hidden)
        g_par = over_chip(d_attn)
        x_sib = over_core(hidden)
        g_sib = over_core(d_attn)

        inv_freq = ROPE_BASE ** (-jnp.arange(0, HEAD_DIM, 2, dtype=F32) / HEAD_DIM)
        angles = pos.astype(F32)[:, None] * jnp.repeat(inv_freq, 2)[None, :]
        cos_t = jnp.cos(angles)
        sin_t = jnp.sin(angles) * jnp.where(jnp.arange(HEAD_DIM) % 2 == 0, -1.0, 1.0)[None, :]

        x_sp = over_core(x_par)
        g_sp = over_core(g_par)

        def pair(b):
            return jnp.stack([hb, toks[b], toks[b + 2]]).astype(jnp.int32)

        h_mine, qkv = qkv_blocks(pair(0), (hidden, x_sib), ln_row, w_q, w_k, w_v, cos_t, sin_t, seq, n_dev, None)
        h_far, qkv = qkv_blocks(pair(1), (x_par, x_sp), ln_row, w_q, w_k, w_v, cos_t, sin_t, seq, n_dev, qkv)
        hs = (h_mine, h_far, h_mine, h_far)
        o_own, o_t, lse = attn_forward(qkv, kv_local)

        wo_t = transpose_rows(hb.reshape(1).astype(jnp.int32), w_o, n_dev)
        gs = [d_attn, g_par, g_sib, g_sp]
        d_o = do_blocks(pair(0), (d_attn, g_sib), wo_t, seq, None)
        d_o = do_blocks(pair(1), (g_par, g_sp), wo_t, seq, d_o)

        def own_rows(val, dev):
            return lax.dynamic_slice_in_dim(val, dev * rows, rows, 0)

        o_par = over_chip(lax.dynamic_slice_in_dim(o_own, (chip ^ 1) * 2 * rows, 2 * rows, 0))
        sources = jnp.stack([me, *hbs]).astype(jnp.int32)
        o_tok = [o_own, o_par, over_core(own_rows(o_own, me ^ 1)), over_core(own_rows(o_par, core ^ 1))]
        attn_out = out_proj(sources, o_tok, w_o, rows)

        def blocks(where):
            return jnp.stack([where, *toks]).astype(jnp.int32)

        d_w_o, *d_w = reserve(w_o.shape, w_q.shape, w_k.shape, w_v.shape)
        d_w_o, piece = out_weight_grad(blocks(hbs[0]), o_own, gs, d_w_o)
        far = over_chip(piece)
        for b, val in ((hbs[2], over_core(piece)), (hbs[1], far), (hbs[3], over_core(far))):
            d_w_o = lax.dynamic_update_slice_in_dim(d_w_o, val, b * cq, 0)

        gr = []
        for t in range(kv_local):
            gr.append(attn_backward(qkv, d_o, o_t, lse, cos_t, sin_t, kv_local, t))
        gr_par = [over_chip(val) for val in gr]

        def col(val):
            return val.reshape(1).astype(jnp.int32)

        *d_w, piece = weight_grad(blocks(hbs[0]), hs, gr, d_w)
        piece = over_core(piece)
        d_w = place(col(hbs[2]), piece, d_w)
        gr_tok = [gr, gr_par, [], []]
        for t in range(kv_local):
            gr_tok[2].append(over_core(own_rows(gr[t], me ^ 1)))
            gr_tok[3].append(over_core(own_rows(gr_par[t], me ^ 1)))
            *d_w, piece = weight_grad(blocks(hbs[1] * kv_local + t), hs, (gr_par[t],), d_w)
            piece = over_core(piece)
            d_w = place(col(hbs[3] * kv_local + t), piece, d_w)
        d_hid, d_lnw = hidden_grad(sources, [val for pair in gr_tok for val in pair], w_q, w_k, w_v, hidden, ln_row, n_dev)
        d_lnw = d_lnw + over_core(d_lnw)
        d_lnw = d_lnw + over_chip(d_lnw)
        return (attn_out, d_hid, d_lnw.reshape(dim).astype(BF16), *d_w, d_w_o)

    return jax.shard_map(layer, mesh=mesh,
                         in_specs=(row_spec, pos_spec, row_spec, P(None), full_spec, full_spec, full_spec, full_spec),
                         out_specs=(row_spec, row_spec, P('dp'), grad_spec, grad_spec, grad_spec, grad_spec),
                         check_vma=False)
```

```python
import functools
import math
import jax
import jax.numpy as jnp
from jax import lax
from jax.experimental import pallas as pl
from jax.experimental.pallas import tpu as pltpu
from jax.sharding import PartitionSpec as P

HEAD_DIM = 128
LN_EPS = 1e-5
ROPE_BASE = 10000.0
REP = 3
BQ = 256
BK = 256
ROWS = 512
LOG2E = math.log2(math.e)
SCALE = HEAD_DIM ** -0.5
VMEM_BYTES = 60 * 1024 * 1024
F32 = jnp.float32
BF16 = jnp.bfloat16


def cost(flops, nbytes):
    return pl.CostEstimate(flops=int(flops), bytes_accessed=int(nbytes), transcendentals=0)


def mm(lhs, rhs, dims):
    return lax.dot_general(lhs, rhs, (dims, ((), ())), preferred_element_type=F32)


def rotate(val, cos_t, sin_t):
    lane = lax.broadcasted_iota(jnp.int32, val.shape, 1)
    swapped = jnp.where(lane % 2 == 0, pltpu.roll(val, HEAD_DIM - 1, 1), pltpu.roll(val, 1, 1))
    return val * cos_t + swapped * sin_t


def pick(pair, sc):
    for n, ref in enumerate(pair):
        @pl.when(pl.program_id(0) == n)
        def _():
            sc[...] = ref[...]


def pair_specs(shape, per):
    return [pl.BlockSpec(shape, lambda p, i, ix: (jnp.where(p == 0, i, per - 1), 0)),
            pl.BlockSpec(shape, lambda p, i, ix: (jnp.where(p == 1, i, 0), 0))]


def qkv_kernel(idx, xa_ref, xb_ref, lnw_ref, wq_ref, wk_ref, wv_ref, cos_ref, sin_ref, *rest):
    h_ref, qkv_ref, x_sc = rest[-3:]
    pick((xa_ref, xb_ref), x_sc)
    weight = lnw_ref[...].astype(F32)
    nq = wq_ref.shape[1]
    nk = wk_ref.shape[1]
    step = 2 * HEAD_DIM
    for sub in range(ROWS // BQ):
        rows = slice(sub * BQ, (sub + 1) * BQ)
        xf = x_sc[rows, :].astype(F32)
        mean = jnp.mean(xf, axis=-1, keepdims=True)
        cen = xf - mean
        var = jnp.mean(cen * cen, axis=-1, keepdims=True)
        h = (cen * lax.rsqrt(var + LN_EPS) * weight).astype(BF16)
        h_ref[rows, :] = h
        cos_t = cos_ref[rows, :]
        sin_t = sin_ref[rows, :]
        for start in range(0, nq + nk, step):
            w = wq_ref[:, start:start + step] if start < nq else wk_ref[:, start - nq:start - nq + step]
            val = mm(h, w, ((1,), (0,)))
            for n in range(2):
                at = start + n * HEAD_DIM
                part = val[:, n * HEAD_DIM:(n + 1) * HEAD_DIM]
                qkv_ref[rows, at:at + HEAD_DIM] = rotate(part, cos_t, sin_t).astype(BF16)
        qkv_ref[rows, nq + nk:] = mm(h, wv_ref[...], ((1,), (0,))).astype(BF16)


def qkv_blocks(idx, xs, ln_w, w_q, w_k, w_v, cos_t, sin_t, seq, n_dev, prev):
    rows, dim = xs[0].shape
    cq, ck = w_q.shape[1] // n_dev, w_k.shape[1] // n_dev
    per = rows // ROWS
    head = lambda p, i, ix: (0, ix[0])
    here = lambda p, i, ix: (ix[1 + p] * per + i, 0)
    in_specs = pair_specs((ROWS, dim), per) + [
        pl.BlockSpec((1, dim), lambda p, i, ix: (0, 0)),
        pl.BlockSpec((dim, cq), head),
        pl.BlockSpec((dim, ck), head),
        pl.BlockSpec((dim, ck), head),
        pl.BlockSpec((ROWS, HEAD_DIM), here),
        pl.BlockSpec((ROWS, HEAD_DIM), here),
    ]
    args = [idx, *xs, ln_w, w_q, w_k, w_v, cos_t, sin_t]
    aliases = {}
    if prev is not None:
        in_specs.append(pl.BlockSpec(memory_space=pl.ANY))
        args.append(prev)
        aliases = {9: 1}
    cols = cq + 2 * ck
    return pl.pallas_call(
        qkv_kernel,
        out_shape=(jax.ShapeDtypeStruct((2 * rows, dim), BF16), jax.ShapeDtypeStruct((seq, cols), BF16)),
        grid_spec=pltpu.PrefetchScalarGridSpec(
            num_scalar_prefetch=1, grid=(2, per), in_specs=in_specs,
            out_specs=(pl.BlockSpec((ROWS, dim), lambda p, i, ix: (p * per + i, 0)), pl.BlockSpec((ROWS, cols), here)),
            scratch_shapes=[pltpu.VMEM((ROWS, dim), BF16)]),
        input_output_aliases=aliases,
        compiler_params=pltpu.CompilerParams(dimension_semantics=("arbitrary", "arbitrary"), vmem_limit_bytes=VMEM_BYTES),
        cost_estimate=cost(4 * rows * dim * cols, 2 * (4 * rows * dim + dim * cols + 2 * rows * cols)),
        name="ln_qkv",
    )(*args)


def wo_t_kernel(idx, wo_ref, out_ref):
    out_ref[...] = wo_ref[...].astype(F32).T.astype(BF16)


def transpose_rows(idx, w_o, n_dev):
    ce, dim = w_o.shape[0] // n_dev, w_o.shape[1]
    blk = 512
    return pl.pallas_call(
        wo_t_kernel,
        out_shape=jax.ShapeDtypeStruct((dim, ce), BF16),
        grid_spec=pltpu.PrefetchScalarGridSpec(
            num_scalar_prefetch=1, grid=(dim // blk,),
            in_specs=[pl.BlockSpec((ce, blk), lambda i, ix: (ix[0], i))],
            out_specs=pl.BlockSpec((blk, ce), lambda i, ix: (i, 0))),
        compiler_params=pltpu.CompilerParams(dimension_semantics=("arbitrary",)),
        cost_estimate=cost(4 * ce * dim, 4 * ce * dim),
        name="wo_t",
    )(idx, w_o)


def do_kernel(idx, ga_ref, gb_ref, wo_ref, *rest):
    do_ref, g_sc = rest[-2:]
    pick((ga_ref, gb_ref), g_sc)
    do_ref[...] = mm(g_sc[...], wo_ref[...], ((1,), (0,))).astype(BF16)


def do_blocks(idx, gs, wo_t, seq, prev):
    rows, dim = gs[0].shape
    ce = wo_t.shape[1]
    per = rows // ROWS
    in_specs = pair_specs((ROWS, dim), per) + [pl.BlockSpec((dim, ce), lambda p, i, ix: (0, 0))]
    args = [idx, *gs, wo_t]
    aliases = {}
    if prev is not None:
        in_specs.append(pl.BlockSpec(memory_space=pl.ANY))
        args.append(prev)
        aliases = {4: 0}
    return pl.pallas_call(
        do_kernel,
        out_shape=jax.ShapeDtypeStruct((seq, ce), BF16),
        grid_spec=pltpu.PrefetchScalarGridSpec(
            num_scalar_prefetch=1, grid=(2, per), in_specs=in_specs,
            out_specs=pl.BlockSpec((ROWS, ce), lambda p, i, ix: (ix[1 + p] * per + i, 0)),
            scratch_shapes=[pltpu.VMEM((ROWS, dim), BF16)]),
        input_output_aliases=aliases,
        compiler_params=pltpu.CompilerParams(dimension_semantics=("arbitrary", "arbitrary"), vmem_limit_bytes=VMEM_BYTES),
        cost_estimate=cost(4 * rows * dim * ce, 2 * (2 * rows * dim + dim * ce + 2 * rows * ce)),
        name="d_o",
    )(*args)


def stack_heads(val):
    return jnp.concatenate([val[:, n * HEAD_DIM:(n + 1) * HEAD_DIM] for n in range(REP)], axis=0)


def flip(val):
    return val.astype(F32).T.astype(BF16)


def causal(shape):
    return lax.broadcasted_iota(jnp.int32, shape, 0) <= lax.broadcasted_iota(jnp.int32, shape, 1) % BQ


def fwd_kernel(q_ref, k_ref, v_ref, o_ref, ot_ref, lse_ref, qt_sc, vt_sc, acc_sc, ml_sc, s_sc):
    blk = pl.program_id(1)
    n_chunks = k_ref.shape[0] // BK
    pairs = blk // 2

    @pl.when(blk == 0)
    def _():
        def one(j, _):
            vt_sc[j] = flip(v_ref[pl.ds(j * BK, BK), :])
            return 0

        lax.fori_loop(0, n_chunks, one, 0)

    qt_sc[...] = flip(stack_heads(q_ref[...]))

    def score(j):
        return mm(k_ref[pl.ds(j * BK, BK), :], qt_sc[...], ((1,), (0,))) * (SCALE * LOG2E)

    def ahead(pair):
        for n in range(2):
            nxt = score(2 * pair + n)
            s_sc[n] = nxt
            ml_sc[2 + n:3 + n, :] = jnp.max(nxt, axis=0, keepdims=True)

    def update(m_new, js, scores, first):
        if first:
            total, acc = 0.0, 0.0
        else:
            alpha = jnp.exp2(ml_sc[0:1, :] - m_new)
            total, acc = ml_sc[1:2, :] * alpha, acc_sc[...] * alpha
        for j, s in zip(js, scores):
            p = jnp.exp2(s - m_new)
            total = total + jnp.sum(p, axis=0, keepdims=True)
            acc = acc + mm(vt_sc[j], p.astype(BF16), ((1,), (0,)))
        ml_sc[0:1, :] = m_new
        ml_sc[1:2, :] = total
        acc_sc[...] = acc

    def last_chunks(js):
        scores = [score(j) for j in js]
        scores[-1] = jnp.where(causal(scores[-1].shape), scores[-1], -jnp.inf)
        m_new = functools.reduce(jnp.maximum, [jnp.max(s, axis=0, keepdims=True) for s in scores])
        ahead(0)
        update(m_new, js, scores, True)

    def held(pair, more):
        m_new = jnp.maximum(ml_sc[0:1, :], jnp.maximum(ml_sc[2:3, :], ml_sc[3:4, :]))
        scores = [s_sc[n] for n in range(2)]
        if more:
            ahead(pair + 1)
        update(m_new, (2 * pair, 2 * pair + 1), scores, False)

    @pl.when(blk % 2 == 1)
    def _():
        last_chunks((blk - 1, blk))

    @pl.when(blk % 2 == 0)
    def _():
        last_chunks((blk,))

    def body(pair, _):
        held(pair, True)
        return 0

    lax.fori_loop(0, pairs - 1, body, 0)

    @pl.when(pairs > 0)
    def _():
        held(pairs - 1, False)

    total = ml_sc[1:2, :]
    out_t = acc_sc[...] / total
    ot_ref[0, 0] = out_t
    lse_ref[0, 0] = ml_sc[0:1, :] + jnp.log2(total)
    for n in range(REP):
        o_ref[:, n * HEAD_DIM:(n + 1) * HEAD_DIM] = out_t[:, n * BQ:(n + 1) * BQ].T.astype(BF16)


def attn_forward(qkv, kv_local):
    seq = qkv.shape[0]
    nq = seq // BQ
    wide = REP * HEAD_DIM
    first_k = kv_local * REP
    flops = 2 * 2 * kv_local * REP * seq * seq // 2 * HEAD_DIM * 2
    return pl.pallas_call(
        fwd_kernel,
        grid=(kv_local, nq),
        in_specs=[
            pl.BlockSpec((BQ, wide), lambda t, i: (i, t)),
            pl.BlockSpec((seq, HEAD_DIM), lambda t, i: (0, first_k + t)),
            pl.BlockSpec((seq, HEAD_DIM), lambda t, i: (0, first_k + kv_local + t)),
        ],
        out_specs=(
            pl.BlockSpec((BQ, wide), lambda t, i: (i, t)),
            pl.BlockSpec((1, 1, HEAD_DIM, REP * BQ), lambda t, i: (t, i, 0, 0)),
            pl.BlockSpec((1, 1, 1, REP * BQ), lambda t, i: (t, i, 0, 0)),
        ),
        out_shape=(
            jax.ShapeDtypeStruct((seq, kv_local * wide), BF16),
            jax.ShapeDtypeStruct((kv_local, nq, HEAD_DIM, REP * BQ), F32),
            jax.ShapeDtypeStruct((kv_local, nq, 1, REP * BQ), F32),
        ),
        scratch_shapes=[
            pltpu.VMEM((HEAD_DIM, REP * BQ), BF16),
            pltpu.VMEM((seq // BK, HEAD_DIM, BK), BF16),
            pltpu.VMEM((HEAD_DIM, REP * BQ), F32),
            pltpu.VMEM((8, REP * BQ), F32),
            pltpu.VMEM((2, BK, REP * BQ), F32),
        ],
        compiler_params=pltpu.CompilerParams(dimension_semantics=("arbitrary", "arbitrary"), vmem_limit_bytes=VMEM_BYTES),
        cost_estimate=cost(flops, 4 * seq * wide * kv_local * 2),
        name="attn_fwd",
    )(qkv, qkv, qkv)


def bwd_kernel(q_ref, k_ref, v_ref, do_ref, ot_ref, lse_ref, cos_ref, sin_ref, out_ref,
               qs_sc, qt_sc, ds_sc, dt_sc, kt_sc, dk_sc, dv_sc, dq_sc, row_sc):
    blk = pl.program_id(0)
    wide = REP * HEAD_DIM
    n_chunks = k_ref.shape[0] // BK

    @pl.when(blk == 0)
    def _():
        def one(j, _):
            rows = pl.ds(j * BK, BK)
            kt_sc[j] = flip(k_ref[rows, :])
            dk_sc[rows, :] = jnp.zeros((BK, HEAD_DIM), F32)
            dv_sc[rows, :] = jnp.zeros((BK, HEAD_DIM), F32)
            return 0

        lax.fori_loop(0, n_chunks, one, 0)

    q_all = stack_heads(q_ref[...])
    do_all = stack_heads(do_ref[...])
    qs_sc[...] = q_all
    qt_sc[...] = flip(q_all)
    ds_sc[...] = do_all
    do_t = do_all.astype(F32).T
    dt_sc[...] = do_t.astype(BF16)
    row_sc[0:1, :] = lse_ref[0, 0]
    row_sc[1:2, :] = jnp.sum(ot_ref[0, 0] * do_t, axis=0, keepdims=True)
    dq_sc[...] = jnp.zeros_like(dq_sc)

    def chunks(js, masked):
        rows = [pl.ds(j * BK, BK) for j in js]
        scores = [mm(k_ref[r, :], qt_sc[...], ((1,), (0,))) * (SCALE * LOG2E) for r in rows]
        dps = [mm(v_ref[r, :], dt_sc[...], ((1,), (0,))) for r in rows]
        dq = dq_sc[...]
        for n, (j, r) in enumerate(zip(js, rows)):
            p = jnp.exp2(scores[n] - row_sc[0:1, :])
            if masked and n == len(js) - 1:
                p = jnp.where(causal(p.shape), p, 0.0)
            dv_sc[r, :] += mm(p.astype(BF16), ds_sc[...], ((1,), (0,)))
            d_s = (p * (dps[n] - row_sc[1:2, :]) * SCALE).astype(BF16)
            dk_sc[r, :] += mm(d_s, qs_sc[...], ((1,), (0,)))
            dq = dq + mm(kt_sc[j], d_s, ((1,), (0,)))
        dq_sc[...] = dq

    def body(j, _):
        chunks((2 * j, 2 * j + 1), False)
        return 0

    lax.fori_loop(0, blk // 2, body, 0)

    @pl.when(blk % 2 == 1)
    def _():
        chunks((blk - 1, blk), True)

    @pl.when(blk % 2 == 0)
    def _():
        chunks((blk,), True)

    rows = pl.ds(blk * BQ, BQ)
    cos_t = cos_ref[rows, :]
    sin_t = -sin_ref[rows, :]
    for n in range(REP):
        dq = dq_sc[:, n * BQ:(n + 1) * BQ].T.astype(BF16).astype(F32)
        out_ref[rows, n * HEAD_DIM:(n + 1) * HEAD_DIM] = rotate(dq, cos_t, sin_t).astype(BF16)

    @pl.when(blk == pl.num_programs(0) - 1)
    def _():
        def one(j, _):
            kr = pl.ds(j * BK, BK)
            dk = dk_sc[kr, :].astype(BF16).astype(F32)
            out_ref[kr, wide:wide + HEAD_DIM] = rotate(dk, cos_ref[kr, :], -sin_ref[kr, :]).astype(BF16)
            out_ref[kr, wide + HEAD_DIM:wide + 2 * HEAD_DIM] = dv_sc[kr, :].astype(BF16)
            return 0

        lax.fori_loop(0, n_chunks, one, 0)


def attn_backward(qkv, d_o, o_t, lse, cos_t, sin_t, kv_local, t):
    seq = qkv.shape[0]
    nq = seq // BQ
    wide = REP * HEAD_DIM
    first_k = kv_local * REP
    flops = 5 * 2 * REP * seq * seq // 2 * HEAD_DIM * 2
    whole = lambda i: (0, 0)
    return pl.pallas_call(
        bwd_kernel,
        grid=(nq,),
        in_specs=[
            pl.BlockSpec((BQ, wide), lambda i: (i, t)),
            pl.BlockSpec((seq, HEAD_DIM), lambda i: (0, first_k + t)),
            pl.BlockSpec((seq, HEAD_DIM), lambda i: (0, first_k + kv_local + t)),
            pl.BlockSpec((BQ, wide), lambda i: (i, t)),
            pl.BlockSpec((1, 1, HEAD_DIM, REP * BQ), lambda i: (t, i, 0, 0)),
            pl.BlockSpec((1, 1, 1, REP * BQ), lambda i: (t, i, 0, 0)),
            pl.BlockSpec((seq, HEAD_DIM), whole),
            pl.BlockSpec((seq, HEAD_DIM), whole),
        ],
        out_specs=pl.BlockSpec((seq, wide + 2 * HEAD_DIM), whole),
        out_shape=jax.ShapeDtypeStruct((seq, wide + 2 * HEAD_DIM), BF16),
        scratch_shapes=[
            pltpu.VMEM((REP * BQ, HEAD_DIM), BF16),
            pltpu.VMEM((HEAD_DIM, REP * BQ), BF16),
            pltpu.VMEM((REP * BQ, HEAD_DIM), BF16),
            pltpu.VMEM((HEAD_DIM, REP * BQ), BF16),
            pltpu.VMEM((seq // BK, HEAD_DIM, BK), BF16),
            pltpu.VMEM((seq, HEAD_DIM), F32),
            pltpu.VMEM((seq, HEAD_DIM), F32),
            pltpu.VMEM((HEAD_DIM, REP * BQ), F32),
            pltpu.VMEM((8, REP * BQ), F32),
        ],
        compiler_params=pltpu.CompilerParams(dimension_semantics=("arbitrary",), vmem_limit_bytes=VMEM_BYTES),
        cost_estimate=cost(flops, 8 * seq * wide * 2),
        name="attn_bwd",
    )(qkv, qkv, qkv, d_o, o_t, lse, cos_t, sin_t)


N_TILE = 1024


def accumulate(acc_sc, weight):
    def tile(n, _):
        cols = pl.ds(pl.multiple_of(n * N_TILE, N_TILE), N_TILE)
        acc_sc[:, cols] += weight(cols)
        return 0

    lax.fori_loop(0, acc_sc.shape[1] // N_TILE, tile, 0)


def fetch_ahead(src, copies):
    @pl.when(src == 0)
    def _():
        for c in copies(0):
            c.start()

    for n in range(4):
        @pl.when(src == n)
        def _():
            if n < 3:
                for c in copies(n + 1):
                    c.start()
            for c in copies(n):
                c.wait()


def out_kernel(idx, *refs):
    pieces, (w_ref, out_ref, cur_sc, acc_sc, sem) = refs[:4], refs[4:]
    src = pl.program_id(0)
    rows = cur_sc.shape[1]

    def copies(n):
        at = pl.ds(pl.multiple_of(idx[0] * rows, rows) if n == 0 else pl.multiple_of(idx[0] % 2 * rows, rows) if n == 1 else 0, rows)
        return [pltpu.make_async_copy(pieces[n].at[at, :], cur_sc.at[n % 2], sem.at[n % 2])]

    fetch_ahead(src, copies)

    @pl.when(src == 0)
    def _():
        acc_sc[...] = jnp.zeros_like(acc_sc)

    accumulate(acc_sc, lambda cols: mm(cur_sc[src % 2], w_ref[:, cols], ((1,), (0,))))

    @pl.when(src == 3)
    def _():
        out_ref[...] = acc_sc[...].astype(BF16)


def single(shape, index):
    return pl.BlockSpec(shape, index, pipeline_mode=pl.Buffered(1))


def out_proj(idx, pieces, w_o, rows):
    wide = pieces[0].shape[1]
    dim = w_o.shape[1]
    return pl.pallas_call(
        out_kernel,
        out_shape=jax.ShapeDtypeStruct((rows, dim), BF16),
        grid_spec=pltpu.PrefetchScalarGridSpec(
            num_scalar_prefetch=1, grid=(4,),
            in_specs=[pl.BlockSpec(memory_space=pl.ANY)] * 4 + [pl.BlockSpec((wide, dim), lambda s, ix: (ix[1 + s], 0))],
            out_specs=pl.BlockSpec((rows, dim), lambda s, ix: (0, 0)),
            scratch_shapes=[pltpu.VMEM((2, rows, wide), BF16), pltpu.VMEM((rows, dim), F32), pltpu.SemaphoreType.DMA((2,))]),
        compiler_params=pltpu.CompilerParams(dimension_semantics=("arbitrary",), vmem_limit_bytes=VMEM_BYTES),
        cost_estimate=cost(8 * rows * dim * wide, 2 * (5 * rows * dim)),
        name="out_proj",
    )(idx, *pieces, w_o)


def dh_kernel(idx, *refs):
    pieces = refs[:8]
    wq_ref, wk_ref, wv_ref, x_hbm, lnw_ref, dx_ref, dw_ref, cur_sc, acc_sc, x_ref, dx_sc, sem, piece_sem, x_sem = refs[8:]
    src = pl.program_id(0)
    wide = wq_ref.shape[1]
    each = wide // 2
    rows = cur_sc.shape[1]
    x_copy = pltpu.make_async_copy(x_hbm, x_ref, x_sem)

    def copies(n):
        at = pl.ds(pl.multiple_of(idx[0] * rows, rows) if n < 2 else 0, rows)
        out = []
        for t in range(2):
            piece = pieces[2 * n + t]
            spans = [(0, each, t * each)] + [(each + part * HEAD_DIM, HEAD_DIM, wide + (2 * part + t) * HEAD_DIM) for part in range(2)]
            for start, size, to in spans:
                out.append(pltpu.make_async_copy(piece.at[at, start:start + size], cur_sc.at[n % 2, :, to:to + size],
                                                 piece_sem.at[n % 2]))
        return out

    fetch_ahead(src, copies)

    @pl.when(src == 0)
    def _():
        x_copy.start()
        acc_sc[...] = jnp.zeros_like(acc_sc)

    both = wide + 2 * HEAD_DIM
    cur = src % 2
    accumulate(acc_sc, lambda cols: mm(cur_sc[cur, :, :wide], wq_ref[cols, :], ((1,), (1,)))
               + mm(cur_sc[cur, :, wide:both], wk_ref[cols, :], ((1,), (1,)))
               + mm(cur_sc[cur, :, both:], wv_ref[cols, :], ((1,), (1,))))

    @pl.when(src == 3)
    def _():
        x_copy.wait()
        blk = dx_sc.shape[1]
        n_blk = x_ref.shape[0] // blk
        weight = lnw_ref[...].astype(F32)
        dw_ref[...] = jnp.zeros_like(dw_ref)

        def put(n, slot):
            return pltpu.make_async_copy(dx_sc.at[slot], dx_ref.at[pl.ds(n * blk, blk), :], sem.at[slot])

        def one(n, _):
            slot = n % 2
            rows = pl.ds(n * blk, blk)

            @pl.when(n >= 2)
            def _():
                put(n - 2, slot).wait()

            xf = x_ref[rows, :].astype(F32)
            mean = jnp.mean(xf, axis=-1, keepdims=True)
            cen = xf - mean
            var = jnp.mean(cen * cen, axis=-1, keepdims=True)
            rstd = lax.rsqrt(var + LN_EPS)
            xhat = cen * rstd
            dh = acc_sc[rows, :]
            dw_ref[...] += jnp.sum(dh * xhat, axis=0, keepdims=True)
            dxh = dh * weight
            mean_d = jnp.mean(dxh, axis=-1, keepdims=True)
            mean_dx = jnp.mean(dxh * xhat, axis=-1, keepdims=True)
            dx_sc[slot] = (rstd * (dxh - mean_d - xhat * mean_dx)).astype(BF16)
            put(n, slot).start()
            return 0

        lax.fori_loop(0, n_blk, one, 0)
        for n in range(n_blk - 2, n_blk):
            put(n, n % 2).wait()


def hidden_grad(idx, pieces, w_q, w_k, w_v, x, ln_w, n_dev):
    rows, dim = x.shape
    cols = pieces[0].shape[1]
    cq, ck = w_q.shape[1] // n_dev, w_k.shape[1] // n_dev
    const = lambda s, ix: (0, 0)
    head = lambda s, ix: (0, ix[1 + s])
    blk = 128
    return pl.pallas_call(
        dh_kernel,
        out_shape=(jax.ShapeDtypeStruct((rows, dim), BF16), jax.ShapeDtypeStruct((1, dim), F32)),
        grid_spec=pltpu.PrefetchScalarGridSpec(
            num_scalar_prefetch=1, grid=(4,),
            in_specs=[pl.BlockSpec(memory_space=pl.ANY)] * 8
            + [pl.BlockSpec((dim, cq), head), pl.BlockSpec((dim, ck), head), pl.BlockSpec((dim, ck), head),
               pl.BlockSpec(memory_space=pl.ANY), pl.BlockSpec((1, dim), const)],
            out_specs=(pl.BlockSpec(memory_space=pl.ANY), pl.BlockSpec((1, dim), const)),
            scratch_shapes=[pltpu.VMEM((2, rows, 2 * cols), BF16), pltpu.VMEM((rows, dim), F32),
                            pltpu.VMEM((rows, dim), BF16), pltpu.VMEM((2, blk, dim), BF16),
                            pltpu.SemaphoreType.DMA((2,)), pltpu.SemaphoreType.DMA((2,)), pltpu.SemaphoreType.DMA]),
        compiler_params=pltpu.CompilerParams(dimension_semantics=("arbitrary",), vmem_limit_bytes=VMEM_BYTES),
        cost_estimate=cost(16 * rows * dim * cols, 2 * (2 * rows * dim + 8 * cols * (rows + dim))),
        name="hidden_grad",
    )(idx, *pieces, w_q, w_k, w_v, x, ln_w)


def reserve(*shapes):
    return pl.pallas_call(
        lambda *refs: None,
        out_shape=tuple(jax.ShapeDtypeStruct(s, BF16) for s in shapes),
        out_specs=tuple(pl.BlockSpec(memory_space=pl.ANY) for _ in shapes),
        cost_estimate=cost(1, 1),
        name="reserve",
    )()


def dw_kernel(idx, *refs):
    hs, refs = refs[:4], refs[4:]
    n = len(refs) - 8
    rows = hs[0].shape[0]
    grs, (q_ref, k_ref, v_ref, piece_ref, gr_sc) = refs[:n], refs[-5:]
    wide = q_ref.shape[1] // n
    cols = piece_ref.shape[1]

    @pl.when(pl.program_id(0) == 0)
    def _():
        for b in range(4):
            to = slice(b * rows, (b + 1) * rows)
            at = pl.ds(idx[1 + b] * rows, rows)
            for t, gr in enumerate(grs):
                gr_sc[to, t * wide:(t + 1) * wide] = gr[at, :wide]
                for part in range(2):
                    start = n * wide + part * n * HEAD_DIM + t * HEAD_DIM
                    gr_sc[to, start:start + HEAD_DIM] = gr[at, wide + part * HEAD_DIM:wide + (part + 1) * HEAD_DIM]

    for start in range(0, cols, 256):
        stop = min(start + 256, cols)
        val = sum(mm(h[...], gr_sc[b * rows:(b + 1) * rows, start:stop], ((0,), (0,))) for b, h in enumerate(hs))
        piece_ref[:, start:stop] = val.astype(BF16)
    q_ref[...] = piece_ref[:, :n * wide]
    k_ref[...] = piece_ref[:, n * wide:n * (wide + HEAD_DIM)]
    v_ref[...] = piece_ref[:, n * (wide + HEAD_DIM):]


def weight_grad(idx, hs, grs, bufs):
    (both, dim), n = hs[0].shape, len(grs)
    rows = both // 2
    seq = 2 * both
    cols = n * grs[0].shape[1]
    wide = REP * HEAD_DIM * n
    blk = 512
    there = lambda i, ix: (i, ix[0])
    flops = 2 * seq * dim * cols
    return pl.pallas_call(
        dw_kernel,
        out_shape=tuple(jax.ShapeDtypeStruct(b.shape, BF16) for b in bufs) + (jax.ShapeDtypeStruct((dim, cols), BF16),),
        grid_spec=pltpu.PrefetchScalarGridSpec(
            num_scalar_prefetch=1, grid=(dim // blk,),
            in_specs=[pl.BlockSpec((rows, blk), lambda i, ix: (0, i))] * 2 + [pl.BlockSpec((rows, blk), lambda i, ix: (1, i))] * 2
            + [pl.BlockSpec((seq, cols // n), lambda i, ix: (0, 0), pipeline_mode=pl.Buffered(1)) for _ in grs]
            + [pl.BlockSpec(memory_space=pl.ANY)] * 3,
            out_specs=(pl.BlockSpec((blk, wide), there), pl.BlockSpec((blk, n * HEAD_DIM), there),
                       pl.BlockSpec((blk, n * HEAD_DIM), there), pl.BlockSpec((blk, cols), lambda i, ix: (i, 0))),
            scratch_shapes=[pltpu.VMEM((seq, cols), BF16)]),
        input_output_aliases={5 + n: 0, 6 + n: 1, 7 + n: 2},
        compiler_params=pltpu.CompilerParams(dimension_semantics=("arbitrary",), vmem_limit_bytes=VMEM_BYTES),
        cost_estimate=cost(flops, 2 * (seq * dim + seq * cols + 2 * dim * cols)),
        name="weight_grad",
    )(idx, *hs, *grs, *bufs)


def dwo_kernel(idx, o_ref, *refs):
    gs, (buf_ref, out_ref, piece_ref) = refs[:4], refs[4:]
    rows = gs[0].shape[0]
    for start in range(0, piece_ref.shape[1], 256):
        cols = slice(start, start + 256)
        val = sum(mm(o_ref[pl.ds(idx[1 + b] * rows, rows), :], g[:, cols], ((0,), (0,))) for b, g in enumerate(gs))
        piece_ref[:, cols] = val.astype(BF16)
    out_ref[...] = piece_ref[...]


def out_weight_grad(idx, o, gs, buf):
    seq, wide = o.shape
    rows, dim = gs[0].shape
    blk = 512
    return pl.pallas_call(
        dwo_kernel,
        out_shape=(jax.ShapeDtypeStruct(buf.shape, BF16), jax.ShapeDtypeStruct((wide, dim), BF16)),
        grid_spec=pltpu.PrefetchScalarGridSpec(
            num_scalar_prefetch=1, grid=(dim // blk,),
            in_specs=[single((seq, wide), lambda i, ix: (0, 0))]
            + [pl.BlockSpec((rows, blk), lambda i, ix: (0, i))] * 4 + [pl.BlockSpec(memory_space=pl.ANY)],
            out_specs=(pl.BlockSpec((wide, blk), lambda i, ix: (ix[0], i)), pl.BlockSpec((wide, blk), lambda i, ix: (0, i)))),
        input_output_aliases={6: 0},
        compiler_params=pltpu.CompilerParams(dimension_semantics=("arbitrary",), vmem_limit_bytes=VMEM_BYTES),
        cost_estimate=cost(2 * seq * wide * dim, 2 * (seq * dim + seq * wide + 2 * wide * dim)),
        name="out_weight_grad",
    )(idx, o, *gs, buf)


def place_kernel(idx, piece_ref, *refs):
    q_ref, k_ref, v_ref = refs[-3:]
    wide, one = q_ref.shape[1], k_ref.shape[1]
    q_ref[...] = piece_ref[:, :wide]
    k_ref[...] = piece_ref[:, wide:wide + one]
    v_ref[...] = piece_ref[:, wide + one:]


def place(idx, piece, bufs):
    dim, cols = piece.shape
    one = cols // (REP + 2)
    blk = 512
    there = lambda i, ix: (i, ix[0])
    return pl.pallas_call(
        place_kernel,
        out_shape=tuple(jax.ShapeDtypeStruct(b.shape, BF16) for b in bufs),
        grid_spec=pltpu.PrefetchScalarGridSpec(
            num_scalar_prefetch=1, grid=(dim // blk,),
            in_specs=[pl.BlockSpec((blk, cols), lambda i, ix: (i, 0))] + [pl.BlockSpec(memory_space=pl.ANY)] * 3,
            out_specs=(pl.BlockSpec((blk, REP * one), there), pl.BlockSpec((blk, one), there),
                       pl.BlockSpec((blk, one), there))),
        input_output_aliases={2: 0, 3: 1, 4: 2},
        compiler_params=pltpu.CompilerParams(dimension_semantics=("arbitrary",)),
        cost_estimate=cost(4 * dim * cols, 4 * dim * cols),
        name="place",
    )(idx, piece, *bufs)


def solution(mesh):
    n_dev = mesh.shape['sp']
    row_spec = P(('dp', 'sp'), None)
    pos_spec = P(('dp', 'sp'))
    full_spec = P(None, None)
    grad_spec = P('dp', None)

    def over_chip(val):
        return lax.ppermute(val, 'sp', [(i, i ^ 2) for i in range(n_dev)])

    def over_core(val):
        return lax.ppermute(val, 'sp', [(i, i ^ 1) for i in range(n_dev)])

    def layer(hidden, positions, d_attn, ln_weight, w_q, w_k, w_v, w_o):
        rows, dim = hidden.shape
        seq = rows * n_dev
        kv_local = w_k.shape[1] // HEAD_DIM // n_dev
        cq = w_q.shape[1] // n_dev
        me = lax.axis_index('sp')
        chip, core = me // 2, me % 2
        hb = 2 * core + chip
        hbs = [hb, hb ^ 1, hb ^ 2, hb ^ 3]
        toks = [me, me ^ 2, me ^ 1, me ^ 3]

        pos_par = over_chip(positions)
        pos_src = (positions, over_core(positions), pos_par, over_core(pos_par))
        pos = jnp.concatenate([lax.select_n(me ^ b, *pos_src) for b in range(n_dev)])
        ln_row = ln_weight.reshape(1, dim)
        x_par = over_chip(hidden)
        g_par = over_chip(d_attn)
        x_sib = over_core(hidden)
        g_sib = over_core(d_attn)

        inv_freq = ROPE_BASE ** (-jnp.arange(0, HEAD_DIM, 2, dtype=F32) / HEAD_DIM)
        angles = pos.astype(F32)[:, None] * jnp.repeat(inv_freq, 2)[None, :]
        cos_t = jnp.cos(angles)
        sin_t = jnp.sin(angles) * jnp.where(jnp.arange(HEAD_DIM) % 2 == 0, -1.0, 1.0)[None, :]

        x_sp = over_core(x_par)
        g_sp = over_core(g_par)

        def pair(b):
            return jnp.stack([hb, toks[b], toks[b + 2]]).astype(jnp.int32)

        h_mine, qkv = qkv_blocks(pair(0), (hidden, x_sib), ln_row, w_q, w_k, w_v, cos_t, sin_t, seq, n_dev, None)
        h_far, qkv = qkv_blocks(pair(1), (x_par, x_sp), ln_row, w_q, w_k, w_v, cos_t, sin_t, seq, n_dev, qkv)
        hs = (h_mine, h_far, h_mine, h_far)
        o_own, o_t, lse = attn_forward(qkv, kv_local)

        wo_t = transpose_rows(hb.reshape(1).astype(jnp.int32), w_o, n_dev)
        gs = [d_attn, g_par, g_sib, g_sp]
        d_o = do_blocks(pair(0), (d_attn, g_sib), wo_t, seq, None)
        d_o = do_blocks(pair(1), (g_par, g_sp), wo_t, seq, d_o)

        def own_rows(val, dev):
            return lax.dynamic_slice_in_dim(val, dev * rows, rows, 0)

        o_par = over_chip(lax.dynamic_slice_in_dim(o_own, (chip ^ 1) * 2 * rows, 2 * rows, 0))
        sources = jnp.stack([me, *hbs]).astype(jnp.int32)
        o_tok = [o_own, o_par, over_core(own_rows(o_own, me ^ 1)), over_core(own_rows(o_par, core ^ 1))]
        attn_out = out_proj(sources, o_tok, w_o, rows)

        def blocks(where):
            return jnp.stack([where, *toks]).astype(jnp.int32)

        d_w_o, *d_w = reserve(w_o.shape, w_q.shape, w_k.shape, w_v.shape)
        d_w_o, piece = out_weight_grad(blocks(hbs[0]), o_own, gs, d_w_o)
        far = over_chip(piece)
        for b, val in ((hbs[2], over_core(piece)), (hbs[1], far), (hbs[3], over_core(far))):
            d_w_o = lax.dynamic_update_slice_in_dim(d_w_o, val, b * cq, 0)

        gr = []
        for t in range(kv_local):
            gr.append(attn_backward(qkv, d_o, o_t, lse, cos_t, sin_t, kv_local, t))
        gr_par = [over_chip(val) for val in gr]

        def col(val):
            return val.reshape(1).astype(jnp.int32)

        *d_w, piece = weight_grad(blocks(hbs[0]), hs, gr, d_w)
        piece = over_core(piece)
        d_w = place(col(hbs[2]), piece, d_w)
        gr_tok = [gr, gr_par, [], []]
        for t in range(kv_local):
            gr_tok[2].append(over_core(own_rows(gr[t], me ^ 1)))
            gr_tok[3].append(over_core(own_rows(gr_par[t], me ^ 1)))
            *d_w, piece = weight_grad(blocks(hbs[1] * kv_local + t), hs, (gr_par[t],), d_w)
            piece = over_core(piece)
            d_w = place(col(hbs[3] * kv_local + t), piece, d_w)
        d_hid, d_lnw = hidden_grad(sources, [val for pair in gr_tok for val in pair], w_q, w_k, w_v, hidden, ln_row, n_dev)
        d_lnw = d_lnw + over_core(d_lnw)
        d_lnw = d_lnw + over_chip(d_lnw)
        return (attn_out, d_hid, d_lnw.reshape(dim).astype(BF16), *d_w, d_w_o)

    return jax.shard_map(layer, mesh=mesh,
                         in_specs=(row_spec, pos_spec, row_spec, P(None), full_spec, full_spec, full_spec, full_spec),
                         out_specs=(row_spec, row_spec, P('dp'), grad_spec, grad_spec, grad_spec, grad_spec),
                         check_vma=False)
```
